32 devices in a mesh: tp: 4 (over z), fsdp: 8 (over y, x, core).
Axes of the slice: x: 2, y: 2, z: 4, core: 2. Of those that a mesh axis runs over, the one named last changes fastest.
Arguments:
- g_qkv: float32 [8, 16, 384, 1152], P('fsdp', None, None, 'tp')
- g_out: float32 [8, 16, 384, 384], P('fsdp', None, None, 'tp')
- g_up: float32 [8, 16, 384, 1536], P('fsdp', None, None, 'tp')
- g_down: float32 [8, 16, 1536, 384], P('fsdp', None, None, 'tp')
- g_vec: float32 [8, 16, 4992], P('fsdp', None, 'tp')
- w_qkv: float32 [16, 384, 1152], P(None, 'fsdp', 'tp')
- w_out: float32 [16, 384, 384], P(None, 'fsdp', 'tp')
- w_up: float32 [16, 384, 1536], P(None, 'fsdp', 'tp')
- w_down: float32 [16, 1536, 384], P(None, 'fsdp', 'tp')
- w_vec: float32 [16, 4992], P(None, 'tp')
- m_qkv: bfloat16 [16, 384, 1152], P(None, 'fsdp', 'tp')
- m_out: bfloat16 [16, 384, 384], P(None, 'fsdp', 'tp')
- m_up: bfloat16 [16, 384, 1536], P(None, 'fsdp', 'tp')
- m_down: bfloat16 [16, 1536, 384], P(None, 'fsdp', 'tp')
- m_vec: bfloat16 [16, 4992], P(None, 'tp')
- vr_qkv: float32 [16, 384], P(None, 'fsdp')
- vc_qkv: float32 [16, 1152], P(None, 'tp')
- vr_out: float32 [16, 384], P(None, 'fsdp')
- vc_out: float32 [16, 384], P(None, 'tp')
- vr_up: float32 [16, 384], P(None, 'fsdp')
- vc_up: float32 [16, 1536], P(None, 'tp')
- vr_down: float32 [16, 1536], P(None, 'fsdp')
- vc_down: float32 [16, 384], P(None, 'tp')
- v_vec: float32 [16, 4992], P(None, 'tp')
Outputs:
- output 1: float32 [16, 384, 1152], P(None, 'fsdp', 'tp')
- output 2: float32 [16, 384, 384], P(None, 'fsdp', 'tp')
- output 3: float32 [16, 384, 1536], P(None, 'fsdp', 'tp')
- output 4: float32 [16, 1536, 384], P(None, 'fsdp', 'tp')
- output 5: float32 [16, 4992], P(None, 'tp')
- output 6: bfloat16 [16, 384, 1152], P(None, 'fsdp', 'tp')
- output 7: bfloat16 [16, 384, 384], P(None, 'fsdp', 'tp')
- output 8: bfloat16 [16, 384, 1536], P(None, 'fsdp', 'tp')
- output 9: bfloat16 [16, 1536, 384], P(None, 'fsdp', 'tp')
- output 10: bfloat16 [16, 4992], P(None, 'tp')
- output 11: float32 [16, 384], P(None, 'fsdp')
- output 12: float32 [16, 1152], P(None, 'tp')
- output 13: float32 [16, 384], P(None, 'fsdp')
- output 14: float32 [16, 384], P(None, 'tp')
- output 15: float32 [16, 384], P(None, 'fsdp')
- output 16: float32 [16, 1536], P(None, 'tp')
- output 17: float32 [16, 1536], P(None, 'fsdp')
- output 18: float32 [16, 384], P(None, 'tp')
- output 19: float32 [16, 4992], P(None, 'tp')
All inputs are finite; a program needn't handle non-finite values.
Results may differ from the reference program's by a relative error of at most 0.001.
Values sent between devices are 32-bit elements.
A program may use at most 1 GiB of HBM per device.

```python
import jax
import jax.numpy as jnp

MODEL_DIM = 384
MLP_DIM = 1536
NUM_LAYERS = 16
GRAD_SHARDS = 8
TRAIN_STEP = 3
VEC_LEN = 9 * MODEL_DIM + MLP_DIM
MAT_PARAMS = 4 * MODEL_DIM * MODEL_DIM + 2 * MODEL_DIM * MLP_DIM
VEC_SCALE = (0.25 * MAT_PARAMS / VEC_LEN) ** 0.5
LEARN_RATE = 0.0008
WEIGHT_DECAY = 0.03
MOMENTUM = 0.9
EPSILON = 1e-30
BETA_TWO = 1.0 - TRAIN_STEP ** -0.8
LEVELS = ((0.2, 0.6), (2.0, 4.0), (0.2, 0.6), (2.0, 4.0))


def mat_shapes():
    return [(MODEL_DIM, 3 * MODEL_DIM), (MODEL_DIM, MODEL_DIM), (MODEL_DIM, MLP_DIM), (MLP_DIM, MODEL_DIM)]


def profile(key, count):
    key_sign, key_noise = jax.random.split(key)
    sign_val = 2.0 * jax.random.randint(key_sign, (NUM_LAYERS, 1), 0, 2).astype(jnp.float32) - 1.0
    ramp_val = jnp.linspace(-1.0, 1.0, count, dtype=jnp.float32)
    noise_val = jax.random.normal(key_noise, (NUM_LAYERS, count), jnp.float32)
    return jnp.exp(0.8 * sign_val * ramp_val[None, :] + 0.4 * noise_val)


def draw_partials(key, row_count, col_count):
    key_row, key_col, key_dev, key_val = jax.random.split(key, 4)
    row_scale = profile(key_row, row_count)
    col_scale = profile(key_col, col_count)
    dev_scale = jax.random.uniform(key_dev, (GRAD_SHARDS, NUM_LAYERS, 1, 1), jnp.float32, 0.5, 1.5)
    noise_val = jax.random.normal(key_val, (GRAD_SHARDS, NUM_LAYERS, row_count, col_count), jnp.float32)
    return noise_val * dev_scale * row_scale[None, :, :, None] * col_scale[None, :, None, :]


def draw_vector_partials(key):
    key_col, key_dev, key_val = jax.random.split(key, 3)
    col_scale = VEC_SCALE * profile(key_col, VEC_LEN)
    dev_scale = jax.random.uniform(key_dev, (GRAD_SHARDS, NUM_LAYERS, 1), jnp.float32, 0.5, 1.5)
    noise_val = jax.random.normal(key_val, (GRAD_SHARDS, NUM_LAYERS, VEC_LEN), jnp.float32)
    return noise_val * dev_scale * col_scale[None]


def setup_inputs(seed: int = 0) -> dict:
    key_list = jax.random.split(jax.random.key(seed), 8)
    shapes = mat_shapes()
    mat_names = ['qkv', 'out', 'up', 'down']
    partials = [draw_partials(jax.random.fold_in(key_list[0], mat_index), shapes[mat_index][0], shapes[mat_index][1]) for mat_index in range(4)]
    vec_partials = draw_vector_partials(key_list[1])
    grad_sums = [jnp.sum(part_val, axis=0) for part_val in partials + [vec_partials]]
    total_sq = sum([jnp.sum(jnp.square(grad_sum)) for grad_sum in grad_sums])
    clip_scale = jnp.minimum(1.0, 1.0 / jnp.sqrt(total_sq))
    result = {}
    for mat_index in range(4):
        result['g_' + mat_names[mat_index]] = partials[mat_index]
    result['g_vec'] = vec_partials
    for mat_index in range(4):
        full_shape = (NUM_LAYERS,) + shapes[mat_index]
        result['w_' + mat_names[mat_index]] = jax.random.normal(jax.random.fold_in(key_list[2], mat_index), full_shape, jnp.float32) * shapes[mat_index][0] ** -0.5
    result['w_vec'] = 0.5 * jax.random.normal(key_list[3], (NUM_LAYERS, VEC_LEN), jnp.float32)
    for mat_index in range(4):
        full_shape = (NUM_LAYERS,) + shapes[mat_index]
        result['m_' + mat_names[mat_index]] = (0.1 * jax.random.normal(jax.random.fold_in(key_list[4], mat_index), full_shape, jnp.float32)).astype(jnp.bfloat16)
    result['m_vec'] = (0.1 * jax.random.normal(key_list[5], (NUM_LAYERS, VEC_LEN), jnp.float32)).astype(jnp.bfloat16)
    for mat_index in range(4):
        key_level, key_row, key_col = jax.random.split(jax.random.fold_in(key_list[6], mat_index), 3)
        grad_sq = jnp.square(grad_sums[mat_index] * clip_scale)
        level_val = jax.random.uniform(key_level, (NUM_LAYERS, 1), jnp.float32, LEVELS[mat_index][0], LEVELS[mat_index][1])
        row_factor = jax.random.uniform(key_row, (NUM_LAYERS, shapes[mat_index][0]), jnp.float32, 0.3, 1.2)
        col_factor = jax.random.uniform(key_col, (NUM_LAYERS, shapes[mat_index][1]), jnp.float32, 0.3, 1.2)
        result['vr_' + mat_names[mat_index]] = level_val * row_factor * jnp.mean(grad_sq, axis=2)
        result['vc_' + mat_names[mat_index]] = level_val * col_factor * jnp.mean(grad_sq, axis=1)
    key_level, key_val = jax.random.split(key_list[7])
    vec_sq = jnp.square(grad_sums[4] * clip_scale)
    level_val = jax.random.uniform(key_level, (NUM_LAYERS, 1), jnp.float32, 0.1, 0.3)
    result['v_vec'] = level_val * jnp.exp(0.5 * jax.random.normal(key_val, (NUM_LAYERS, VEC_LEN), jnp.float32)) * jnp.mean(vec_sq, axis=1, keepdims=True)
    return result


def finish_step(update_val, weight, moment):
    moment_new = (MOMENTUM * moment.astype(jnp.float32) + (1.0 - MOMENTUM) * update_val).astype(jnp.bfloat16)
    weight_new = weight - LEARN_RATE * (moment_new.astype(jnp.float32) + WEIGHT_DECAY * weight)
    return weight_new, moment_new


def matrix_step(grad_sum, clip_scale, weight, moment, row_var, col_var):
    grad_val = grad_sum * clip_scale
    grad_sq = jnp.square(grad_val) + EPSILON
    row_new = BETA_TWO * row_var + (1.0 - BETA_TWO) * jnp.mean(grad_sq, axis=2)
    col_new = BETA_TWO * col_var + (1.0 - BETA_TWO) * jnp.mean(grad_sq, axis=1)
    row_norm = row_new / jnp.mean(row_new, axis=1, keepdims=True)
    update_val = grad_val / jnp.sqrt(row_norm[:, :, None] * col_new[:, None, :])
    update_rms = jnp.sqrt(jnp.mean(jnp.square(update_val), axis=(1, 2), keepdims=True))
    update_val = update_val / jnp.maximum(1.0, update_rms)
    weight_new, moment_new = finish_step(update_val, weight, moment)
    return weight_new, moment_new, row_new, col_new


def vector_step(grad_sum, clip_scale, weight, moment, var_old):
    grad_val = grad_sum * clip_scale
    var_new = BETA_TWO * var_old + (1.0 - BETA_TWO) * (jnp.square(grad_val) + EPSILON)
    update_val = grad_val / jnp.sqrt(var_new)
    update_rms = jnp.sqrt(jnp.mean(jnp.square(update_val), axis=1, keepdims=True))
    update_val = update_val / jnp.maximum(1.0, update_rms)
    weight_new, moment_new = finish_step(update_val, weight, moment)
    return weight_new, moment_new, var_new


def reference(g_qkv, g_out, g_up, g_down, g_vec, w_qkv, w_out, w_up, w_down, w_vec, m_qkv, m_out, m_up, m_down, m_vec, vr_qkv, vc_qkv, vr_out, vc_out, vr_up, vc_up, vr_down, vc_down, v_vec):
    grad_sums = [jnp.sum(g_part, axis=0) for g_part in (g_qkv, g_out, g_up, g_down, g_vec)]
    total_sq = sum([jnp.sum(jnp.square(grad_sum)) for grad_sum in grad_sums])
    clip_scale = jnp.minimum(1.0, 1.0 / jnp.sqrt(total_sq))
    weights = (w_qkv, w_out, w_up, w_down)
    moments = (m_qkv, m_out, m_up, m_down)
    row_vars = (vr_qkv, vr_out, vr_up, vr_down)
    col_vars = (vc_qkv, vc_out, vc_up, vc_down)
    results = [matrix_step(grad_sums[mat_index], clip_scale, weights[mat_index], moments[mat_index], row_vars[mat_index], col_vars[mat_index]) for mat_index in range(4)]
    vec_res = vector_step(grad_sums[4], clip_scale, w_vec, m_vec, v_vec)
    return (results[0][0], results[1][0], results[2][0], results[3][0], vec_res[0], results[0][1], results[1][1], results[2][1], results[3][1], vec_res[1], results[0][2], results[0][3], results[1][2], results[1][3], results[2][2], results[2][3], results[3][2], results[3][3], vec_res[2])
```

```python
import functools

import jax
import jax.numpy as jnp
from jax import lax
from jax.experimental import pallas as pl
from jax.experimental.pallas import tpu as pltpu
from jax.sharding import PartitionSpec as P

TRAIN_STEP = 3
LEARN_RATE = 0.0008
WEIGHT_DECAY = 0.03
MOMENTUM = 0.9
EPSILON = 1e-30
BETA_TWO = 1.0 - TRAIN_STEP ** -0.8

MESH = pl.DeviceIdType.MESH
F32 = jnp.float32
LAYERS = 16
PAIR = 2
GROUP = 4
SOURCES = 5
UNITS = 6
BAND = 8
ROWS = 48
HALF = 64
CHIP = 96
LANES = 128
DIM = 384
VEC = 1248
PIECES = 12
SLOTS = 6
TILE_SLOT = (0, 0, 0, 1, 1, 1, 2, 3, 4, 5, 6)
TILE_COL = (0, 1, 2, 3, 4, 5, 6, 7, 7, 7, 7)


def row_parts(block):
    parts, row = [], LANES * block
    while row < LANES * block + LANES:
        stop = min((row // ROWS + 1) * ROWS, LANES * block + LANES)
        parts.append((row // ROWS, row % ROWS, row - LANES * block, stop - row))
        row = stop
    return parts


def lane_iota(shape):
    return lax.broadcasted_iota(jnp.int32, shape, len(shape) - 1)


def shifted(tiles, start, width):
    base, shift = start // LANES, start % LANES
    value = tiles[base] if shift == 0 else pltpu.roll(tiles[base], LANES - shift, 1)
    lane = lane_iota(value.shape)
    if shift + width > LANES:
        value = jnp.where(lane < LANES - shift, value, pltpu.roll(tiles[base + 1], LANES - shift, 1))
    return value if width == LANES else jnp.where(lane < width, value, 0.0)


def sum_down(value):
    slot = (lane_iota(value.shape) // BAND) % BAND
    part = jnp.where((slot >= 3) & (slot <= UNITS), value, 0.0)
    total = part + pltpu.roll(part, BAND, 1) + pltpu.roll(part, LAYERS, 1) + pltpu.roll(part, 24, 1)
    total = jnp.where(slot == UNITS, total, 0.0)
    total = total + pltpu.roll(total, 120, 1) + pltpu.roll(total, 112, 1) + pltpu.roll(total, 104, 1)
    return jnp.where((slot >= 3) & (slot <= UNITS), total, value)


def reduce_kernel(
    tp_size,
    gq, go, gu, gd, gvec, vr_q, vc_q, vr_o, vc_o, vr_u, vc_u, vr_d, vc_d, v_old,
    ut, vr_new, vc_new, scale, u_vec, v_new,
    own_u, own_q, own_o, own_d, rr_u, rr_q, rr_o, rr_d, cs, rxa, ryb, r2a, r2b, ff, fs,
    cr, rs, rrx, rv, vco, trx, t2rx, table, vd_pad, vec_a, vec_b, vec_c, vec_rx, vec_full,
    own_sem, d_send, d_recv, s1_send, s1_recv, s2_send, s2_recv, f_send, f_recv,
    c_send, c_recv, r_sem, t_sem, v_send, v_recv,
):
    f = lax.axis_index("fsdp")
    z = lax.axis_index("tp")
    c, x, y = f % PAIR, (f // PAIR) % PAIR, f // GROUP
    xn, yn, cn = 1 - x, 1 - y, 1 - c
    f_c, f_x, f_y = f + 1 - PAIR * c, f + PAIR - GROUP * x, f + GROUP - BAND * y
    me = z * BAND + f
    devices = tp_size * BAND

    def remote(src, dst, send, recv, **device):
        return pltpu.make_async_remote_copy(
            src_ref=src, dst_ref=dst, send_sem=send, recv_sem=recv, device_id=device, device_id_type=MESH
        )

    def wait_bytes(ref, sem):
        pltpu.make_async_copy(ref, ref, sem).wait()

    def source(k, n, group):
        if n < PAIR:
            return gu.at[pl.ds(GROUP * group + PAIR * n, PAIR)], own_u.at[PAIR * n : PAIR * n + PAIR], rr_u.at[k, PAIR * n : PAIR * n + PAIR]
        if n == PAIR:
            return gq.at[pl.ds(pl.multiple_of(1152 * group, BAND), 1152)], own_q, rr_q.at[k]
        if n == 3:
            return go.at[pl.ds(pl.multiple_of(DIM * group, BAND), DIM)], own_o, rr_o.at[k]
        return gd.at[pl.ds(pl.multiple_of(DIM * group, BAND), DIM)], own_d, rr_d.at[k]

    def own_copy(k, n):
        src, dst, _ = source(k, n, PAIR * k + c)
        return pltpu.make_async_copy(src, dst, own_sem.at[n])

    def core_copy(k, n):
        src, _, dst = source(k, n, PAIR * k + cn)
        return remote(src, dst, d_send.at[SOURCES * k + n], d_recv.at[SOURCES * k + n], fsdp=f_c)

    def s1_copies(p):
        slot = p % SLOTS
        return (
            remote(cs.at[slot, :, xn, 0:3], rxa.at[p], s1_send.at[PAIR * p], s1_recv.at[PAIR * p], fsdp=f_x),
            remote(cs.at[slot, yn, :, 3:UNITS], ryb.at[p], s1_send.at[PAIR * p + 1], s1_recv.at[PAIR * p + 1], fsdp=f_y),
        )

    def s2_copies(p):
        return (
            remote(rxa.at[p, yn], r2a.at[p], s2_send.at[PAIR * p], s2_recv.at[PAIR * p], fsdp=f_y),
            remote(ryb.at[p, xn], r2b.at[p], s2_send.at[PAIR * p + 1], s2_recv.at[PAIR * p + 1], fsdp=f_x),
        )

    def final_copy(p):
        return remote(fs.at[p], ff.at[c, p], f_send.at[p], f_recv.at[p], fsdp=f_c)

    for n in range(SOURCES):
        own_copy(0, n).start()

    barrier = pltpu.get_barrier_semaphore()

    def signal_all(d, carry):
        other = (me + d) % devices
        pl.semaphore_signal(
            barrier, inc=1, device_id={"tp": other // BAND, "fsdp": other % BAND}, device_id_type=MESH
        )
        return carry

    lax.fori_loop(1, devices, signal_all, 0)
    pl.semaphore_wait(barrier, devices - 1)

    for n in range(PAIR):
        core_copy(0, n).start()

    own_half = pl.ds(pl.multiple_of(BAND * c, BAND), BAND)
    other_half = pl.ds(pl.multiple_of(BAND * cn, BAND), BAND)
    vec_copies = (
        remote(gvec.at[other_half], vec_rx.at[0], v_send.at[0], v_recv.at[0], fsdp=f_c),
        remote(vec_a, vec_rx.at[1], v_send.at[1], v_recv.at[1], fsdp=f_x),
        remote(vec_b, vec_rx.at[PAIR], v_send.at[PAIR], v_recv.at[PAIR], fsdp=f_y),
        remote(vec_c, vec_full.at[own_half], v_send.at[3], v_recv.at[3], fsdp=f_c),
    )

    def vec_step(n):
        if n > 0:
            vec_copies[n - 1].wait_recv()
        if n == 1:
            vec_a[...] = gvec[own_half] + vec_rx[0]
        elif n == PAIR:
            vec_b[...] = vec_a[...] + vec_rx[1]
        elif n == 3:
            total = vec_b[...] + vec_rx[PAIR]
            vec_c[...] = total
            vec_full[own_half] = total
        if n < GROUP:
            vec_copies[n].start()

    vec_step(0)

    rs[...] = jnp.zeros((ROWS, LANES), F32)
    vco[...] = jnp.zeros((LANES, LANES), F32)
    table[...] = jnp.zeros((LANES, LANES), F32)
    vd_pad[...] = jnp.zeros((LAYERS, 256), F32)
    vd_pad[:, 0:192] = vr_d[...]
    for k in range(PAIR):
        rows = slice(BAND * k, BAND * k + BAND)
        for t, (ref, tile, width) in enumerate(
            [(vc_u, 0, LANES), (vc_u, 1, LANES), (vc_u, PAIR, LANES), (vc_q, 0, LANES), (vc_q, 1, LANES), (vc_q, PAIR, 32), (vc_o, 0, CHIP), (vc_d, 0, CHIP)]
        ):
            vco[HALF * k + BAND * t : HALF * k + BAND * t + BAND, 0:width] = ref[rows, LANES * tile : LANES * tile + width]
        for s, ref in enumerate((vr_u, vr_q, vr_o)):
            table[HALF * k + BAND * s : HALF * k + BAND * s + BAND, 0:ROWS] = ref[rows, :]
        tiles = (vd_pad[rows, 0:LANES], vd_pad[rows, LANES:256])
        for b in range(GROUP):
            table[HALF * k + 24 + BAND * b : HALF * k + 32 + BAND * b, :] = shifted(tiles, ROWS * b, ROWS)
    rv[...] = jnp.transpose(table[...])[0:ROWS, :]

    def pack_up(k, half, slot):
        def body(h, carry):
            q, core = h // PAIR, h % PAIR
            rows = pl.ds(pl.multiple_of(ROWS * h, BAND), ROWS)
            for i in range(PAIR):
                for t in range(3):
                    lanes = slice(LANES * t, LANES * t + LANES)
                    cs[slot, q // PAIR, q % PAIR, 3 * i + t, core] = (
                        own_u[PAIR * half + i, rows, lanes] + rr_u[k, PAIR * half + i, rows, lanes]
                    )
            return carry

        lax.fori_loop(0, BAND, body, 0)

    def pack_flat(own, other, slot, first, count, unit):
        def body(n, carry):
            rows = pl.ds(pl.multiple_of(LANES * (first + n), LANES), LANES)
            for block in range(3):
                lanes = slice(LANES * block, LANES * block + LANES)
                value = jnp.transpose(own[rows, lanes] + other[rows, lanes])
                for h, row, here, size in row_parts(block):
                    cs[slot, h // GROUP, (h // PAIR) % PAIR, unit + n, h % PAIR, row : row + size, :] = value[here : here + size]
            return carry

        lax.fori_loop(0, count, body, 0)

    def pack_down(k, slot):
        def body(n, carry):
            q, t = n // 3, n % 3
            rows = pl.ds(pl.multiple_of(LANES * t, LANES), LANES)
            for block in range(3):
                lanes = pl.ds(pl.multiple_of(DIM * q + LANES * block, LANES), LANES)
                value = jnp.transpose(own_d[rows, lanes] + rr_d[k, rows, lanes])
                for h, row, here, size in row_parts(block):
                    core, b = h // GROUP, h % GROUP
                    cs[slot + b // PAIR, q // PAIR, q % PAIR, 3 * (b % PAIR) + t, core, row : row + size, :] = value[
                        here : here + size
                    ]
            return carry

        lax.fori_loop(0, 12, body, 0)

    def prepare(p):
        k, n, slot = p // UNITS, p % UNITS, p % SLOTS
        needs = {0: (0,), 1: (1,), PAIR: (PAIR,), 3: (3,), GROUP: (GROUP,), SOURCES: ()}[n]
        for source_index in needs:
            own_copy(k, source_index).wait()
            core_copy(k, source_index).wait_recv()
        if p >= SLOTS and n != SOURCES:
            for copy in s1_copies(p - SLOTS):
                copy.wait_send()
            if n == GROUP:
                for copy in s1_copies(p + 1 - SLOTS):
                    copy.wait_send()
        if n < PAIR:
            pack_up(k, n, slot)
        elif n == PAIR:
            pack_flat(own_q, rr_q.at[k], slot, 0, UNITS, 0)
        elif n == 3:
            pack_flat(own_q, rr_q.at[k], slot, UNITS, 3, 0)
            pack_flat(own_o, rr_o.at[k], slot, 0, 3, 3)
        elif n == GROUP:
            pack_down(k, slot)
        for copy in s1_copies(p):
            copy.start()
        if n == 0 and k == 0:
            core_copy(0, PAIR).start()
            core_copy(0, 3).start()
        elif n == 1 and k == 0:
            core_copy(0, GROUP).start()
        if k == 0:
            reload = {0: (0,), 1: (1,), 3: (PAIR, 3), GROUP: (GROUP,)}.get(n, ())
            for source_index in reload:
                own_copy(1, source_index).start()
            for source_index in {PAIR: (0,), 3: (1,), GROUP: (PAIR, 3), SOURCES: (GROUP,)}.get(n, ()):
                core_copy(1, source_index).start()

    def stage_two(p):
        slot = p % SLOTS
        for copy in s1_copies(p):
            copy.wait_recv()

        def body(u, carry):
            for core in range(PAIR):
                rxa[p, yn, u, core] = rxa[p, yn, u, core] + cs[slot, yn, x, u, core]
                ryb[p, xn, u, core] = ryb[p, xn, u, core] + cs[slot, y, xn, 3 + u, core]
            return carry

        lax.fori_loop(0, 3, body, 0)
        for copy in s2_copies(p):
            copy.start()

    def stage_three(p):
        slot = p % SLOTS
        for copy in s2_copies(p):
            copy.wait_recv()

        def body(u, carry):
            fs[p, u] = cs[slot, y, x, u, cn] + rxa[p, y, u, cn] + r2a[p, u, cn]
            fs[p, 3 + u] = cs[slot, y, x, 3 + u, cn] + ryb[p, x, u, cn] + r2b[p, u, cn]
            return carry

        lax.fori_loop(0, 3, body, 0)
        final_copy(p).start()

        def body_own(u, carry):
            ff[c, p, u] = cs[slot, y, x, u, c] + rxa[p, y, u, c] + r2a[p, u, c]
            ff[c, p, 3 + u] = cs[slot, y, x, 3 + u, c] + ryb[p, x, u, c] + r2b[p, u, c]
            return carry

        lax.fori_loop(0, 3, body_own, 0)

    def keep(layer, tile, value, first=True):
        ut[layer, tile] = value
        square = value * value
        row = pl.ds(HALF * (layer // BAND) + BAND * TILE_COL[tile] + layer % BAND, 1)
        sums = jnp.sum(square, axis=0, keepdims=True)
        cr[f, row, :] = sums if first else cr[f, row, :] + sums
        return square

    def keep_rows(layer, slot, square):
        lane = HALF * (layer // BAND) + BAND * slot + layer % BAND
        sums = jnp.sum(square, axis=1, keepdims=True)
        rs[...] = jnp.where(lane_iota((ROWS, LANES)) == lane, sums, rs[...])

    def finish_up(k):
        def body(i8, carry):
            core, i = i8 // GROUP, i8 % GROUP
            layer = BAND * k + i8
            square = [keep(layer, t, ff[core, UNITS * k + i // PAIR, 3 * (i % PAIR) + t]) for t in range(3)]
            keep_rows(layer, 0, square[0] + square[1] + square[PAIR])
            return carry

        lax.fori_loop(0, BAND, body, 0)

    def finish_qkv(k):
        def body(core, carry):
            tiles = [ff.at[core, UNITS * k + PAIR + t // UNITS, t % UNITS] for t in range(12)]
            for i in range(GROUP):
                layer = BAND * k + GROUP * core + i
                first = PAIR * i
                part = [tiles[t][...] for t in range(first, min(first + GROUP, 9))]
                square = [
                    keep(layer, 3 + t, shifted(part, 32 * i + LANES * t, LANES if t < PAIR else 32)) for t in range(3)
                ]
                keep_rows(layer, 1, square[0] + square[1] + square[PAIR])
                part = [tiles[9 + t][...] for t in range(3)]
                keep_rows(layer, PAIR, keep(layer, UNITS, shifted(part, CHIP * i, CHIP)))
            return carry

        lax.fori_loop(0, PAIR, body, 0)

    def finish_down(k, half):
        def body(core, carry):
            for b in (PAIR * half, PAIR * half + 1):
                part = [ff[core, UNITS * k + GROUP + half, 3 * (b % PAIR) + t] for t in range(3)]
                for i in range(GROUP):
                    layer = BAND * k + GROUP * core + i
                    keep_rows(layer, 3 + b, keep(layer, 7 + b, shifted(part, CHIP * i, CHIP), first=b == 0))
            return carry

        lax.fori_loop(0, PAIR, body, 0)

    def column_rows(k, n):
        start, size = ((0, 24), (24, 32), (56, BAND))[n]
        return slice(HALF * k + start, HALF * k + start + size)

    def send_columns(k, n):
        rows = column_rows(k, n)

        def body(d, carry):
            remote(
                cr.at[f, rows], cr.at[f, rows], c_send.at[3 * k + n], c_recv.at[3 * k + n], fsdp=(f + d) % BAND
            ).start()
            return carry

        lax.fori_loop(1, BAND, body, 0)

    def finish(p):
        k, n = p // UNITS, p % UNITS
        final_copy(p).wait_recv()
        if n == 1:
            finish_up(k)
            send_columns(k, 0)
        elif n == 3:
            finish_qkv(k)
            send_columns(k, 1)
        elif n == GROUP:
            finish_down(k, 0)
        elif n == SOURCES:
            finish_down(k, 1)
            send_columns(k, PAIR)

    for step in range(PIECES + 3):
        if step < PIECES:
            prepare(step)
        if 0 <= step - 1 < PIECES:
            stage_two(step - 1)
        if 0 <= step - PAIR < PIECES:
            stage_three(step - PAIR)
        if 0 <= step - 3 < PIECES:
            finish(step - 3)
        if step in (1, 3, SOURCES, 7):
            vec_step((step + 1) // PAIR)

    rrx[z] = rs[...]

    def send_rows(d, carry):
        remote(rrx.at[z], rrx.at[z], r_sem.at[0], r_sem.at[1], tp=(z + d) % tp_size).start()
        return carry

    lax.fori_loop(1, tp_size, send_rows, 0)

    def exchange(ref, sems):
        def body(d, carry):
            other = (me + d) % devices
            remote(ref.at[me], ref.at[me], sems.at[0], sems.at[1], tp=other // BAND, fsdp=other % BAND).start()
            return carry

        lax.fori_loop(1, devices, body, 0)
        wait_bytes(ref.at[0 : devices - 1], sems.at[1])

    vec_sum = vec_full[...]
    vec_square = vec_sum * vec_sum
    vec_total = jnp.sum(jnp.sum(vec_square, axis=1, keepdims=True), axis=0, keepdims=True)
    trx[me, :, 0:LANES] = jnp.sum(rs[...], axis=0, keepdims=True)
    trx[me, :, LANES:256] = jnp.sum(rv[...], axis=0, keepdims=True)
    trx[me, :, 256:DIM] = jnp.broadcast_to(vec_total, (1, LANES))
    exchange(trx, t_sem)
    totals = jnp.sum(trx[...], axis=0)
    square_sum = totals[:, 0:LANES]
    old_sum = totals[:, LANES:256] * (1.0 / tp_size)
    vec_part = totals[:, 256:257] * 0.125
    total = jnp.sum(square_sum, axis=1, keepdims=True) + vec_part
    clip = jnp.minimum(1.0, 1.0 / jnp.sqrt(total))

    def clipped(value):
        return jnp.where(clip > 0.0, clip * (clip * value), 0.0)

    slot = (lane_iota((1, LANES)) // BAND) % BAND
    row_inv = jnp.where(slot >= 3, 1.0 / 1536.0, 1.0 / 384.0).astype(F32)
    col_inv = jnp.where(
        slot == 0, 1.0 / (384.0 * tp_size), jnp.where(slot == 1, 1.0 / (288.0 * tp_size), 1.0 / (96.0 * tp_size))
    ).astype(F32)
    mean_new = BETA_TWO * (sum_down(old_sum) * row_inv) + (1.0 - BETA_TWO) * (
        clipped(sum_down(square_sum)) * (row_inv * col_inv) + EPSILON
    )
    wait_bytes(rrx.at[0 : tp_size - 1], r_sem.at[1])
    row_new = BETA_TWO * rv[...] + (1.0 - BETA_TWO) * (clipped(jnp.sum(rrx[...], axis=0)) * col_inv + EPSILON)
    rv[...] = clip * lax.rsqrt(row_new / mean_new)
    table[0:ROWS, :] = row_new
    vr_new[...] = jnp.transpose(table[...])

    for k in range(PAIR):
        for n in range(3):
            rows = column_rows(k, n)
            wait_bytes(cr.at[0:7, rows], c_recv.at[3 * k + n])
    col_sum = cr[0]
    for other in range(1, BAND):
        col_sum = col_sum + cr[other]
    down_row = (lax.broadcasted_iota(jnp.int32, (LANES, LANES), 0) // BAND) % BAND == 7
    col_new = BETA_TWO * vco[...] + (1.0 - BETA_TWO) * (
        clipped(col_sum) * jnp.where(down_row, 1.0 / 1536.0, 1.0 / 384.0).astype(F32) + EPSILON
    )
    vc_new[...] = col_new
    vco[...] = lax.rsqrt(col_new)

    vec_grad = vec_sum * clip
    vec_var = BETA_TWO * v_old[...] + (1.0 - BETA_TWO) * (vec_grad * vec_grad + EPSILON)
    v_new[...] = vec_var
    vec_update = vec_grad / jnp.sqrt(vec_var)
    u_vec[...] = vec_update
    vec_rows = jnp.sum(vec_update * vec_update, axis=1, keepdims=True) * (0.125 / 128.0)
    vec_rows = jnp.broadcast_to(vec_rows, (LAYERS, LANES))
    table[56:HALF, :] = vec_rows[0:BAND]
    table[120:LANES, :] = vec_rows[BAND:LAYERS]

    def update(layer, carry):
        index = HALF * (layer // BAND) + layer % BAND
        lane = lane_iota((ROWS, LANES))
        factors = rv[...]
        tile = 0
        for s in range(7):
            row = jnp.sum(jnp.where(lane == index + BAND * s, factors, 0.0), axis=1, keepdims=True)
            square = None
            while tile < 11 and TILE_SLOT[tile] == s:
                value = ut[layer, tile] * row * vco[pl.ds(index + BAND * TILE_COL[tile], 1), :]
                ut[layer, tile] = value
                square = value * value if square is None else square + value * value
                tile += 1
            table[pl.ds(index + BAND * s, 1), :] = jnp.sum(square, axis=0, keepdims=True)
        return carry

    lax.fori_loop(0, LAYERS, update, 0)

    t2rx[me] = jnp.sum(jnp.transpose(table[...]), axis=0, keepdims=True)
    exchange(t2rx, t_sem.at[PAIR:GROUP])
    update_sum = sum_down(jnp.sum(t2rx[...], axis=0))
    inverse = jnp.where(slot == 7, 1.0 / (1248.0 * tp_size), row_inv * col_inv).astype(F32)
    factor = 1.0 / jnp.maximum(1.0, jnp.sqrt(update_sum * inverse))
    scale[...] = jnp.transpose(jnp.broadcast_to(factor, (LANES, LANES)))

    for k in range(PAIR):
        for n in range(SOURCES):
            core_copy(k, n).wait_send()
        for n in range(3):
            wait_bytes(cr.at[0:7, column_rows(k, n)], c_send.at[3 * k + n])
    for p in range(PIECES):
        if p >= PIECES - SLOTS:
            for copy in s1_copies(p):
                copy.wait_send()
        for copy in s2_copies(p):
            copy.wait_send()
        final_copy(p).wait_send()
    for copy in vec_copies:
        copy.wait_send()
    wait_bytes(rrx.at[0 : tp_size - 1], r_sem.at[0])
    wait_bytes(trx.at[0 : devices - 1], t_sem.at[0])
    wait_bytes(t2rx.at[0 : devices - 1], t_sem.at[PAIR])


def update_kernel(
    ut, vr_new, vc_new, scale, u_vec, v_new, w_q, w_o, w_u, w_d, w_v, m_q, m_o, m_u, m_d, m_v,
    wo_q, wo_o, wo_u, wo_d, wo_v, mo_q, mo_o, mo_u, mo_d, mo_v,
    vr_q, vc_q, vr_o, vc_o, vr_u, vc_u, vr_d, vc_d, v_out,
):
    step = pl.program_id(0)
    count = w_q.shape[0]

    def finish(update, weight, moment):
        moment_new = (MOMENTUM * moment.astype(F32) + (1.0 - MOMENTUM) * update).astype(jnp.bfloat16)
        return weight - LEARN_RATE * (moment_new.astype(F32) + WEIGHT_DECAY * weight), moment_new

    def body(i, carry):
        layer = step * count + i
        index = HALF * (layer // BAND) + layer % BAND

        def one(tile, slot, w, m, wo, mo, rows, lanes):
            factor = scale[pl.ds(index + BAND * slot, 1), :]
            update = (ut[i, tile] * factor)[:, 0 : lanes.stop - lanes.start]
            weight_new, moment_new = finish(update, w[i, rows, lanes], m[i, rows, lanes])
            wo[i, rows, lanes] = weight_new
            mo[i, rows, lanes] = moment_new

        every = slice(0, ROWS)
        for t in range(3):
            one(t, 0, w_u, m_u, wo_u, mo_u, every, slice(LANES * t, LANES * t + LANES))
            one(3 + t, 1, w_q, m_q, wo_q, mo_q, every, slice(LANES * t, min(LANES * t + LANES, 288)))
        one(UNITS, PAIR, w_o, m_o, wo_o, mo_o, every, slice(0, CHIP))
        for b in range(GROUP):
            one(7 + b, 3, w_d, m_d, wo_d, mo_d, slice(ROWS * b, ROWS * b + ROWS), slice(0, CHIP))
        return carry

    lax.fori_loop(0, count, body, 0)

    @pl.when(step == 0)
    def _():
        v_out[...] = v_new[...]
        for k in range(PAIR):
            rows = slice(BAND * k, BAND * k + BAND)
            for t in range(10):
                lanes = slice(LANES * t, min(LANES * t + LANES, VEC))
                factor = scale[HALF * k + 56 : HALF * k + HALF, 0 : lanes.stop - lanes.start]
                weight_new, moment_new = finish(u_vec[rows, lanes] * factor, w_v[rows, lanes], m_v[rows, lanes])
                wo_v[rows, lanes] = weight_new
                mo_v[rows, lanes] = moment_new
            for t, (ref, tile, width) in enumerate(
                [(vc_u, 0, LANES), (vc_u, 1, LANES), (vc_u, PAIR, LANES), (vc_q, 0, LANES), (vc_q, 1, LANES), (vc_q, PAIR, 32), (vc_o, 0, CHIP), (vc_d, 0, CHIP)]
            ):
                ref[rows, LANES * tile : LANES * tile + width] = vc_new[HALF * k + BAND * t : HALF * k + BAND * t + BAND, 0:width]
            for s, ref in enumerate((vr_u, vr_q, vr_o)):
                ref[rows, :] = vr_new[HALF * k + BAND * s : HALF * k + BAND * s + BAND, 0:ROWS]
            b0, b1, b2, b3 = (vr_new[HALF * k + 24 + BAND * b : HALF * k + 32 + BAND * b, :] for b in range(GROUP))
            lane = lane_iota((BAND, LANES))
            b2 = pltpu.roll(b2, CHIP, 1)
            vr_d[rows, 0:LANES] = jnp.where(lane < ROWS, b0, jnp.where(lane < CHIP, pltpu.roll(b1, ROWS, 1), b2))
            vr_d[rows, LANES:192] = jnp.where(lane < LAYERS, b2, pltpu.roll(b3, LAYERS, 1))[:, 0:HALF]


def solution(mesh):
    tp_size = mesh.shape["tp"]
    devices = tp_size * mesh.shape["fsdp"]
    vmem = pl.BlockSpec(memory_space=pltpu.VMEM)
    hbm = pl.BlockSpec(memory_space=pl.ANY)

    def local_step(g_qkv, g_out, g_up, g_down, g_vec, w_qkv, w_out, w_up, w_down, w_vec, m_qkv, m_out, m_up, m_down, m_vec, vr_qkv, vc_qkv, vr_out, vc_out, vr_up, vc_up, vr_down, vc_down, v_vec):
        def flat(g):
            g = jnp.swapaxes(g[0], 1, PAIR)
            return g.reshape(g.shape[0] * g.shape[1], g.shape[PAIR])

        dma = pltpu.SemaphoreType.DMA
        half = (BAND, VEC)
        sums = pl.pallas_call(
            functools.partial(reduce_kernel, tp_size),
            out_shape=[
                jax.ShapeDtypeStruct((LAYERS, 11, ROWS, LANES), F32),
                jax.ShapeDtypeStruct((LANES, LANES), F32),
                jax.ShapeDtypeStruct((LANES, LANES), F32),
                jax.ShapeDtypeStruct((LANES, LANES), F32),
                jax.ShapeDtypeStruct((LAYERS, VEC), F32),
                jax.ShapeDtypeStruct((LAYERS, VEC), F32),
            ],
            in_specs=[hbm] * GROUP + [vmem] * 10,
            out_specs=[vmem] * UNITS,
            scratch_shapes=[
                pltpu.VMEM((GROUP, DIM, DIM), F32),
                pltpu.VMEM((1152, DIM), F32),
                pltpu.VMEM((DIM, DIM), F32),
                pltpu.VMEM((DIM, 1536), F32),
                pltpu.VMEM((PAIR, GROUP, DIM, DIM), F32),
                pltpu.VMEM((PAIR, 1152, DIM), F32),
                pltpu.VMEM((PAIR, DIM, DIM), F32),
                pltpu.VMEM((PAIR, DIM, 1536), F32),
                pltpu.VMEM((SLOTS, PAIR, PAIR, UNITS, PAIR, ROWS, LANES), F32),
                pltpu.VMEM((PIECES, PAIR, 3, PAIR, ROWS, LANES), F32),
                pltpu.VMEM((PIECES, PAIR, 3, PAIR, ROWS, LANES), F32),
                pltpu.VMEM((PIECES, 3, PAIR, ROWS, LANES), F32),
                pltpu.VMEM((PIECES, 3, PAIR, ROWS, LANES), F32),
                pltpu.VMEM((PAIR, PIECES, UNITS, ROWS, LANES), F32),
                pltpu.VMEM((PIECES, UNITS, ROWS, LANES), F32),
                pltpu.VMEM((BAND, LANES, LANES), F32),
                pltpu.VMEM((ROWS, LANES), F32),
                pltpu.VMEM((tp_size, ROWS, LANES), F32),
                pltpu.VMEM((ROWS, LANES), F32),
                pltpu.VMEM((LANES, LANES), F32),
                pltpu.VMEM((devices, 1, DIM), F32),
                pltpu.VMEM((devices, 1, LANES), F32),
                pltpu.VMEM((LANES, LANES), F32),
                pltpu.VMEM((LAYERS, 256), F32),
                pltpu.VMEM(half, F32),
                pltpu.VMEM(half, F32),
                pltpu.VMEM(half, F32),
                pltpu.VMEM((3,) + half, F32),
                pltpu.VMEM((LAYERS, VEC), F32),
                dma((SOURCES,)),
                dma((10,)), dma((10,)),
                dma((PAIR * PIECES,)), dma((PAIR * PIECES,)),
                dma((PAIR * PIECES,)), dma((PAIR * PIECES,)),
                dma((PIECES,)), dma((PIECES,)),
                dma((UNITS,)), dma((UNITS,)),
                dma((PAIR,)), dma((GROUP,)),
                dma((GROUP,)), dma((GROUP,)),
            ],
            compiler_params=pltpu.CompilerParams(
                collective_id=0, has_side_effects=True, vmem_limit_bytes=56 * 1024 * 1024
            ),
            name="reduce",
        )(flat(g_qkv), flat(g_out), g_up[0], flat(g_down), g_vec[0], vr_qkv, vc_qkv, vr_out, vc_out, vr_up, vc_up, vr_down, vc_down, v_vec)

        block = GROUP

        def whole(a):
            return pl.BlockSpec(a.shape, lambda i: (0,) * a.ndim)

        def split(a):
            return pl.BlockSpec((block,) + a.shape[1:], lambda i: (i,) + (0,) * (a.ndim - 1))

        weights = (w_qkv, w_out, w_up, w_down)
        moments = (m_qkv, m_out, m_up, m_down)
        rest = (vr_qkv, vc_qkv, vr_out, vc_out, vr_up, vc_up, vr_down, vc_down, v_vec)
        in_specs = [split(sums[0])] + [whole(a) for a in sums[1:]]
        state_specs = [split(a) for a in weights] + [whole(w_vec)] + [split(a) for a in moments] + [whole(m_vec)]
        outs = weights + (w_vec,) + moments + (m_vec,) + rest
        return tuple(
            pl.pallas_call(
                update_kernel,
                grid=(LAYERS // block,),
                out_shape=[jax.ShapeDtypeStruct(a.shape, a.dtype) for a in outs],
                in_specs=in_specs + state_specs,
                out_specs=state_specs + [whole(a) for a in rest],
                compiler_params=pltpu.CompilerParams(vmem_limit_bytes=24 * 1024 * 1024),
                name="update",
            )(*sums, *weights, w_vec, *moments, m_vec)
        )

    grad_spec = P("fsdp", None, None, "tp")
    vec_grad_spec = P("fsdp", None, "tp")
    mat_spec = P(None, "fsdp", "tp")
    vec_spec = P(None, "tp")
    row_spec = P(None, "fsdp")
    state_specs = (mat_spec,) * GROUP + (vec_spec,) + (mat_spec,) * GROUP + (vec_spec,) + (row_spec, vec_spec) * GROUP + (vec_spec,)
    arg_specs = (grad_spec,) * GROUP + (vec_grad_spec,) + state_specs
    return jax.shard_map(local_step, mesh=mesh, in_specs=arg_specs, out_specs=state_specs, check_vma=False)
```

```python
import functools

import jax
import jax.numpy as jnp
from jax import lax
from jax.experimental import pallas as pl
from jax.experimental.pallas import tpu as pltpu
from jax.sharding import PartitionSpec as P

TRAIN_STEP = 3
LEARN_RATE = 0.0008
WEIGHT_DECAY = 0.03
MOMENTUM = 0.9
EPSILON = 1e-30
BETA_TWO = 1.0 - TRAIN_STEP ** -0.8

MESH = pl.DeviceIdType.MESH
F32 = jnp.float32
LAYERS = 16
PAIR = 2
GROUP = 4
OUTS = 19
SMALL = 10
SOURCES = 5
UNITS = 6
BAND = 8
ROWS = 48
HALF = 64
CHIP = 96
LANES = 128
DIM = 384
VEC = 1248
PIECES = 12
SLOTS = 6
TILE_SLOT = (0, 0, 0, 1, 1, 1, 2, 3, 4, 5, 6)
COLUMN_TILES = (
    ("u", 0, LANES), ("u", 1, LANES), ("u", PAIR, LANES),
    ("q", 0, LANES), ("q", 1, LANES), ("q", PAIR, 32), ("o", 0, CHIP), ("d", 0, CHIP),
)
TILE_COL = (0, 1, 2, 3, 4, 5, 6, 7, 7, 7, 7)


def row_parts(block):
    parts, row = [], LANES * block
    while row < LANES * block + LANES:
        stop = min((row // ROWS + 1) * ROWS, LANES * block + LANES)
        parts.append((row // ROWS, row % ROWS, row - LANES * block, stop - row))
        row = stop
    return parts


def lane_iota(shape):
    return lax.broadcasted_iota(jnp.int32, shape, len(shape) - 1)


def shifted(tiles, start, width):
    base, shift = start // LANES, start % LANES
    value = tiles[base] if shift == 0 else pltpu.roll(tiles[base], LANES - shift, 1)
    lane = lane_iota(value.shape)
    if shift + width > LANES:
        value = jnp.where(lane < LANES - shift, value, pltpu.roll(tiles[base + 1], LANES - shift, 1))
    return value if width == LANES else jnp.where(lane < width, value, 0.0)


def sum_down(value):
    slot = (lane_iota(value.shape) // BAND) % BAND
    part = jnp.where((slot >= 3) & (slot <= UNITS), value, 0.0)
    total = part + pltpu.roll(part, BAND, 1) + pltpu.roll(part, LAYERS, 1) + pltpu.roll(part, 24, 1)
    total = jnp.where(slot == UNITS, total, 0.0)
    total = total + pltpu.roll(total, 120, 1) + pltpu.roll(total, 112, 1) + pltpu.roll(total, 104, 1)
    return jnp.where((slot >= 3) & (slot <= UNITS), total, value)


def reduce_kernel(tp_size, gq, go, gu, gd, *refs):
    small_hbm, refs = refs[:SMALL], refs[SMALL:]
    ut, vr_new, vc_new, scale, u_vec, v_new, *refs = refs
    small, refs = refs[:SMALL], refs[SMALL:]
    gvec, vr_q, vc_q, vr_o, vc_o, vr_u, vc_u, vr_d, vc_d, v_old = small
    own_u, own_q, own_o, own_d, rr_u, rr_q, rr_o, rr_d, cs, rxa, ryb, r2a, r2b, ff, fs, *refs = refs
    cr, rs, rrx, rv, vco, trx, t2rx, table, vd_pad, vec_a, vec_b, vec_c, vec_rx, vec_full, *refs = refs
    small_sem, own_sem, d_send, d_recv, s1_send, s1_recv, s2_send, s2_recv, f_send, f_recv, *refs = refs
    c_send, c_recv, r_sem, t_sem, v_send, v_recv = refs
    f = lax.axis_index("fsdp")
    z = lax.axis_index("tp")
    c, x, y = f % PAIR, (f // PAIR) % PAIR, f // GROUP
    xn, yn, cn = 1 - x, 1 - y, 1 - c
    f_c, f_x, f_y = f + 1 - PAIR * c, f + PAIR - GROUP * x, f + GROUP - BAND * y
    me = z * BAND + f
    devices = tp_size * BAND

    def remote(src, dst, send, recv, **device):
        return pltpu.make_async_remote_copy(
            src_ref=src, dst_ref=dst, send_sem=send, recv_sem=recv, device_id=device, device_id_type=MESH
        )

    def wait_bytes(ref, sem):
        pltpu.make_async_copy(ref, ref, sem).wait()

    def source(k, n, group):
        if n < PAIR:
            return gu.at[pl.ds(GROUP * group + PAIR * n, PAIR)], own_u.at[PAIR * n : PAIR * n + PAIR], rr_u.at[k, PAIR * n : PAIR * n + PAIR]
        if n == PAIR:
            return gq.at[pl.ds(pl.multiple_of(1152 * group, BAND), 1152)], own_q, rr_q.at[k]
        if n == 3:
            return go.at[pl.ds(pl.multiple_of(DIM * group, BAND), DIM)], own_o, rr_o.at[k]
        return gd.at[pl.ds(pl.multiple_of(DIM * group, BAND), DIM)], own_d, rr_d.at[k]

    def own_copy(k, n):
        src, dst, _ = source(k, n, PAIR * k + c)
        return pltpu.make_async_copy(src, dst, own_sem.at[n])

    def core_copy(k, n):
        src, _, dst = source(k, n, PAIR * k + cn)
        return remote(src, dst, d_send.at[SOURCES * k + n], d_recv.at[SOURCES * k + n], fsdp=f_c)

    def s1_copies(p):
        slot = p % SLOTS
        return (
            remote(cs.at[slot, :, xn, 0:3], rxa.at[p], s1_send.at[PAIR * p], s1_recv.at[PAIR * p], fsdp=f_x),
            remote(cs.at[slot, yn, :, 3:UNITS], ryb.at[p], s1_send.at[PAIR * p + 1], s1_recv.at[PAIR * p + 1], fsdp=f_y),
        )

    def s2_copies(p):
        return (
            remote(rxa.at[p, yn], r2a.at[p], s2_send.at[PAIR * p], s2_recv.at[PAIR * p], fsdp=f_y),
            remote(ryb.at[p, xn], r2b.at[p], s2_send.at[PAIR * p + 1], s2_recv.at[PAIR * p + 1], fsdp=f_x),
        )

    def final_copy(p):
        return remote(fs.at[p], ff.at[c, p], f_send.at[p], f_recv.at[p], fsdp=f_c)

    for n in range(SOURCES):
        own_copy(0, n).start()
    small_copies = [pltpu.make_async_copy(small_hbm[n], small[n], small_sem.at[n]) for n in range(SMALL)]
    for copy in small_copies:
        copy.start()

    barrier = pltpu.get_barrier_semaphore()

    def signal_all(d, carry):
        other = (me + d) % devices
        pl.semaphore_signal(
            barrier, inc=1, device_id={"tp": other // BAND, "fsdp": other % BAND}, device_id_type=MESH
        )
        return carry

    lax.fori_loop(1, devices, signal_all, 0)
    pl.semaphore_wait(barrier, devices - 1)

    for n in range(PAIR):
        core_copy(0, n).start()

    own_half = pl.ds(pl.multiple_of(BAND * c, BAND), BAND)
    other_half = pl.ds(pl.multiple_of(BAND * cn, BAND), BAND)
    vec_copies = (
        remote(gvec.at[other_half], vec_rx.at[0], v_send.at[0], v_recv.at[0], fsdp=f_c),
        remote(vec_a, vec_rx.at[1], v_send.at[1], v_recv.at[1], fsdp=f_x),
        remote(vec_b, vec_rx.at[PAIR], v_send.at[PAIR], v_recv.at[PAIR], fsdp=f_y),
        remote(vec_c, vec_full.at[own_half], v_send.at[3], v_recv.at[3], fsdp=f_c),
    )

    for copy in small_copies:
        copy.wait()

    def vec_step(n):
        if n > 0:
            vec_copies[n - 1].wait_recv()
        if n == 1:
            vec_a[...] = gvec[own_half] + vec_rx[0]
        elif n == PAIR:
            vec_b[...] = vec_a[...] + vec_rx[1]
        elif n == 3:
            total = vec_b[...] + vec_rx[PAIR]
            vec_c[...] = total
            vec_full[own_half] = total
        if n < GROUP:
            vec_copies[n].start()

    vec_step(0)

    rs[...] = jnp.zeros((ROWS, LANES), F32)
    vco[...] = jnp.zeros((LANES, LANES), F32)
    table[...] = jnp.zeros((LANES, LANES), F32)
    vd_pad[...] = jnp.zeros((LAYERS, 256), F32)
    vd_pad[:, 0:192] = vr_d[...]
    for k in range(PAIR):
        rows = slice(BAND * k, BAND * k + BAND)
        for t, (name, tile, width) in enumerate(COLUMN_TILES):
            ref = {"u": vc_u, "q": vc_q, "o": vc_o, "d": vc_d}[name]
            row = HALF * k + BAND * t
            vco[row : row + BAND, 0:width] = ref[rows, LANES * tile : LANES * tile + width]
        for s, ref in enumerate((vr_u, vr_q, vr_o)):
            table[HALF * k + BAND * s : HALF * k + BAND * s + BAND, 0:ROWS] = ref[rows, :]
        tiles = (vd_pad[rows, 0:LANES], vd_pad[rows, LANES:256])
        for b in range(GROUP):
            table[HALF * k + 24 + BAND * b : HALF * k + 32 + BAND * b, :] = shifted(tiles, ROWS * b, ROWS)
    rv[...] = jnp.transpose(table[...])[0:ROWS, :]

    def pack_up(k, half, slot):
        def body(h, carry):
            q, core = h // PAIR, h % PAIR
            rows = pl.ds(pl.multiple_of(ROWS * h, BAND), ROWS)
            for i in range(PAIR):
                for t in range(3):
                    lanes = slice(LANES * t, LANES * t + LANES)
                    cs[slot, q // PAIR, q % PAIR, 3 * i + t, core] = (
                        own_u[PAIR * half + i, rows, lanes] + rr_u[k, PAIR * half + i, rows, lanes]
                    )
            return carry

        lax.fori_loop(0, BAND, body, 0)

    def pack_flat(own, other, slot, first, count, unit):
        def body(n, carry):
            rows = pl.ds(pl.multiple_of(LANES * (first + n), LANES), LANES)
            for block in range(3):
                lanes = slice(LANES * block, LANES * block + LANES)
                value = jnp.transpose(own[rows, lanes] + other[rows, lanes])
                for h, row, here, size in row_parts(block):
                    cs[slot, h // GROUP, (h // PAIR) % PAIR, unit + n, h % PAIR, row : row + size, :] = value[here : here + size]
            return carry

        lax.fori_loop(0, count, body, 0)

    def pack_down(k, slot):
        def body(n, carry):
            q, t = n // 3, n % 3
            rows = pl.ds(pl.multiple_of(LANES * t, LANES), LANES)
            for block in range(3):
                lanes = pl.ds(pl.multiple_of(DIM * q + LANES * block, LANES), LANES)
                value = jnp.transpose(own_d[rows, lanes] + rr_d[k, rows, lanes])
                for h, row, here, size in row_parts(block):
                    core, b = h // GROUP, h % GROUP
                    cs[slot + b // PAIR, q // PAIR, q % PAIR, 3 * (b % PAIR) + t, core, row : row + size, :] = value[
                        here : here + size
                    ]
            return carry

        lax.fori_loop(0, 12, body, 0)

    def prepare(p):
        k, n, slot = p // UNITS, p % UNITS, p % SLOTS
        needs = {0: (0,), 1: (1,), PAIR: (PAIR,), 3: (3,), GROUP: (GROUP,), SOURCES: ()}[n]
        for source_index in needs:
            own_copy(k, source_index).wait()
            core_copy(k, source_index).wait_recv()
        if p >= SLOTS and n != SOURCES:
            for copy in s1_copies(p - SLOTS):
                copy.wait_send()
            if n == GROUP:
                for copy in s1_copies(p + 1 - SLOTS):
                    copy.wait_send()
        if n < PAIR:
            pack_up(k, n, slot)
        elif n == PAIR:
            pack_flat(own_q, rr_q.at[k], slot, 0, UNITS, 0)
        elif n == 3:
            pack_flat(own_q, rr_q.at[k], slot, UNITS, 3, 0)
            pack_flat(own_o, rr_o.at[k], slot, 0, 3, 3)
        elif n == GROUP:
            pack_down(k, slot)
        for copy in s1_copies(p):
            copy.start()
        if n == 0 and k == 0:
            core_copy(0, PAIR).start()
            core_copy(0, 3).start()
        elif n == 1 and k == 0:
            core_copy(0, GROUP).start()
        if k == 0:
            reload = {0: (0,), 1: (1,), 3: (PAIR, 3), GROUP: (GROUP,)}.get(n, ())
            for source_index in reload:
                own_copy(1, source_index).start()
            for source_index in {PAIR: (0,), 3: (1,), GROUP: (PAIR, 3), SOURCES: (GROUP,)}.get(n, ()):
                core_copy(1, source_index).start()

    def stage_two(p):
        slot = p % SLOTS
        for copy in s1_copies(p):
            copy.wait_recv()

        def body(u, carry):
            for core in range(PAIR):
                rxa[p, yn, u, core] = rxa[p, yn, u, core] + cs[slot, yn, x, u, core]
                ryb[p, xn, u, core] = ryb[p, xn, u, core] + cs[slot, y, xn, 3 + u, core]
            return carry

        lax.fori_loop(0, 3, body, 0)
        for copy in s2_copies(p):
            copy.start()

    def stage_three(p):
        slot = p % SLOTS
        for copy in s2_copies(p):
            copy.wait_recv()

        def body(u, carry):
            fs[p, u] = cs[slot, y, x, u, cn] + rxa[p, y, u, cn] + r2a[p, u, cn]
            fs[p, 3 + u] = cs[slot, y, x, 3 + u, cn] + ryb[p, x, u, cn] + r2b[p, u, cn]
            return carry

        lax.fori_loop(0, 3, body, 0)
        final_copy(p).start()

        def body_own(u, carry):
            ff[c, p, u] = cs[slot, y, x, u, c] + rxa[p, y, u, c] + r2a[p, u, c]
            ff[c, p, 3 + u] = cs[slot, y, x, 3 + u, c] + ryb[p, x, u, c] + r2b[p, u, c]
            return carry

        lax.fori_loop(0, 3, body_own, 0)

    def keep(layer, tile, value, first=True):
        ut[layer, tile] = value
        square = value * value
        row = pl.ds(HALF * (layer // BAND) + BAND * TILE_COL[tile] + layer % BAND, 1)
        sums = jnp.sum(square, axis=0, keepdims=True)
        cr[f, row, :] = sums if first else cr[f, row, :] + sums
        return square

    def keep_rows(layer, slot, square):
        lane = HALF * (layer // BAND) + BAND * slot + layer % BAND
        sums = jnp.sum(square, axis=1, keepdims=True)
        rs[...] = jnp.where(lane_iota((ROWS, LANES)) == lane, sums, rs[...])

    def finish_up(k):
        def body(i8, carry):
            core, i = i8 // GROUP, i8 % GROUP
            layer = BAND * k + i8
            square = [keep(layer, t, ff[core, UNITS * k + i // PAIR, 3 * (i % PAIR) + t]) for t in range(3)]
            keep_rows(layer, 0, square[0] + square[1] + square[PAIR])
            return carry

        lax.fori_loop(0, BAND, body, 0)

    def finish_qkv(k):
        def body(core, carry):
            tiles = [ff.at[core, UNITS * k + PAIR + t // UNITS, t % UNITS] for t in range(12)]
            for i in range(GROUP):
                layer = BAND * k + GROUP * core + i
                first = PAIR * i
                part = [tiles[t][...] for t in range(first, min(first + GROUP, 9))]
                square = [
                    keep(layer, 3 + t, shifted(part, 32 * i + LANES * t, LANES if t < PAIR else 32)) for t in range(3)
                ]
                keep_rows(layer, 1, square[0] + square[1] + square[PAIR])
                part = [tiles[9 + t][...] for t in range(3)]
                keep_rows(layer, PAIR, keep(layer, UNITS, shifted(part, CHIP * i, CHIP)))
            return carry

        lax.fori_loop(0, PAIR, body, 0)

    def finish_down(k, half):
        def body(core, carry):
            for b in (PAIR * half, PAIR * half + 1):
                part = [ff[core, UNITS * k + GROUP + half, 3 * (b % PAIR) + t] for t in range(3)]
                for i in range(GROUP):
                    layer = BAND * k + GROUP * core + i
                    keep_rows(layer, 3 + b, keep(layer, 7 + b, shifted(part, CHIP * i, CHIP), first=b == 0))
            return carry

        lax.fori_loop(0, PAIR, body, 0)

    def column_rows(k, n):
        start, size = ((0, 24), (24, 32), (56, BAND))[n]
        return slice(HALF * k + start, HALF * k + start + size)

    def send_columns(k, n):
        rows = column_rows(k, n)

        def body(d, carry):
            remote(
                cr.at[f, rows], cr.at[f, rows], c_send.at[3 * k + n], c_recv.at[3 * k + n], fsdp=(f + d) % BAND
            ).start()
            return carry

        lax.fori_loop(1, BAND, body, 0)

    def finish(p):
        k, n = p // UNITS, p % UNITS
        final_copy(p).wait_recv()
        if n == 1:
            finish_up(k)
            send_columns(k, 0)
        elif n == 3:
            finish_qkv(k)
            send_columns(k, 1)
        elif n == GROUP:
            finish_down(k, 0)
        elif n == SOURCES:
            finish_down(k, 1)
            send_columns(k, PAIR)

    for step in range(PIECES + 3):
        for lag, part in enumerate((prepare, stage_two, stage_three, finish)):
            if 0 <= step - lag < PIECES:
                with jax.named_scope(f"{part.__name__}_{step - lag}"):
                    part(step - lag)
        if step in (1, 3, SOURCES, 7):
            vec_step((step + 1) // PAIR)

    rrx[z] = rs[...]

    def send_rows(d, carry):
        remote(rrx.at[z], rrx.at[z], r_sem.at[0], r_sem.at[1], tp=(z + d) % tp_size).start()
        return carry

    lax.fori_loop(1, tp_size, send_rows, 0)

    def exchange(ref, sems):
        def body(d, carry):
            other = (me + d) % devices
            remote(ref.at[me], ref.at[me], sems.at[0], sems.at[1], tp=other // BAND, fsdp=other % BAND).start()
            return carry

        lax.fori_loop(1, devices, body, 0)
        wait_bytes(ref.at[0 : devices - 1], sems.at[1])

    vec_sum = vec_full[...]
    vec_square = vec_sum * vec_sum
    vec_total = jnp.sum(jnp.sum(vec_square, axis=1, keepdims=True), axis=0, keepdims=True)
    trx[me, :, 0:LANES] = jnp.sum(rs[...], axis=0, keepdims=True)
    trx[me, :, LANES:256] = jnp.sum(rv[...], axis=0, keepdims=True)
    trx[me, :, 256:DIM] = jnp.broadcast_to(vec_total, (1, LANES))
    exchange(trx, t_sem)
    totals = jnp.sum(trx[...], axis=0)
    square_sum = totals[:, 0:LANES]
    old_sum = totals[:, LANES:256] * (1.0 / tp_size)
    vec_part = totals[:, 256:257] * 0.125
    total = jnp.sum(square_sum, axis=1, keepdims=True) + vec_part
    clip = jnp.minimum(1.0, 1.0 / jnp.sqrt(total))

    def clipped(value):
        return jnp.where(clip > 0.0, clip * (clip * value), 0.0)

    slot = (lane_iota((1, LANES)) // BAND) % BAND
    row_inv = jnp.where(slot >= 3, 1.0 / 1536.0, 1.0 / 384.0).astype(F32)
    col_inv = jnp.where(
        slot == 0, 1.0 / (384.0 * tp_size), jnp.where(slot == 1, 1.0 / (288.0 * tp_size), 1.0 / (96.0 * tp_size))
    ).astype(F32)
    mean_new = BETA_TWO * (sum_down(old_sum) * row_inv) + (1.0 - BETA_TWO) * (
        clipped(sum_down(square_sum)) * (row_inv * col_inv) + EPSILON
    )
    wait_bytes(rrx.at[0 : tp_size - 1], r_sem.at[1])
    row_new = BETA_TWO * rv[...] + (1.0 - BETA_TWO) * (clipped(jnp.sum(rrx[...], axis=0)) * col_inv + EPSILON)
    rv[...] = clip * lax.rsqrt(row_new / mean_new)
    table[0:ROWS, :] = row_new
    vr_new[...] = jnp.transpose(table[...])

    for k in range(PAIR):
        for n in range(3):
            rows = column_rows(k, n)
            wait_bytes(cr.at[0:7, rows], c_recv.at[3 * k + n])
    col_sum = cr[0]
    for other in range(1, BAND):
        col_sum = col_sum + cr[other]
    down_row = (lax.broadcasted_iota(jnp.int32, (LANES, LANES), 0) // BAND) % BAND == 7
    col_new = BETA_TWO * vco[...] + (1.0 - BETA_TWO) * (
        clipped(col_sum) * jnp.where(down_row, 1.0 / 1536.0, 1.0 / 384.0).astype(F32) + EPSILON
    )
    vc_new[...] = col_new
    vco[...] = lax.rsqrt(col_new)

    vec_grad = vec_sum * clip
    vec_var = BETA_TWO * v_old[...] + (1.0 - BETA_TWO) * (vec_grad * vec_grad + EPSILON)
    v_new[...] = vec_var
    vec_update = vec_grad / jnp.sqrt(vec_var)
    u_vec[...] = vec_update
    vec_rows = jnp.sum(vec_update * vec_update, axis=1, keepdims=True) * (0.125 / 128.0)
    vec_rows = jnp.broadcast_to(vec_rows, (LAYERS, LANES))
    table[56:HALF, :] = vec_rows[0:BAND]
    table[120:LANES, :] = vec_rows[BAND:LAYERS]

    def update(layer, carry):
        index = HALF * (layer // BAND) + layer % BAND
        lane = lane_iota((ROWS, LANES))
        factors = rv[...]
        tile = 0
        for s in range(7):
            row = jnp.sum(jnp.where(lane == index + BAND * s, factors, 0.0), axis=1, keepdims=True)
            square = None
            while tile < 11 and TILE_SLOT[tile] == s:
                value = ut[layer, tile] * row * vco[pl.ds(index + BAND * TILE_COL[tile], 1), :]
                ut[layer, tile] = value
                square = value * value if square is None else square + value * value
                tile += 1
            table[pl.ds(index + BAND * s, 1), :] = jnp.sum(square, axis=0, keepdims=True)
        return carry

    lax.fori_loop(0, LAYERS, update, 0)

    t2rx[me] = jnp.sum(jnp.transpose(table[...]), axis=0, keepdims=True)
    exchange(t2rx, t_sem.at[PAIR:GROUP])
    update_sum = sum_down(jnp.sum(t2rx[...], axis=0))
    inverse = jnp.where(slot == 7, 1.0 / (1248.0 * tp_size), row_inv * col_inv).astype(F32)
    factor = 1.0 / jnp.maximum(1.0, jnp.sqrt(update_sum * inverse))
    scale[...] = jnp.transpose(jnp.broadcast_to(factor, (LANES, LANES)))

    for k in range(PAIR):
        for n in range(SOURCES):
            core_copy(k, n).wait_send()
        for n in range(3):
            wait_bytes(cr.at[0:7, column_rows(k, n)], c_send.at[3 * k + n])
    for p in range(PIECES):
        if p >= PIECES - SLOTS:
            for copy in s1_copies(p):
                copy.wait_send()
        for copy in s2_copies(p):
            copy.wait_send()
        final_copy(p).wait_send()
    for copy in vec_copies:
        copy.wait_send()
    wait_bytes(rrx.at[0 : tp_size - 1], r_sem.at[0])
    wait_bytes(trx.at[0 : devices - 1], t_sem.at[0])
    wait_bytes(t2rx.at[0 : devices - 1], t_sem.at[PAIR])


def update_kernel(ut, vr_new, vc_new, scale, u_vec, v_new, w_q, w_o, w_u, w_d, w_v, m_q, m_o, m_u, m_d, m_v, *refs):
    outs, refs = refs[:OUTS], refs[OUTS:]
    buffers, sems = refs[:OUTS], refs[OUTS]
    wo_q, wo_o, wo_u, wo_d, wo_v, mo_q, mo_o, mo_u, mo_d, mo_v, *rest = buffers
    vr_q, vc_q, vr_o, vc_o, vr_u, vc_u, vr_d, vc_d, v_out = rest
    by_layer = [n for n in range(OUTS) if len(outs[n].shape) == 3]
    copies = [pltpu.make_async_copy(buffers[n], outs[n], sems.at[n]) for n in range(OUTS)]

    def finish(update, weight, moment):
        moment_new = (MOMENTUM * moment.astype(F32) + (1.0 - MOMENTUM) * update).astype(jnp.bfloat16)
        return weight - LEARN_RATE * (moment_new.astype(F32) + WEIGHT_DECAY * weight), moment_new

    v_out[...] = v_new[...]
    for k in range(PAIR):
        rows = slice(BAND * k, BAND * k + BAND)
        for t in range(10):
            lanes = slice(LANES * t, min(LANES * t + LANES, VEC))
            factor = scale[HALF * k + 56 : HALF * k + HALF, 0 : lanes.stop - lanes.start]
            weight_new, moment_new = finish(u_vec[rows, lanes] * factor, w_v[rows, lanes], m_v[rows, lanes])
            wo_v[rows, lanes] = weight_new
            mo_v[rows, lanes] = moment_new
        for t, (name, tile, width) in enumerate(COLUMN_TILES):
            ref = {"u": vc_u, "q": vc_q, "o": vc_o, "d": vc_d}[name]
            row = HALF * k + BAND * t
            ref[rows, LANES * tile : LANES * tile + width] = vc_new[row : row + BAND, 0:width]
        for s, ref in enumerate((vr_u, vr_q, vr_o)):
            row = HALF * k + BAND * s
            ref[rows, :] = vr_new[row : row + BAND, 0:ROWS]
        b0, b1, b2, b3 = (vr_new[HALF * k + BAND * (3 + b) : HALF * k + BAND * (GROUP + b), :] for b in range(GROUP))
        lane = lane_iota((BAND, LANES))
        b2 = pltpu.roll(b2, CHIP, 1)
        vr_d[rows, 0:LANES] = jnp.where(lane < ROWS, b0, jnp.where(lane < CHIP, pltpu.roll(b1, ROWS, 1), b2))
        vr_d[rows, LANES:192] = jnp.where(lane < LAYERS, b2, pltpu.roll(b3, LAYERS, 1))[:, 0:HALF]
    for n in range(OUTS):
        if n not in by_layer:
            copies[n].start()

    def body(layer, carry):
        index = HALF * (layer // BAND) + layer % BAND

        def one(tile, slot, w, m, wo, mo, rows, lanes):
            factor = scale[pl.ds(index + BAND * slot, 1), :]
            update = (ut[layer, tile] * factor)[:, 0 : lanes.stop - lanes.start]
            weight_new, moment_new = finish(update, w[layer, rows, lanes], m[layer, rows, lanes])
            wo[layer, rows, lanes] = weight_new
            mo[layer, rows, lanes] = moment_new

        every = slice(0, ROWS)
        for t in range(3):
            one(t, 0, w_u, m_u, wo_u, mo_u, every, slice(LANES * t, LANES * t + LANES))
            one(3 + t, 1, w_q, m_q, wo_q, mo_q, every, slice(LANES * t, min(LANES * t + LANES, 288)))
        one(UNITS, PAIR, w_o, m_o, wo_o, mo_o, every, slice(0, CHIP))
        for b in range(GROUP):
            one(7 + b, 3, w_d, m_d, wo_d, mo_d, slice(ROWS * b, ROWS * b + ROWS), slice(0, CHIP))
        for n in by_layer:
            pltpu.make_async_copy(buffers[n].at[layer], outs[n].at[layer], sems.at[n]).start()
        return carry

    lax.fori_loop(0, LAYERS, body, 0)
    for copy in copies:
        copy.wait()


def solution(mesh):
    tp_size = mesh.shape["tp"]
    devices = tp_size * mesh.shape["fsdp"]
    vmem = pl.BlockSpec(memory_space=pltpu.VMEM)
    hbm = pl.BlockSpec(memory_space=pltpu.HBM)

    def local_step(g_qkv, g_out, g_up, g_down, g_vec, w_qkv, w_out, w_up, w_down, w_vec, m_qkv, m_out, m_up, m_down, m_vec, vr_qkv, vc_qkv, vr_out, vc_out, vr_up, vc_up, vr_down, vc_down, v_vec):
        def flat(g):
            g = jnp.swapaxes(g[0], 1, PAIR)
            return g.reshape(g.shape[0] * g.shape[1], g.shape[PAIR])

        dma = pltpu.SemaphoreType.DMA
        half = (BAND, VEC)
        small = (g_vec[0], vr_qkv, vc_qkv, vr_out, vc_out, vr_up, vc_up, vr_down, vc_down, v_vec)
        sums = pl.pallas_call(
            functools.partial(reduce_kernel, tp_size),
            out_shape=[
                jax.ShapeDtypeStruct((LAYERS, 11, ROWS, LANES), F32),
                jax.ShapeDtypeStruct((LANES, LANES), F32),
                jax.ShapeDtypeStruct((LANES, LANES), F32),
                jax.ShapeDtypeStruct((LANES, LANES), F32),
                jax.ShapeDtypeStruct((LAYERS, VEC), F32),
                jax.ShapeDtypeStruct((LAYERS, VEC), F32),
            ],
            in_specs=[hbm] * (GROUP + SMALL),
            out_specs=[vmem] * UNITS,
            scratch_shapes=[pltpu.VMEM(a.shape, a.dtype) for a in small]
            + [
                pltpu.VMEM((GROUP, DIM, DIM), F32),
                pltpu.VMEM((1152, DIM), F32),
                pltpu.VMEM((DIM, DIM), F32),
                pltpu.VMEM((DIM, 1536), F32),
                pltpu.VMEM((PAIR, GROUP, DIM, DIM), F32),
                pltpu.VMEM((PAIR, 1152, DIM), F32),
                pltpu.VMEM((PAIR, DIM, DIM), F32),
                pltpu.VMEM((PAIR, DIM, 1536), F32),
                pltpu.VMEM((SLOTS, PAIR, PAIR, UNITS, PAIR, ROWS, LANES), F32),
                pltpu.VMEM((PIECES, PAIR, 3, PAIR, ROWS, LANES), F32),
                pltpu.VMEM((PIECES, PAIR, 3, PAIR, ROWS, LANES), F32),
                pltpu.VMEM((PIECES, 3, PAIR, ROWS, LANES), F32),
                pltpu.VMEM((PIECES, 3, PAIR, ROWS, LANES), F32),
                pltpu.VMEM((PAIR, PIECES, UNITS, ROWS, LANES), F32),
                pltpu.VMEM((PIECES, UNITS, ROWS, LANES), F32),
                pltpu.VMEM((BAND, LANES, LANES), F32),
                pltpu.VMEM((ROWS, LANES), F32),
                pltpu.VMEM((tp_size, ROWS, LANES), F32),
                pltpu.VMEM((ROWS, LANES), F32),
                pltpu.VMEM((LANES, LANES), F32),
                pltpu.VMEM((devices, 1, DIM), F32),
                pltpu.VMEM((devices, 1, LANES), F32),
                pltpu.VMEM((LANES, LANES), F32),
                pltpu.VMEM((LAYERS, 256), F32),
                pltpu.VMEM(half, F32),
                pltpu.VMEM(half, F32),
                pltpu.VMEM(half, F32),
                pltpu.VMEM((3,) + half, F32),
                pltpu.VMEM((LAYERS, VEC), F32),
                dma((SMALL,)), dma((SOURCES,)),
                dma((10,)), dma((10,)),
                dma((PAIR * PIECES,)), dma((PAIR * PIECES,)),
                dma((PAIR * PIECES,)), dma((PAIR * PIECES,)),
                dma((PIECES,)), dma((PIECES,)),
                dma((UNITS,)), dma((UNITS,)),
                dma((PAIR,)), dma((GROUP,)),
                dma((GROUP,)), dma((GROUP,)),
            ],
            compiler_params=pltpu.CompilerParams(
                collective_id=0, has_side_effects=True, vmem_limit_bytes=46 * 1024 * 1024
            ),
            name="reduce",
        )(*[pltpu.with_memory_space_constraint(a, pltpu.HBM) for a in (flat(g_qkv), flat(g_out), g_up[0], flat(g_down)) + small])

        weights = (w_qkv, w_out, w_up, w_down, w_vec)
        moments = (m_qkv, m_out, m_up, m_down, m_vec)
        outs = weights + moments + small[1:]
        return tuple(
            pl.pallas_call(
                update_kernel,
                out_shape=[jax.ShapeDtypeStruct(a.shape, a.dtype) for a in outs],
                in_specs=[vmem] * (len(sums) + len(weights) + len(moments)),
                out_specs=[hbm] * OUTS,
                scratch_shapes=[pltpu.VMEM(a.shape, a.dtype) for a in outs] + [dma((OUTS,))],
                compiler_params=pltpu.CompilerParams(vmem_limit_bytes=24 * 1024 * 1024),
                name="update",
            )(*sums, *weights, *moments)
        )

    grad_spec = P("fsdp", None, None, "tp")
    vec_grad_spec = P("fsdp", None, "tp")
    mat_spec = P(None, "fsdp", "tp")
    vec_spec = P(None, "tp")
    row_spec = P(None, "fsdp")
    state_specs = (mat_spec,) * GROUP + (vec_spec,) + (mat_spec,) * GROUP + (vec_spec,) + (row_spec, vec_spec) * GROUP + (vec_spec,)
    arg_specs = (grad_spec,) * GROUP + (vec_grad_spec,) + state_specs
    return jax.shard_map(local_step, mesh=mesh, in_specs=arg_specs, out_specs=state_specs, check_vma=False)
```

```python
import functools

import jax
import jax.numpy as jnp
from jax import lax
from jax.experimental import pallas as pl
from jax.experimental.pallas import tpu as pltpu
from jax.sharding import PartitionSpec as P

TRAIN_STEP = 3
LEARN_RATE = 0.0008
WEIGHT_DECAY = 0.03
MOMENTUM = 0.9
EPSILON = 1e-30
BETA_TWO = 1.0 - TRAIN_STEP ** -0.8

MESH = pl.DeviceIdType.MESH
F32 = jnp.float32
LAYERS = 16
PAIR = 2
GROUP = 4
OUTS = 19
SMALL = 10
SOURCES = 5
UNITS = 6
BAND = 8
ROWS = 48
HALF = 64
CHIP = 96
LANES = 128
DIM = 384
VEC = 1248
PIECES = 12
IN_FLIGHT = 4
SLOTS = 6
TILE_SLOT = (0, 0, 0, 1, 1, 1, 2, 3, 4, 5, 6)
COLUMN_TILES = (
    ("u", 0, LANES), ("u", 1, LANES), ("u", PAIR, LANES),
    ("q", 0, LANES), ("q", 1, LANES), ("q", PAIR, 32), ("o", 0, CHIP), ("d", 0, CHIP),
)
TILE_COL = (0, 1, 2, 3, 4, 5, 6, 7, 7, 7, 7)


def row_parts(block):
    parts, row = [], LANES * block
    while row < LANES * block + LANES:
        stop = min((row // ROWS + 1) * ROWS, LANES * block + LANES)
        parts.append((row // ROWS, row % ROWS, row - LANES * block, stop - row))
        row = stop
    return parts


def lane_iota(shape):
    return lax.broadcasted_iota(jnp.int32, shape, len(shape) - 1)


def shifted(tiles, start, width):
    base, shift = start // LANES, start % LANES
    value = tiles[base] if shift == 0 else pltpu.roll(tiles[base], LANES - shift, 1)
    lane = lane_iota(value.shape)
    if shift + width > LANES:
        value = jnp.where(lane < LANES - shift, value, pltpu.roll(tiles[base + 1], LANES - shift, 1))
    return value if width == LANES else jnp.where(lane < width, value, 0.0)


def sum_down(value):
    slot = (lane_iota(value.shape) // BAND) % BAND
    part = jnp.where((slot >= 3) & (slot <= UNITS), value, 0.0)
    total = part + pltpu.roll(part, BAND, 1) + pltpu.roll(part, LAYERS, 1) + pltpu.roll(part, 24, 1)
    total = jnp.where(slot == UNITS, total, 0.0)
    total = total + pltpu.roll(total, 120, 1) + pltpu.roll(total, 112, 1) + pltpu.roll(total, 104, 1)
    return jnp.where((slot >= 3) & (slot <= UNITS), total, value)


def reduce_kernel(tp_size, gq, go, gu, gd, *refs):
    small_hbm, refs = refs[:SMALL], refs[SMALL:]
    ut, vr_new, vc_new, scale, u_vec, v_new, *refs = refs
    small, refs = refs[:SMALL], refs[SMALL:]
    gvec, vr_q, vc_q, vr_o, vc_o, vr_u, vc_u, vr_d, vc_d, v_old = small
    own_u, own_q, own_o, own_d, rr_u, rr_q, rr_o, rr_d, cs, rxa, ryb, r2a, r2b, ff, fs, *refs = refs
    ck, cg, co, cd, rs, rrx, rv, vco, trx, t2rx, table, vd_pad, vec_a, vec_b, vec_c, vec_rx, vec_full, *refs = refs
    own_sem, d_send, d_recv, s1_send, s1_recv, s2_send, s2_recv, f_send, f_recv, *refs = refs
    c_send, c_recv, r_sem, t_sem, v_send, v_recv, hello_sem = refs
    f = lax.axis_index("fsdp")
    z = lax.axis_index("tp")
    c, x, y = f % PAIR, (f // PAIR) % PAIR, f // GROUP
    xn, yn, cn = 1 - x, 1 - y, 1 - c
    f_c, f_x, f_y = f + 1 - PAIR * c, f + PAIR - GROUP * x, f + GROUP - BAND * y
    me = z * BAND + f
    flip_f = [
        f + (j % PAIR) * (1 - PAIR * c) + (j // PAIR % PAIR) * (PAIR - GROUP * x) + j // GROUP * (GROUP - BAND * y)
        for j in range(BAND)
    ]
    flip_z = [z, z + 1 - PAIR * (z % PAIR), z + PAIR - GROUP * (z // PAIR), tp_size - 1 - z][:tp_size]
    z_near = (z - 1 + (tp_size - 1 - z) // (tp_size - 1), z + 1 - z // (tp_size - 1))
    far_first = sorted(
        range(1, tp_size * BAND), key=lambda m: -(m // BAND + m // GROUP % PAIR + m // PAIR % PAIR)
    )
    devices = tp_size * BAND

    def remote(src, dst, send, recv, **device):
        return pltpu.make_async_remote_copy(
            src_ref=src, dst_ref=dst, send_sem=send, recv_sem=recv, device_id=device, device_id_type=MESH
        )

    def wait_bytes(ref, sem):
        pltpu.make_async_copy(ref, ref, sem).wait()

    def source(k, n, group):
        if n < PAIR:
            return gu.at[pl.ds(GROUP * group + PAIR * n, PAIR)], own_u.at[PAIR * n : PAIR * n + PAIR], rr_u.at[k, PAIR * n : PAIR * n + PAIR]
        if n == PAIR:
            return gq.at[pl.ds(pl.multiple_of(1152 * group, BAND), 1152)], own_q, rr_q.at[k]
        if n == 3:
            return go.at[pl.ds(pl.multiple_of(DIM * group, BAND), DIM)], own_o, rr_o.at[k]
        return gd.at[pl.ds(pl.multiple_of(DIM * group, BAND), DIM)], own_d, rr_d.at[k]

    def own_copy(k, n):
        src, dst, _ = source(k, n, PAIR * k + c)
        return pltpu.make_async_copy(src, dst, own_sem.at[n])

    def core_copy(k, n):
        src, _, dst = source(k, n, PAIR * k + cn)
        return remote(src, dst, d_send.at[n], d_recv.at[n], fsdp=f_c)

    def s1_copies(p):
        slot, sem = p % SLOTS, PAIR * (p % IN_FLIGHT)
        return (
            remote(cs.at[slot, :, xn, 0:3], rxa.at[p], s1_send.at[sem], s1_recv.at[sem], fsdp=f_x),
            remote(cs.at[slot, yn, :, 3:UNITS], ryb.at[p], s1_send.at[sem + 1], s1_recv.at[sem + 1], fsdp=f_y),
        )

    def s2_copies(p):
        sem = PAIR * (p % IN_FLIGHT)
        return (
            remote(rxa.at[p, yn], r2a.at[p], s2_send.at[sem], s2_recv.at[sem], fsdp=f_y),
            remote(ryb.at[p, xn], r2b.at[p], s2_send.at[sem + 1], s2_recv.at[sem + 1], fsdp=f_x),
        )

    def final_copy(p):
        return remote(fs.at[p], ff.at[c, p], f_send.at[p % IN_FLIGHT], f_recv.at[p % IN_FLIGHT], fsdp=f_c)

    for n in range(SOURCES):
        own_copy(0, n).start()
    idle_sems = [s2_send.at[n] for n in range(BAND)] + [f_send.at[n] for n in range(PAIR)]
    small_copies = [pltpu.make_async_copy(small_hbm[n], small[n], idle_sems[n]) for n in range(SMALL)]
    for copy in small_copies:
        copy.start()

    barrier = pltpu.get_barrier_semaphore()

    def signal_near(sem):
        for other in z_near:
            pl.semaphore_signal(sem, inc=1, device_id={"tp": other}, device_id_type=MESH)

    for other in (f_c, f_x, f_y):
        pl.semaphore_signal(barrier, inc=1, device_id={"fsdp": other}, device_id_type=MESH)
    signal_near(barrier)
    pl.semaphore_wait(barrier, SOURCES)

    for n in range(PAIR):
        core_copy(0, n).start()

    own_half = pl.ds(pl.multiple_of(BAND * c, BAND), BAND)
    other_half = pl.ds(pl.multiple_of(BAND * cn, BAND), BAND)
    vec_copies = (
        remote(gvec.at[other_half], vec_rx.at[0], v_send.at[0], v_recv.at[0], fsdp=f_c),
        remote(vec_a, vec_rx.at[1], v_send.at[0], v_recv.at[1], fsdp=f_x),
        remote(vec_b, vec_rx.at[PAIR], v_send.at[0], v_recv.at[PAIR], fsdp=f_y),
        remote(vec_c, vec_full.at[own_half], v_send.at[0], v_recv.at[3], fsdp=f_c),
    )

    for copy in small_copies:
        copy.wait()

    def vec_step(n):
        if n > 0:
            vec_copies[n - 1].wait_recv()
            vec_copies[n - 1].wait_send()
        if n == 1:
            vec_a[...] = gvec[own_half] + vec_rx[0]
        elif n == PAIR:
            vec_b[...] = vec_a[...] + vec_rx[1]
        elif n == 3:
            total = vec_b[...] + vec_rx[PAIR]
            vec_c[...] = total
            vec_full[own_half] = total
        if n < GROUP:
            vec_copies[n].start()

    vec_step(0)

    rs[...] = jnp.zeros((ROWS, LANES), F32)
    ck[1, 7] = jnp.zeros((BAND, LANES), F32)
    vco[...] = jnp.zeros((LANES, LANES), F32)
    table[...] = jnp.zeros((LANES, LANES), F32)
    vd_pad[...] = jnp.zeros((LAYERS, 256), F32)
    vd_pad[:, 0:192] = vr_d[...]
    for k in range(PAIR):
        rows = slice(BAND * k, BAND * k + BAND)
        for t, (name, tile, width) in enumerate(COLUMN_TILES):
            ref = {"u": vc_u, "q": vc_q, "o": vc_o, "d": vc_d}[name]
            row = HALF * k + BAND * t
            vco[row : row + BAND, 0:width] = ref[rows, LANES * tile : LANES * tile + width]
        for s, ref in enumerate((vr_u, vr_q, vr_o)):
            table[HALF * k + BAND * s : HALF * k + BAND * s + BAND, 0:ROWS] = ref[rows, :]
        tiles = (vd_pad[rows, 0:LANES], vd_pad[rows, LANES:256])
        for b in range(GROUP):
            table[HALF * k + 24 + BAND * b : HALF * k + 32 + BAND * b, :] = shifted(tiles, ROWS * b, ROWS)
    rv[...] = jnp.transpose(table[...])[0:ROWS, :]

    def pack_up(k, half, slot):
        def body(h, carry):
            q, core = h // PAIR, h % PAIR
            rows = pl.ds(pl.multiple_of(ROWS * h, BAND), ROWS)
            for i in range(PAIR):
                for t in range(3):
                    lanes = slice(LANES * t, LANES * t + LANES)
                    cs[slot, q // PAIR, q % PAIR, 3 * i + t, core] = (
                        own_u[PAIR * half + i, rows, lanes] + rr_u[k, PAIR * half + i, rows, lanes]
                    )
            return carry

        lax.fori_loop(0, BAND, body, 0)

    def pack_flat(own, other, slot, first, count, unit):
        def body(n, carry):
            rows = pl.ds(pl.multiple_of(LANES * (first + n), LANES), LANES)
            for block in range(3):
                lanes = slice(LANES * block, LANES * block + LANES)
                value = jnp.transpose(own[rows, lanes] + other[rows, lanes])
                for h, row, here, size in row_parts(block):
                    cs[slot, h // GROUP, (h // PAIR) % PAIR, unit + n, h % PAIR, row : row + size, :] = value[here : here + size]
            return carry

        lax.fori_loop(0, count, body, 0)

    def pack_down(k, slot):
        def body(n, carry):
            q, t = n // 3, n % 3
            rows = pl.ds(pl.multiple_of(LANES * t, LANES), LANES)
            for block in range(3):
                lanes = pl.ds(pl.multiple_of(DIM * q + LANES * block, LANES), LANES)
                value = jnp.transpose(own_d[rows, lanes] + rr_d[k, rows, lanes])
                for h, row, here, size in row_parts(block):
                    core, b = h // GROUP, h % GROUP
                    cs[slot + b // PAIR, q // PAIR, q % PAIR, 3 * (b % PAIR) + t, core, row : row + size, :] = value[
                        here : here + size
                    ]
            return carry

        lax.fori_loop(0, 12, body, 0)

    def prepare(p):
        k, n, slot = p // UNITS, p % UNITS, p % SLOTS
        needs = {0: (0,), 1: (1,), PAIR: (PAIR,), 3: (3,), GROUP: (GROUP,), SOURCES: ()}[n]
        for source_index in needs:
            own_copy(k, source_index).wait()
            core_copy(k, source_index).wait_recv()
        if p >= IN_FLIGHT:
            for copy in s1_copies(p - IN_FLIGHT):
                copy.wait_send()
        if n < PAIR:
            pack_up(k, n, slot)
        elif n == PAIR:
            pack_flat(own_q, rr_q.at[k], slot, 0, UNITS, 0)
        elif n == 3:
            pack_flat(own_q, rr_q.at[k], slot, UNITS, 3, 0)
            pack_flat(own_o, rr_o.at[k], slot, 0, 3, 3)
        elif n == GROUP:
            pack_down(k, slot)
        for copy in s1_copies(p):
            copy.start()
        if n == 0 and k == 0:
            core_copy(0, PAIR).start()
            core_copy(0, 3).start()
        elif n == 1 and k == 0:
            core_copy(0, GROUP).start()
        if k == 0:
            reload = {0: (0,), 1: (1,), 3: (PAIR, 3), GROUP: (GROUP,)}.get(n, ())
            for source_index in reload:
                own_copy(1, source_index).start()
        for source_index in {GROUP: (0, 1), SOURCES: (PAIR, 3), UNITS: (GROUP,)}.get(p, ()):
            core_copy(0, source_index).wait_send()
            core_copy(1, source_index).start()

    def stage_two(p):
        slot = p % SLOTS
        for copy in s1_copies(p):
            copy.wait_recv()

        def body(u, carry):
            for core in range(PAIR):
                rxa[p, yn, u, core] = rxa[p, yn, u, core] + cs[slot, yn, x, u, core]
                ryb[p, xn, u, core] = ryb[p, xn, u, core] + cs[slot, y, xn, 3 + u, core]
            return carry

        lax.fori_loop(0, 3, body, 0)
        if p >= IN_FLIGHT:
            for copy in s2_copies(p - IN_FLIGHT):
                copy.wait_send()
        for copy in s2_copies(p):
            copy.start()

    def stage_three(p):
        slot = p % SLOTS
        for copy in s2_copies(p):
            copy.wait_recv()

        def body(u, carry):
            fs[p, u] = cs[slot, y, x, u, cn] + rxa[p, y, u, cn] + r2a[p, u, cn]
            fs[p, 3 + u] = cs[slot, y, x, 3 + u, cn] + ryb[p, x, u, cn] + r2b[p, u, cn]
            return carry

        if p >= IN_FLIGHT:
            final_copy(p - IN_FLIGHT).wait_send()
        lax.fori_loop(0, 3, body, 0)
        final_copy(p).start()

        def body_own(u, carry):
            ff[c, p, u] = cs[slot, y, x, u, c] + rxa[p, y, u, c] + r2a[p, u, c]
            ff[c, p, 3 + u] = cs[slot, y, x, 3 + u, c] + ryb[p, x, u, c] + r2b[p, u, c]
            return carry

        lax.fori_loop(0, 3, body_own, 0)
        if p % UNITS >= GROUP:
            finish_down(p // UNITS, p % PAIR, c)

    def keep(step_k, layer, tile, value, first=True):
        ut[layer, tile] = value
        square = value * value
        sums = jnp.sum(square, axis=0, keepdims=True)
        row = pl.ds(layer % BAND, 1)
        column = TILE_COL[tile]
        ref = cd.at[f] if step_k == 1 and column == 7 else ck.at[step_k, column]
        ref[row, :] = sums if first else ref[row, :] + sums
        return square

    def keep_rows(layer, slot, square):
        lane = HALF * (layer // BAND) + BAND * slot + layer % BAND
        sums = jnp.sum(square, axis=1, keepdims=True)
        rs[...] = jnp.where(lane_iota((ROWS, LANES)) == lane, sums, rs[...])

    def finish_up(k):
        def body(i8, carry):
            core, i = i8 // GROUP, i8 % GROUP
            layer = BAND * k + i8
            square = [keep(k, layer, t, ff[core, UNITS * k + i // PAIR, 3 * (i % PAIR) + t]) for t in range(3)]
            keep_rows(layer, 0, square[0] + square[1] + square[PAIR])
            return carry

        lax.fori_loop(0, BAND, body, 0)

    def finish_qkv(k):
        def body(core, carry):
            tiles = [ff.at[core, UNITS * k + PAIR + t // UNITS, t % UNITS] for t in range(12)]
            for i in range(GROUP):
                layer = BAND * k + GROUP * core + i
                first = PAIR * i
                part = [tiles[t][...] for t in range(first, min(first + GROUP, 9))]
                square = [
                    keep(k, layer, 3 + t, shifted(part, 32 * i + LANES * t, LANES if t < PAIR else 32)) for t in range(3)
                ]
                keep_rows(layer, 1, square[0] + square[1] + square[PAIR])
                part = [tiles[9 + t][...] for t in range(3)]
                keep_rows(layer, PAIR, keep(k, layer, UNITS, shifted(part, CHIP * i, CHIP)))
            return carry

        lax.fori_loop(0, PAIR, body, 0)

    def finish_down(k, half, core):
        for b in (PAIR * half, PAIR * half + 1):
            part = [ff[core, UNITS * k + GROUP + half, 3 * (b % PAIR) + t] for t in range(3)]
            for i in range(GROUP):
                layer = BAND * k + GROUP * core + i
                keep_rows(layer, 3 + b, keep(k, layer, 7 + b, shifted(part, CHIP * i, CHIP), first=b == 0))

    def columns_to_owner(k):
        for other in flip_f[:0:-1]:
            remote(ck.at[k, other], cg.at[k, f], c_send.at[PAIR * k], c_recv.at[PAIR * k], fsdp=other).start()
        cg[k, f] = ck[k, f]

    def columns_to_all(k):
        sem = PAIR * k + 1
        wait_bytes(cg.at[k, 0:7], c_recv.at[PAIR * k])
        total = cg[k, 0]
        for other in range(1, BAND):
            total = total + cg[k, other]
        co[k, f] = total
        for other in flip_f[:0:-1]:
            remote(co.at[k, f], co.at[k, f], c_send.at[sem], c_recv.at[sem], fsdp=other).start()

    def last_columns():
        for other in flip_f[:0:-1]:
            remote(cd.at[f], cd.at[f], c_send.at[GROUP], c_recv.at[GROUP], fsdp=other).start()

    def finish(p):
        k, n = p // UNITS, p % UNITS
        final_copy(p).wait_recv()
        if n == 1:
            finish_up(k)
        elif n == 3:
            finish_qkv(k)
            if k == 1:
                columns_to_owner(k)
        elif n >= GROUP:
            finish_down(k, n % PAIR, cn)
            if n == SOURCES:
                columns_to_owner(k) if k == 0 else last_columns()

    for step in range(PIECES + 3):
        for lag, part in ((0, prepare), (1, stage_two), (3, finish), (PAIR, stage_three)):
            if 0 <= step - lag < PIECES:
                with jax.named_scope(f"{part.__name__}_{step - lag}"):
                    part(step - lag)
        if step in (1, 3, SOURCES, 7):
            vec_step((step + 1) // PAIR)
        if step in (PAIR, GROUP):
            signal_near(hello_sem.at[step // GROUP])
        if step in (3, SOURCES):
            pl.semaphore_wait(hello_sem.at[step // SOURCES], PAIR)
        if step == 10:
            columns_to_all(0)

    def send_all(ref, sems):
        for m in far_first:
            device = {"tp": flip_z[m // BAND], "fsdp": flip_f[m % BAND]}
            remote(ref.at[me], ref.at[me], sems.at[0], sems.at[1], **device).start()

    vec_sum = vec_full[...]
    vec_square = vec_sum * vec_sum
    vec_total = jnp.sum(jnp.sum(vec_square, axis=1, keepdims=True), axis=0, keepdims=True)
    trx[me, :, 0:LANES] = jnp.sum(rs[...], axis=0, keepdims=True)
    trx[me, :, LANES:256] = jnp.sum(rv[...], axis=0, keepdims=True)
    trx[me, :, 256:DIM] = jnp.broadcast_to(vec_total, (1, LANES))
    send_all(trx, t_sem)
    rrx[z] = rs[...]
    for other in flip_z[:0:-1]:
        remote(rrx.at[z], rrx.at[z], r_sem.at[0], r_sem.at[1], tp=other).start()
    columns_to_all(1)
    wait_bytes(trx.at[0 : devices - 1], t_sem.at[1])
    totals = jnp.sum(trx[...], axis=0)
    square_sum = totals[:, 0:LANES]
    old_sum = totals[:, LANES:256] * (1.0 / tp_size)
    vec_part = totals[:, 256:257] * 0.125
    total = jnp.sum(square_sum, axis=1, keepdims=True) + vec_part
    clip = jnp.minimum(1.0, 1.0 / jnp.sqrt(total))

    def clipped(value):
        return jnp.where(clip > 0.0, clip * (clip * value), 0.0)

    slot = (lane_iota((1, LANES)) // BAND) % BAND
    row_inv = jnp.where(slot >= 3, 1.0 / 1536.0, 1.0 / 384.0).astype(F32)
    col_inv = jnp.where(
        slot == 0, 1.0 / (384.0 * tp_size), jnp.where(slot == 1, 1.0 / (288.0 * tp_size), 1.0 / (96.0 * tp_size))
    ).astype(F32)
    mean_new = BETA_TWO * (sum_down(old_sum) * row_inv) + (1.0 - BETA_TWO) * (
        clipped(sum_down(square_sum)) * (row_inv * col_inv) + EPSILON
    )
    wait_bytes(rrx.at[0 : tp_size - 1], r_sem.at[1])
    row_new = BETA_TWO * rv[...] + (1.0 - BETA_TWO) * (clipped(jnp.sum(rrx[...], axis=0)) * col_inv + EPSILON)
    rv[...] = clip * lax.rsqrt(row_new / mean_new)
    table[0:ROWS, :] = row_new
    vr_new[...] = jnp.transpose(table[...])

    for k in range(PAIR):
        wait_bytes(co.at[k, 0:7], c_recv.at[PAIR * k + 1])
    wait_bytes(cd.at[0:7], c_recv.at[GROUP])
    last_sum = cd[0]
    for other in range(1, BAND):
        last_sum = last_sum + cd[other]
    wait_bytes(cd.at[0:7], c_send.at[3])
    co[1, 7] = last_sum
    col_sum = co[...].reshape(LANES, LANES)
    down_row = (lax.broadcasted_iota(jnp.int32, (LANES, LANES), 0) // BAND) % BAND == 7
    col_new = BETA_TWO * vco[...] + (1.0 - BETA_TWO) * (
        clipped(col_sum) * jnp.where(down_row, 1.0 / 1536.0, 1.0 / 384.0).astype(F32) + EPSILON
    )
    vc_new[...] = col_new
    vco[...] = lax.rsqrt(col_new)

    vec_grad = vec_sum * clip
    vec_var = BETA_TWO * v_old[...] + (1.0 - BETA_TWO) * (vec_grad * vec_grad + EPSILON)
    v_new[...] = vec_var
    vec_update = vec_grad / jnp.sqrt(vec_var)
    u_vec[...] = vec_update
    vec_rows = jnp.sum(vec_update * vec_update, axis=1, keepdims=True) * (0.125 / 128.0)
    vec_rows = jnp.broadcast_to(vec_rows, (LAYERS, LANES))
    table[56:HALF, :] = vec_rows[0:BAND]
    table[120:LANES, :] = vec_rows[BAND:LAYERS]

    def update(layer, carry):
        index = HALF * (layer // BAND) + layer % BAND
        lane = lane_iota((ROWS, LANES))
        factors = rv[...]
        tile = 0
        for s in range(7):
            row = jnp.sum(jnp.where(lane == index + BAND * s, factors, 0.0), axis=1, keepdims=True)
            square = None
            while tile < 11 and TILE_SLOT[tile] == s:
                value = ut[layer, tile] * row * vco[pl.ds(index + BAND * TILE_COL[tile], 1), :]
                ut[layer, tile] = value
                square = value * value if square is None else square + value * value
                tile += 1
            table[pl.ds(index + BAND * s, 1), :] = jnp.sum(square, axis=0, keepdims=True)
        return carry

    lax.fori_loop(0, LAYERS, update, 0, unroll=PAIR)

    t2rx[me] = jnp.sum(jnp.transpose(table[...]), axis=0, keepdims=True)
    send_all(t2rx, t_sem.at[PAIR:GROUP])
    wait_bytes(t2rx.at[0 : devices - 1], t_sem.at[3])
    update_sum = sum_down(jnp.sum(t2rx[...], axis=0))
    inverse = jnp.where(slot == 7, 1.0 / (1248.0 * tp_size), row_inv * col_inv).astype(F32)
    factor = 1.0 / jnp.maximum(1.0, jnp.sqrt(update_sum * inverse))
    scale[...] = jnp.transpose(jnp.broadcast_to(factor, (LANES, LANES)))

    for n in range(SOURCES):
        core_copy(1, n).wait_send()
    for n in (0, 1, PAIR, GROUP):
        wait_bytes(cd.at[0:7], c_send.at[n])
    for p in range(PIECES - IN_FLIGHT, PIECES):
        for copy in s1_copies(p) + s2_copies(p):
            copy.wait_send()
        final_copy(p).wait_send()
    wait_bytes(rrx.at[0 : tp_size - 1], r_sem.at[0])
    wait_bytes(trx.at[0 : devices - 1], t_sem.at[0])
    wait_bytes(t2rx.at[0 : devices - 1], t_sem.at[PAIR])


def update_kernel(ut, vr_new, vc_new, scale, u_vec, v_new, w_q, w_o, w_u, w_d, w_v, m_q, m_o, m_u, m_d, m_v, *refs):
    outs, refs = refs[:OUTS], refs[OUTS:]
    buffers, sems = refs[:OUTS], refs[OUTS]
    wo_q, wo_o, wo_u, wo_d, wo_v, mo_q, mo_o, mo_u, mo_d, mo_v, *rest = buffers
    vr_q, vc_q, vr_o, vc_o, vr_u, vc_u, vr_d, vc_d, v_out = rest
    by_layer = [n for n in range(OUTS) if len(outs[n].shape) == 3]
    copies = [pltpu.make_async_copy(buffers[n], outs[n], sems.at[n]) for n in range(OUTS)]

    def finish(update, weight, moment):
        moment_new = (MOMENTUM * moment.astype(F32) + (1.0 - MOMENTUM) * update).astype(jnp.bfloat16)
        return weight - LEARN_RATE * (moment_new.astype(F32) + WEIGHT_DECAY * weight), moment_new

    v_out[...] = v_new[...]
    for k in range(PAIR):
        rows = slice(BAND * k, BAND * k + BAND)
        for t in range(10):
            lanes = slice(LANES * t, min(LANES * t + LANES, VEC))
            factor = scale[HALF * k + 56 : HALF * k + HALF, 0 : lanes.stop - lanes.start]
            weight_new, moment_new = finish(u_vec[rows, lanes] * factor, w_v[rows, lanes], m_v[rows, lanes])
            wo_v[rows, lanes] = weight_new
            mo_v[rows, lanes] = moment_new
        for t, (name, tile, width) in enumerate(COLUMN_TILES):
            ref = {"u": vc_u, "q": vc_q, "o": vc_o, "d": vc_d}[name]
            row = HALF * k + BAND * t
            ref[rows, LANES * tile : LANES * tile + width] = vc_new[row : row + BAND, 0:width]
        for s, ref in enumerate((vr_u, vr_q, vr_o)):
            row = HALF * k + BAND * s
            ref[rows, :] = vr_new[row : row + BAND, 0:ROWS]
        b0, b1, b2, b3 = (vr_new[HALF * k + BAND * (3 + b) : HALF * k + BAND * (GROUP + b), :] for b in range(GROUP))
        lane = lane_iota((BAND, LANES))
        b2 = pltpu.roll(b2, CHIP, 1)
        vr_d[rows, 0:LANES] = jnp.where(lane < ROWS, b0, jnp.where(lane < CHIP, pltpu.roll(b1, ROWS, 1), b2))
        vr_d[rows, LANES:192] = jnp.where(lane < LAYERS, b2, pltpu.roll(b3, LAYERS, 1))[:, 0:HALF]
    for n in range(OUTS):
        if n not in by_layer:
            copies[n].start()

    def body(layer, carry):
        index = HALF * (layer // BAND) + layer % BAND

        def one(tile, slot, w, m, wo, mo, rows, lanes):
            factor = scale[pl.ds(index + BAND * slot, 1), :]
            update = (ut[layer, tile] * factor)[:, 0 : lanes.stop - lanes.start]
            weight_new, moment_new = finish(update, w[layer, rows, lanes], m[layer, rows, lanes])
            wo[layer, rows, lanes] = weight_new
            mo[layer, rows, lanes] = moment_new

        every = slice(0, ROWS)
        for t in range(3):
            one(t, 0, w_u, m_u, wo_u, mo_u, every, slice(LANES * t, LANES * t + LANES))
            one(3 + t, 1, w_q, m_q, wo_q, mo_q, every, slice(LANES * t, min(LANES * t + LANES, 288)))
        one(UNITS, PAIR, w_o, m_o, wo_o, mo_o, every, slice(0, CHIP))
        for b in range(GROUP):
            one(7 + b, 3, w_d, m_d, wo_d, mo_d, slice(ROWS * b, ROWS * b + ROWS), slice(0, CHIP))
        for n in by_layer:
            pltpu.make_async_copy(buffers[n].at[layer], outs[n].at[layer], sems.at[n]).start()
        return carry

    lax.fori_loop(0, LAYERS, body, 0, unroll=PAIR)
    for copy in copies:
        copy.wait()


def solution(mesh):
    tp_size = mesh.shape["tp"]
    devices = tp_size * mesh.shape["fsdp"]
    vmem = pl.BlockSpec(memory_space=pltpu.VMEM)
    hbm = pl.BlockSpec(memory_space=pltpu.HBM)

    def local_step(g_qkv, g_out, g_up, g_down, g_vec, w_qkv, w_out, w_up, w_down, w_vec, m_qkv, m_out, m_up, m_down, m_vec, vr_qkv, vc_qkv, vr_out, vc_out, vr_up, vc_up, vr_down, vc_down, v_vec):
        def flat(g):
            g = jnp.swapaxes(g[0], 1, PAIR)
            return g.reshape(g.shape[0] * g.shape[1], g.shape[PAIR])

        dma = pltpu.SemaphoreType.DMA
        half = (BAND, VEC)
        small = (g_vec[0], vr_qkv, vc_qkv, vr_out, vc_out, vr_up, vc_up, vr_down, vc_down, v_vec)
        sums = pl.pallas_call(
            functools.partial(reduce_kernel, tp_size),
            out_shape=[
                jax.ShapeDtypeStruct((LAYERS, 11, ROWS, LANES), F32),
                jax.ShapeDtypeStruct((LANES, LANES), F32),
                jax.ShapeDtypeStruct((LANES, LANES), F32),
                jax.ShapeDtypeStruct((LANES, LANES), F32),
                jax.ShapeDtypeStruct((LAYERS, VEC), F32),
                jax.ShapeDtypeStruct((LAYERS, VEC), F32),
            ],
            in_specs=[hbm] * (GROUP + SMALL),
            out_specs=[vmem] * UNITS,
            scratch_shapes=[pltpu.VMEM(a.shape, a.dtype) for a in small]
            + [
                pltpu.VMEM((GROUP, DIM, DIM), F32),
                pltpu.VMEM((1152, DIM), F32),
                pltpu.VMEM((DIM, DIM), F32),
                pltpu.VMEM((DIM, 1536), F32),
                pltpu.VMEM((PAIR, GROUP, DIM, DIM), F32),
                pltpu.VMEM((PAIR, 1152, DIM), F32),
                pltpu.VMEM((PAIR, DIM, DIM), F32),
                pltpu.VMEM((PAIR, DIM, 1536), F32),
                pltpu.VMEM((SLOTS, PAIR, PAIR, UNITS, PAIR, ROWS, LANES), F32),
                pltpu.VMEM((PIECES, PAIR, 3, PAIR, ROWS, LANES), F32),
                pltpu.VMEM((PIECES, PAIR, 3, PAIR, ROWS, LANES), F32),
                pltpu.VMEM((PIECES, 3, PAIR, ROWS, LANES), F32),
                pltpu.VMEM((PIECES, 3, PAIR, ROWS, LANES), F32),
                pltpu.VMEM((PAIR, PIECES, UNITS, ROWS, LANES), F32),
                pltpu.VMEM((PIECES, UNITS, ROWS, LANES), F32),
                pltpu.VMEM((PAIR, BAND, BAND, LANES), F32),
                pltpu.VMEM((PAIR, BAND, BAND, LANES), F32),
                pltpu.VMEM((PAIR, BAND, BAND, LANES), F32),
                pltpu.VMEM((BAND, BAND, LANES), F32),
                pltpu.VMEM((ROWS, LANES), F32),
                pltpu.VMEM((tp_size, ROWS, LANES), F32),
                pltpu.VMEM((ROWS, LANES), F32),
                pltpu.VMEM((LANES, LANES), F32),
                pltpu.VMEM((devices, 1, DIM), F32),
                pltpu.VMEM((devices, 1, LANES), F32),
                pltpu.VMEM((LANES, LANES), F32),
                pltpu.VMEM((LAYERS, 256), F32),
                pltpu.VMEM(half, F32),
                pltpu.VMEM(half, F32),
                pltpu.VMEM(half, F32),
                pltpu.VMEM((3,) + half, F32),
                pltpu.VMEM((LAYERS, VEC), F32),
                dma((SOURCES,)),
                dma((SOURCES,)), dma((SOURCES,)),
                dma((PAIR * IN_FLIGHT,)), dma((PAIR * IN_FLIGHT,)),
                dma((PAIR * IN_FLIGHT,)), dma((PAIR * IN_FLIGHT,)),
                dma((IN_FLIGHT,)), dma((IN_FLIGHT,)),
                dma((SOURCES,)), dma((SOURCES,)),
                dma((PAIR,)), dma((GROUP,)),
                dma((1,)), dma((GROUP,)),
                pltpu.SemaphoreType.REGULAR((PAIR,)),
            ],
            compiler_params=pltpu.CompilerParams(
                collective_id=0, has_side_effects=True, vmem_limit_bytes=46 * 1024 * 1024
            ),
            name="reduce",
        )(*[pltpu.with_memory_space_constraint(a, pltpu.HBM) for a in (flat(g_qkv), flat(g_out), g_up[0], flat(g_down)) + small])

        weights = (w_qkv, w_out, w_up, w_down, w_vec)
        moments = (m_qkv, m_out, m_up, m_down, m_vec)
        outs = weights + moments + small[1:]
        return tuple(
            pl.pallas_call(
                update_kernel,
                out_shape=[jax.ShapeDtypeStruct(a.shape, a.dtype) for a in outs],
                in_specs=[vmem] * (len(sums) + len(weights) + len(moments)),
                out_specs=[hbm] * OUTS,
                scratch_shapes=[pltpu.VMEM(a.shape, a.dtype) for a in outs] + [dma((OUTS,))],
                compiler_params=pltpu.CompilerParams(vmem_limit_bytes=24 * 1024 * 1024),
                name="update",
            )(*sums, *weights, *moments)
        )

    grad_spec = P("fsdp", None, None, "tp")
    vec_grad_spec = P("fsdp", None, "tp")
    mat_spec = P(None, "fsdp", "tp")
    vec_spec = P(None, "tp")
    row_spec = P(None, "fsdp")
    state_specs = (mat_spec,) * GROUP + (vec_spec,) + (mat_spec,) * GROUP + (vec_spec,) + (row_spec, vec_spec) * GROUP + (vec_spec,)
    arg_specs = (grad_spec,) * GROUP + (vec_grad_spec,) + state_specs
    return jax.shard_map(local_step, mesh=mesh, in_specs=arg_specs, out_specs=state_specs, check_vma=False)
```

```python
import functools

import jax
import jax.numpy as jnp
from jax import lax
from jax.experimental import pallas as pl
from jax.experimental.pallas import tpu as pltpu
from jax.sharding import PartitionSpec as P

TRAIN_STEP = 3
LEARN_RATE = 0.0008
WEIGHT_DECAY = 0.03
MOMENTUM = 0.9
EPSILON = 1e-30
BETA_TWO = 1.0 - TRAIN_STEP ** -0.8

MESH = pl.DeviceIdType.MESH
F32 = jnp.float32
LAYERS = 16
TILES = 3
PAIR = 2
GROUP = 4
OUTS = 19
SMALL = 10
SOURCES = 5
UNITS = 6
BAND = 8
ROWS = 48
HALF = 64
CHIP = 96
LANES = 128
DIM = 384
VEC = 1248
PIECES = 12
IN_FLIGHT = 4
SLOTS = 6
TILE_SLOT = (0, 0, 0, 1, 1, 1, 2, 3, 4, 5, 6)
COLUMN_TILES = (
    ("u", 0, LANES), ("u", 1, LANES), ("u", PAIR, LANES),
    ("q", 0, LANES), ("q", 1, LANES), ("q", PAIR, 32), ("o", 0, CHIP), ("d", 0, CHIP),
)
TILE_COL = (0, 1, 2, 3, 4, 5, 6, 7, 7, 7, 7)


def row_parts(block):
    parts, row = [], LANES * block
    while row < LANES * block + LANES:
        stop = min((row // ROWS + 1) * ROWS, LANES * block + LANES)
        parts.append((row // ROWS, row % ROWS, row - LANES * block, stop - row))
        row = stop
    return parts


def lane_iota(shape):
    return lax.broadcasted_iota(jnp.int32, shape, len(shape) - 1)


def shifted(tiles, start, width):
    base, shift = start // LANES, start % LANES
    value = tiles[base] if shift == 0 else pltpu.roll(tiles[base], LANES - shift, 1)
    lane = lane_iota(value.shape)
    if shift + width > LANES:
        value = jnp.where(lane < LANES - shift, value, pltpu.roll(tiles[base + 1], LANES - shift, 1))
    return value if width == LANES else jnp.where(lane < width, value, 0.0)


def sum_down(value):
    slot = (lane_iota(value.shape) // BAND) % BAND
    part = jnp.where((slot >= TILES) & (slot <= UNITS), value, 0.0)
    total = part + pltpu.roll(part, BAND, 1) + pltpu.roll(part, LAYERS, 1) + pltpu.roll(part, 24, 1)
    total = jnp.where(slot == UNITS, total, 0.0)
    total = total + pltpu.roll(total, 120, 1) + pltpu.roll(total, 112, 1) + pltpu.roll(total, 104, 1)
    return jnp.where((slot >= TILES) & (slot <= UNITS), total, value)


def reduce_kernel(tp_size, gq, go, gu, gd, *refs):
    small_hbm, refs = refs[:SMALL], refs[SMALL:]
    ut, vr_new, vc_new, scale, u_vec, v_new, *refs = refs
    small, refs = refs[:SMALL], refs[SMALL:]
    gvec, vr_q, vc_q, vr_o, vc_o, vr_u, vc_u, vr_d, vc_d, v_old = small
    own_u, own_q, own_o, own_d, rr_u, rr_q, rr_o, rr_d, cs, rxa, ryb, r2a, r2b, ff, fs, *refs = refs
    ck, cg, co, cd, rs, rrx, rv, vco, trx, t2rx, table, vd_pad, vec_a, vec_b, vec_c, vec_rx, vec_full, *refs = refs
    own_sem, d_send, d_recv, s1_send, s1_recv, s2_send, s2_recv, f_send, f_recv, *refs = refs
    c_send, c_recv, r_sem, t_sem, v_send, v_recv, hello_sem = refs
    f = lax.axis_index("fsdp")
    z = lax.axis_index("tp")
    c, x, y = f % PAIR, (f // PAIR) % PAIR, f // GROUP
    xn, yn, cn = 1 - x, 1 - y, 1 - c
    f_c, f_x, f_y = f + 1 - PAIR * c, f + PAIR - GROUP * x, f + GROUP - BAND * y
    me = z * BAND + f
    flip_f = [
        f + (j % PAIR) * (1 - PAIR * c) + (j // PAIR % PAIR) * (PAIR - GROUP * x) + j // GROUP * (GROUP - BAND * y)
        for j in range(BAND)
    ]
    flip_z = [z, z + 1 - PAIR * (z % PAIR), z + PAIR - GROUP * (z // PAIR), tp_size - 1 - z][:tp_size]
    z_near = (z - 1 + (tp_size - 1 - z) // (tp_size - 1), z + 1 - z // (tp_size - 1))
    far_first = sorted(
        range(1, tp_size * BAND), key=lambda m: -(m // BAND + m // GROUP % PAIR + m // PAIR % PAIR)
    )
    devices = tp_size * BAND

    def remote(src, dst, send, recv, **device):
        return pltpu.make_async_remote_copy(
            src_ref=src, dst_ref=dst, send_sem=send, recv_sem=recv, device_id=device, device_id_type=MESH
        )

    def wait_bytes(ref, sem):
        pltpu.make_async_copy(ref, ref, sem).wait()

    def source(k, n, group):
        if n < PAIR:
            return gu.at[pl.ds(GROUP * group + PAIR * n, PAIR)], own_u.at[PAIR * n : PAIR * n + PAIR], rr_u.at[k, PAIR * n : PAIR * n + PAIR]
        if n == PAIR:
            return gq.at[pl.ds(pl.multiple_of(1152 * group, BAND), 1152)], own_q, rr_q.at[k]
        if n == TILES:
            return go.at[pl.ds(pl.multiple_of(DIM * group, BAND), DIM)], own_o, rr_o.at[k]
        return gd.at[pl.ds(pl.multiple_of(DIM * group, BAND), DIM)], own_d, rr_d.at[k]

    def own_copy(k, n):
        src, dst, _ = source(k, n, PAIR * k + c)
        return pltpu.make_async_copy(src, dst, own_sem.at[n])

    def core_copy(k, n):
        src, _, dst = source(k, n, PAIR * k + cn)
        return remote(src, dst, d_send.at[n], d_recv.at[n], fsdp=f_c)

    def s1_copies(p):
        slot, sem = p % SLOTS, PAIR * (p % IN_FLIGHT)
        return (
            remote(cs.at[slot, :, xn, 0:TILES], rxa.at[p], s1_send.at[sem], s1_recv.at[sem], fsdp=f_x),
            remote(cs.at[slot, yn, :, TILES:UNITS], ryb.at[p], s1_send.at[sem + 1], s1_recv.at[sem + 1], fsdp=f_y),
        )

    def s2_copies(p):
        sem = PAIR * (p % IN_FLIGHT)
        return (
            remote(rxa.at[p, yn], r2a.at[p], s2_send.at[sem], s2_recv.at[sem], fsdp=f_y),
            remote(ryb.at[p, xn], r2b.at[p], s2_send.at[sem + 1], s2_recv.at[sem + 1], fsdp=f_x),
        )

    def final_copy(p):
        return remote(fs.at[p], ff.at[c, p], f_send.at[p % IN_FLIGHT], f_recv.at[p % IN_FLIGHT], fsdp=f_c)

    for n in range(SOURCES):
        own_copy(0, n).start()
    idle_sems = [s2_send.at[n] for n in range(BAND)] + [f_send.at[n] for n in range(PAIR)]
    small_copies = [pltpu.make_async_copy(small_hbm[n], small[n], idle_sems[n]) for n in range(SMALL)]
    for copy in small_copies:
        copy.start()

    barrier = pltpu.get_barrier_semaphore()

    def signal_near(sem):
        for other in z_near:
            pl.semaphore_signal(sem, inc=1, device_id={"tp": other}, device_id_type=MESH)

    for other in (f_c, f_x, f_y):
        pl.semaphore_signal(barrier, inc=1, device_id={"fsdp": other}, device_id_type=MESH)
    signal_near(barrier)
    pl.semaphore_wait(barrier, SOURCES)

    def first_copies(xa, yb, sem):
        for layer, start, size in ((0, xa, CHIP), (0, PAIR + xa, CHIP), (1, PAIR * yb, PAIR * CHIP)):
            rows = pl.ds(pl.multiple_of(CHIP * start, BAND), size)
            remote(
                gu.at[GROUP * cn + layer, rows], rr_u.at[0, layer, rows], d_send.at[sem], d_recv.at[sem], fsdp=f_c
            ).start()

    first_copies(xn, yn, 0)
    first_copies(x, y, SOURCES)
    core_copy(0, 1).start()

    own_half = pl.ds(pl.multiple_of(BAND * c, BAND), BAND)
    other_half = pl.ds(pl.multiple_of(BAND * cn, BAND), BAND)
    vec_copies = (
        remote(gvec.at[other_half], vec_rx.at[0], v_send.at[0], v_recv.at[0], fsdp=f_c),
        remote(vec_a, vec_rx.at[1], v_send.at[0], v_recv.at[1], fsdp=f_x),
        remote(vec_b, vec_rx.at[PAIR], v_send.at[0], v_recv.at[PAIR], fsdp=f_y),
        remote(vec_c, vec_full.at[own_half], v_send.at[0], v_recv.at[TILES], fsdp=f_c),
    )

    for copy in small_copies:
        copy.wait()

    def vec_step(n):
        if n > 0:
            vec_copies[n - 1].wait_recv()
            vec_copies[n - 1].wait_send()
        if n == 1:
            vec_a[...] = gvec[own_half] + vec_rx[0]
        elif n == PAIR:
            vec_b[...] = vec_a[...] + vec_rx[1]
        elif n == TILES:
            total = vec_b[...] + vec_rx[PAIR]
            vec_c[...] = total
            vec_full[own_half] = total
        if n < GROUP:
            vec_copies[n].start()

    vec_step(0)

    rs[...] = jnp.zeros((ROWS, LANES), F32)
    ck[1, 7] = jnp.zeros((BAND, LANES), F32)
    vco[...] = jnp.zeros((LANES, LANES), F32)
    table[...] = jnp.zeros((LANES, LANES), F32)
    vd_pad[...] = jnp.zeros((LAYERS, 256), F32)
    vd_pad[:, 0:192] = vr_d[...]
    for k in range(PAIR):
        rows = slice(BAND * k, BAND * k + BAND)
        for t, (name, tile, width) in enumerate(COLUMN_TILES):
            ref = {"u": vc_u, "q": vc_q, "o": vc_o, "d": vc_d}[name]
            row = HALF * k + BAND * t
            vco[row : row + BAND, 0:width] = ref[rows, LANES * tile : LANES * tile + width]
        for s, ref in enumerate((vr_u, vr_q, vr_o)):
            table[HALF * k + BAND * s : HALF * k + BAND * s + BAND, 0:ROWS] = ref[rows, :]
        tiles = (vd_pad[rows, 0:LANES], vd_pad[rows, LANES:256])
        for b in range(GROUP):
            table[HALF * k + 24 + BAND * b : HALF * k + 32 + BAND * b, :] = shifted(tiles, ROWS * b, ROWS)
    rv[...] = jnp.transpose(table[...])[0:ROWS, :]

    def pack_up(k, half, slot):
        def body(h, carry):
            q, core = h // PAIR, h % PAIR
            rows = pl.ds(pl.multiple_of(ROWS * h, BAND), ROWS)
            for i in range(PAIR):
                for t in range(TILES):
                    lanes = slice(LANES * t, LANES * t + LANES)
                    cs[slot, q // PAIR, q % PAIR, TILES * i + t, core] = (
                        own_u[PAIR * half + i, rows, lanes] + rr_u[k, PAIR * half + i, rows, lanes]
                    )
            return carry

        lax.fori_loop(0, BAND, body, 0)

    def pack_flat(own, other, slot, first, count, unit):
        def body(n, carry):
            rows = pl.ds(pl.multiple_of(LANES * (first + n), LANES), LANES)
            for block in range(TILES):
                lanes = slice(LANES * block, LANES * block + LANES)
                value = jnp.transpose(own[rows, lanes] + other[rows, lanes])
                for h, row, here, size in row_parts(block):
                    cs[slot, h // GROUP, (h // PAIR) % PAIR, unit + n, h % PAIR, row : row + size, :] = value[here : here + size]
            return carry

        lax.fori_loop(0, count, body, 0)

    def pack_down(k, slot):
        def body(n, carry):
            q, t = n // TILES, n % TILES
            rows = pl.ds(pl.multiple_of(LANES * t, LANES), LANES)
            for block in range(TILES):
                lanes = pl.ds(pl.multiple_of(DIM * q + LANES * block, LANES), LANES)
                value = jnp.transpose(own_d[rows, lanes] + rr_d[k, rows, lanes])
                for h, row, here, size in row_parts(block):
                    core, b = h // GROUP, h % GROUP
                    cs[slot + b // PAIR, q // PAIR, q % PAIR, TILES * (b % PAIR) + t, core, row : row + size, :] = value[
                        here : here + size
                    ]
            return carry

        lax.fori_loop(0, 12, body, 0)

    def pack_first(xa, yb):
        def body(n, carry):
            part, core = n // PAIR, n % PAIR
            for i, q in ((0, PAIR * part + xa), (1, PAIR * yb + part)):
                rows = pl.ds(pl.multiple_of(CHIP * q + ROWS * core, BAND), ROWS)
                for t in range(TILES):
                    lanes = slice(LANES * t, LANES * t + LANES)
                    cs[0, q // PAIR, q % PAIR, TILES * i + t, core] = own_u[i, rows, lanes] + rr_u[0, i, rows, lanes]
            return carry

        lax.fori_loop(0, GROUP, body, 0)

    def prepare_first():
        own_copy(0, 0).wait()
        wait_bytes(rr_u.at[0, 0], d_recv.at[0])
        pack_first(xn, yn)
        for copy in s1_copies(0):
            copy.start()
        for n in (PAIR, TILES):
            core_copy(0, n).start()
        wait_bytes(rr_u.at[0, 0], d_recv.at[SOURCES])
        pack_first(x, y)
        own_copy(1, 0).start()

    def prepare(p):
        if p == 0:
            return prepare_first()
        k, n, slot = p // UNITS, p % UNITS, p % SLOTS
        needs = {0: (0,), 1: (1,), PAIR: (PAIR,), TILES: (TILES,), GROUP: (GROUP,), SOURCES: ()}[n]
        for source_index in needs:
            own_copy(k, source_index).wait()
            core_copy(k, source_index).wait_recv()
        if p >= IN_FLIGHT:
            for copy in s1_copies(p - IN_FLIGHT):
                copy.wait_send()
        if n < PAIR:
            pack_up(k, n, slot)
        elif n == PAIR:
            pack_flat(own_q, rr_q.at[k], slot, 0, UNITS, 0)
        elif n == TILES:
            pack_flat(own_q, rr_q.at[k], slot, UNITS, TILES, 0)
            pack_flat(own_o, rr_o.at[k], slot, 0, TILES, TILES)
        elif n == GROUP:
            pack_down(k, slot)
        for copy in s1_copies(p):
            copy.start()
        if p == 1:
            core_copy(0, GROUP).start()
        if k == 0:
            reload = {0: (0,), 1: (1,), TILES: (PAIR, TILES), GROUP: (GROUP,)}.get(n, ())
            for source_index in reload:
                own_copy(1, source_index).start()
        for source_index in {GROUP: (0, 1), SOURCES: (PAIR, TILES), UNITS: (GROUP,)}.get(p, ()):
            if source_index == 0:
                for sem in (0, SOURCES):
                    wait_bytes(rr_u.at[0, 0], d_send.at[sem])
            else:
                core_copy(0, source_index).wait_send()
            core_copy(1, source_index).start()

    def stage_two(p):
        slot = p % SLOTS
        for copy in s1_copies(p):
            copy.wait_recv()

        def body(u, carry):
            for core in range(PAIR):
                rxa[p, yn, u, core] = rxa[p, yn, u, core] + cs[slot, yn, x, u, core]
                ryb[p, xn, u, core] = ryb[p, xn, u, core] + cs[slot, y, xn, TILES + u, core]
            return carry

        lax.fori_loop(0, TILES, body, 0)
        if p >= IN_FLIGHT:
            for copy in s2_copies(p - IN_FLIGHT):
                copy.wait_send()
        for copy in s2_copies(p):
            copy.start()

    def stage_three(p):
        slot = p % SLOTS
        for copy in s2_copies(p):
            copy.wait_recv()

        def body(u, carry):
            fs[p, u] = cs[slot, y, x, u, cn] + rxa[p, y, u, cn] + r2a[p, u, cn]
            fs[p, TILES + u] = cs[slot, y, x, TILES + u, cn] + ryb[p, x, u, cn] + r2b[p, u, cn]
            return carry

        if p >= IN_FLIGHT:
            final_copy(p - IN_FLIGHT).wait_send()
        lax.fori_loop(0, TILES, body, 0)
        final_copy(p).start()

        def body_own(u, carry):
            ff[c, p, u] = cs[slot, y, x, u, c] + rxa[p, y, u, c] + r2a[p, u, c]
            ff[c, p, TILES + u] = cs[slot, y, x, TILES + u, c] + ryb[p, x, u, c] + r2b[p, u, c]
            return carry

        lax.fori_loop(0, TILES, body_own, 0)
        if p % UNITS >= GROUP:
            finish_down(p // UNITS, p % PAIR, c)

    def keep(step_k, layer, tile, value, first=True):
        ut[layer, tile] = value
        square = value * value
        sums = jnp.sum(square, axis=0, keepdims=True)
        row = pl.ds(layer % BAND, 1)
        column = TILE_COL[tile]
        ref = cd.at[f] if step_k == 1 and column == 7 else ck.at[step_k, column]
        ref[row, :] = sums if first else ref[row, :] + sums
        return square

    def keep_rows(layer, slot, square):
        lane = HALF * (layer // BAND) + BAND * slot + layer % BAND
        sums = jnp.sum(square, axis=1, keepdims=True)
        rs[...] = jnp.where(lane_iota((ROWS, LANES)) == lane, sums, rs[...])

    def finish_up(k):
        def body(i8, carry):
            core, i = i8 // GROUP, i8 % GROUP
            layer = BAND * k + i8
            square = [keep(k, layer, t, ff[core, UNITS * k + i // PAIR, TILES * (i % PAIR) + t]) for t in range(TILES)]
            keep_rows(layer, 0, square[0] + square[1] + square[PAIR])
            return carry

        lax.fori_loop(0, BAND, body, 0)

    def finish_qkv(k):
        def body(core, carry):
            tiles = [ff.at[core, UNITS * k + PAIR + t // UNITS, t % UNITS] for t in range(12)]
            for i in range(GROUP):
                layer = BAND * k + GROUP * core + i
                first = PAIR * i
                part = [tiles[t][...] for t in range(first, min(first + GROUP, 9))]
                square = [
                    keep(k, layer, TILES + t, shifted(part, 32 * i + LANES * t, LANES if t < PAIR else 32)) for t in range(TILES)
                ]
                keep_rows(layer, 1, square[0] + square[1] + square[PAIR])
                part = [tiles[9 + t][...] for t in range(TILES)]
                keep_rows(layer, PAIR, keep(k, layer, UNITS, shifted(part, CHIP * i, CHIP)))
            return carry

        lax.fori_loop(0, PAIR, body, 0)

    def finish_down(k, half, core):
        for b in (PAIR * half, PAIR * half + 1):
            part = [ff[core, UNITS * k + GROUP + half, TILES * (b % PAIR) + t] for t in range(TILES)]
            for i in range(GROUP):
                layer = BAND * k + GROUP * core + i
                keep_rows(layer, TILES + b, keep(k, layer, 7 + b, shifted(part, CHIP * i, CHIP), first=b == 0))

    def columns_to_owner(k):
        for other in flip_f[:0:-1]:
            remote(ck.at[k, other], cg.at[k, f], c_send.at[PAIR * k], c_recv.at[PAIR * k], fsdp=other).start()
        cg[k, f] = ck[k, f]

    def columns_to_all(k):
        sem = PAIR * k + 1
        wait_bytes(cg.at[k, 0:7], c_recv.at[PAIR * k])
        total = cg[k, 0]
        for other in range(1, BAND):
            total = total + cg[k, other]
        co[k, f] = total
        for other in flip_f[:0:-1]:
            remote(co.at[k, f], co.at[k, f], c_send.at[sem], c_recv.at[sem], fsdp=other).start()

    def last_columns():
        for other in flip_f[:0:-1]:
            remote(cd.at[f], cd.at[f], c_send.at[GROUP], c_recv.at[GROUP], fsdp=other).start()

    def finish(p):
        k, n = p // UNITS, p % UNITS
        final_copy(p).wait_recv()
        if n == 1:
            finish_up(k)
        elif n == TILES:
            finish_qkv(k)
            if k == 1:
                columns_to_owner(k)
        elif n >= GROUP:
            finish_down(k, n % PAIR, cn)
            if n == SOURCES:
                columns_to_owner(k) if k == 0 else last_columns()

    def send_all(ref, sems):
        for m in far_first:
            device = {"tp": flip_z[m // BAND], "fsdp": flip_f[m % BAND]}
            remote(ref.at[me], ref.at[me], sems.at[0], sems.at[1], **device).start()

    def prepare_totals():
        square = vec_full[...] * vec_full[...]
        vec_total = jnp.sum(jnp.sum(square, axis=1, keepdims=True), axis=0, keepdims=True)
        trx[me, :, LANES : PAIR * LANES] = jnp.sum(rv[...], axis=0, keepdims=True)
        trx[me, :, PAIR * LANES : TILES * LANES] = jnp.broadcast_to(vec_total, (1, LANES))

    def send_totals():
        lane = lane_iota((1, LANES))
        total = jnp.sum(rs[...], axis=0, keepdims=True)
        for i in range(GROUP):
            square = None
            for b in range(PAIR):
                value = shifted([fs[PIECES - 1, TILES * b + t] for t in range(TILES)], CHIP * i, CHIP)
                square = value * value if square is None else square + value * value
            sums = jnp.sum(jnp.sum(square, axis=0, keepdims=True), axis=1, keepdims=True)
            total = total + jnp.where(lane == HALF + BAND * TILES + GROUP * c + i, sums, 0.0)
        trx[me, :, 0:LANES] = total
        send_all(trx, t_sem)

    for step in range(PIECES + TILES):
        for lag, part in ((0, prepare), (1, stage_two), (TILES, finish), (PAIR, stage_three)):
            if 0 <= step - lag < PIECES:
                with jax.named_scope(f"{part.__name__}_{step - lag}"):
                    part(step - lag)
        if step in (1, TILES, SOURCES, 7):
            vec_step((step + 1) // PAIR)
        if step in (PAIR, GROUP):
            signal_near(hello_sem.at[step // GROUP])
        if step in (TILES, SOURCES):
            pl.semaphore_wait(hello_sem.at[step // SOURCES], PAIR)
        if step == 10:
            columns_to_all(0)
            prepare_totals()
        if step == PIECES + 1:
            send_totals()

    rrx[z] = rs[...]
    for other in flip_z[:0:-1]:
        remote(rrx.at[z], rrx.at[z], r_sem.at[0], r_sem.at[1], tp=other).start()
    columns_to_all(1)
    wait_bytes(trx.at[0 : devices - 1], t_sem.at[1])
    totals = jnp.sum(trx[...], axis=0)
    square_sum = totals[:, 0:LANES]
    old_sum = totals[:, LANES:256] * (1.0 / tp_size)
    vec_part = totals[:, 256:257] * 0.125
    total = jnp.sum(square_sum, axis=1, keepdims=True) + vec_part
    clip = jnp.minimum(1.0, 1.0 / jnp.sqrt(total))

    def clipped(value):
        return jnp.where(clip > 0.0, clip * (clip * value), 0.0)

    slot = (lane_iota((1, LANES)) // BAND) % BAND
    row_inv = jnp.where(slot >= TILES, 1.0 / 1536.0, 1.0 / 384.0).astype(F32)
    col_inv = jnp.where(
        slot == 0, 1.0 / (384.0 * tp_size), jnp.where(slot == 1, 1.0 / (288.0 * tp_size), 1.0 / (96.0 * tp_size))
    ).astype(F32)
    mean_new = BETA_TWO * (sum_down(old_sum) * row_inv) + (1.0 - BETA_TWO) * (
        clipped(sum_down(square_sum)) * (row_inv * col_inv) + EPSILON
    )
    wait_bytes(rrx.at[0 : tp_size - 1], r_sem.at[1])
    row_new = BETA_TWO * rv[...] + (1.0 - BETA_TWO) * (clipped(jnp.sum(rrx[...], axis=0)) * col_inv + EPSILON)
    rv[...] = clip * lax.rsqrt(row_new / mean_new)
    rs[...] = row_new

    for k in range(PAIR):
        wait_bytes(co.at[k, 0:7], c_recv.at[PAIR * k + 1])
    wait_bytes(cd.at[0:7], c_recv.at[GROUP])
    last_sum = cd[0]
    for other in range(1, BAND):
        last_sum = last_sum + cd[other]
    wait_bytes(cd.at[0:7], c_send.at[TILES])
    co[1, 7] = last_sum
    col_sum = co[...].reshape(LANES, LANES)
    down_row = (lax.broadcasted_iota(jnp.int32, (LANES, LANES), 0) // BAND) % BAND == 7
    col_new = BETA_TWO * vco[...] + (1.0 - BETA_TWO) * (
        clipped(col_sum) * jnp.where(down_row, 1.0 / 1536.0, 1.0 / 384.0).astype(F32) + EPSILON
    )
    vc_new[...] = col_new
    vco[...] = lax.rsqrt(col_new)

    vec_grad = vec_full[...] * clip
    vec_var = BETA_TWO * v_old[...] + (1.0 - BETA_TWO) * (vec_grad * vec_grad + EPSILON)
    v_new[...] = vec_var
    vec_update = vec_grad / jnp.sqrt(vec_var)
    u_vec[...] = vec_update
    vec_rows = jnp.sum(vec_update * vec_update, axis=1, keepdims=True) * (0.125 / 128.0)
    vec_rows = jnp.broadcast_to(vec_rows, (LAYERS, LANES))
    table[56:HALF, :] = vec_rows[0:BAND]
    table[120:LANES, :] = vec_rows[BAND:LAYERS]

    def update(layer, carry):
        index = HALF * (layer // BAND) + layer % BAND
        lane = lane_iota((ROWS, LANES))
        factors = rv[...]
        tile = 0
        for s in range(7):
            row = jnp.sum(jnp.where(lane == index + BAND * s, factors, 0.0), axis=1, keepdims=True)
            square = None
            while tile < 11 and TILE_SLOT[tile] == s:
                value = ut[layer, tile] * row * vco[pl.ds(index + BAND * TILE_COL[tile], 1), :]
                ut[layer, tile] = value
                square = value * value if square is None else square + value * value
                tile += 1
            table[pl.ds(index + BAND * s, 1), :] = jnp.sum(square, axis=0, keepdims=True)
        return carry

    lax.fori_loop(0, LAYERS, update, 0, unroll=PAIR)

    t2rx[me] = jnp.sum(jnp.transpose(table[...]), axis=0, keepdims=True)
    send_all(t2rx, t_sem.at[PAIR:GROUP])
    table[0:ROWS, :] = rs[...]
    vr_new[...] = jnp.transpose(table[...])
    wait_bytes(t2rx.at[0 : devices - 1], t_sem.at[TILES])
    update_sum = sum_down(jnp.sum(t2rx[...], axis=0))
    inverse = jnp.where(slot == 7, 1.0 / (1248.0 * tp_size), row_inv * col_inv).astype(F32)
    factor = (1.0 - MOMENTUM) / jnp.maximum(1.0, jnp.sqrt(update_sum * inverse))
    scale[...] = jnp.transpose(jnp.broadcast_to(factor, (LANES, LANES)))

    for n in range(SOURCES):
        core_copy(1, n).wait_send()
    for n in (0, 1, PAIR, GROUP):
        wait_bytes(cd.at[0:7], c_send.at[n])
    for p in range(PIECES - IN_FLIGHT, PIECES):
        for copy in s1_copies(p) + s2_copies(p):
            copy.wait_send()
        final_copy(p).wait_send()
    wait_bytes(rrx.at[0 : tp_size - 1], r_sem.at[0])
    wait_bytes(trx.at[0 : devices - 1], t_sem.at[0])
    wait_bytes(t2rx.at[0 : devices - 1], t_sem.at[PAIR])


def update_kernel(ut, vr_new, vc_new, scale, u_vec, v_new, w_q, w_o, w_u, w_d, w_v, m_q, m_o, m_u, m_d, m_v, *refs):
    outs, refs = refs[:OUTS], refs[OUTS:]
    buffers, sems = refs[:OUTS], refs[OUTS]
    wo_q, wo_o, wo_u, wo_d, wo_v, mo_q, mo_o, mo_u, mo_d, mo_v, *rest = buffers
    vr_q, vc_q, vr_o, vc_o, vr_u, vc_u, vr_d, vc_d, v_out = rest
    by_layer = [n for n in range(OUTS) if len(outs[n].shape) == TILES]
    copies = [pltpu.make_async_copy(buffers[n], outs[n], sems.at[n]) for n in range(OUTS)]

    def finish(update, weight, moment):
        moment_new = (MOMENTUM * moment.astype(F32) + update).astype(jnp.bfloat16)
        return (1.0 - LEARN_RATE * WEIGHT_DECAY) * weight - LEARN_RATE * moment_new.astype(F32), moment_new

    v_out[...] = v_new[...]
    for k in range(PAIR):
        rows = slice(BAND * k, BAND * k + BAND)
        for t in range(10):
            lanes = slice(LANES * t, min(LANES * t + LANES, VEC))
            factor = scale[HALF * k + 56 : HALF * k + HALF, 0 : lanes.stop - lanes.start]
            weight_new, moment_new = finish(u_vec[rows, lanes] * factor, w_v[rows, lanes], m_v[rows, lanes])
            wo_v[rows, lanes] = weight_new
            mo_v[rows, lanes] = moment_new
        for t, (name, tile, width) in enumerate(COLUMN_TILES):
            ref = {"u": vc_u, "q": vc_q, "o": vc_o, "d": vc_d}[name]
            row = HALF * k + BAND * t
            ref[rows, LANES * tile : LANES * tile + width] = vc_new[row : row + BAND, 0:width]
        for s, ref in enumerate((vr_u, vr_q, vr_o)):
            row = HALF * k + BAND * s
            ref[rows, :] = vr_new[row : row + BAND, 0:ROWS]
        b0, b1, b2, b3 = (vr_new[HALF * k + BAND * (TILES + b) : HALF * k + BAND * (GROUP + b), :] for b in range(GROUP))
        lane = lane_iota((BAND, LANES))
        b2 = pltpu.roll(b2, CHIP, 1)
        vr_d[rows, 0:LANES] = jnp.where(lane < ROWS, b0, jnp.where(lane < CHIP, pltpu.roll(b1, ROWS, 1), b2))
        vr_d[rows, LANES:192] = jnp.where(lane < LAYERS, b2, pltpu.roll(b3, LAYERS, 1))[:, 0:HALF]
    for n in range(OUTS):
        if n not in by_layer:
            copies[n].start()

    def body(layer, carry):
        index = HALF * (layer // BAND) + layer % BAND

        def one(tile, slot, w, m, wo, mo, rows, lanes):
            factor = scale[pl.ds(index + BAND * slot, 1), :]
            update = (ut[layer, tile] * factor)[:, 0 : lanes.stop - lanes.start]
            weight_new, moment_new = finish(update, w[layer, rows, lanes], m[layer, rows, lanes])
            wo[layer, rows, lanes] = weight_new
            mo[layer, rows, lanes] = moment_new

        every = slice(0, ROWS)
        for t in range(TILES):
            one(t, 0, w_u, m_u, wo_u, mo_u, every, slice(LANES * t, LANES * t + LANES))
            one(TILES + t, 1, w_q, m_q, wo_q, mo_q, every, slice(LANES * t, min(LANES * t + LANES, 288)))
        one(UNITS, PAIR, w_o, m_o, wo_o, mo_o, every, slice(0, CHIP))
        for b in range(GROUP):
            one(7 + b, TILES, w_d, m_d, wo_d, mo_d, slice(ROWS * b, ROWS * b + ROWS), slice(0, CHIP))
        for n in by_layer:
            pltpu.make_async_copy(buffers[n].at[layer], outs[n].at[layer], sems.at[n]).start()
        return carry

    lax.fori_loop(0, LAYERS, body, 0, unroll=PAIR)
    for copy in copies:
        copy.wait()


def solution(mesh):
    tp_size = mesh.shape["tp"]
    devices = tp_size * mesh.shape["fsdp"]
    vmem = pl.BlockSpec(memory_space=pltpu.VMEM)
    hbm = pl.BlockSpec(memory_space=pltpu.HBM)

    def local_step(g_qkv, g_out, g_up, g_down, g_vec, w_qkv, w_out, w_up, w_down, w_vec, m_qkv, m_out, m_up, m_down, m_vec, vr_qkv, vc_qkv, vr_out, vc_out, vr_up, vc_up, vr_down, vc_down, v_vec):
        def flat(g):
            g = jnp.swapaxes(g[0], 1, PAIR)
            return g.reshape(g.shape[0] * g.shape[1], g.shape[PAIR])

        dma = pltpu.SemaphoreType.DMA
        half = (BAND, VEC)
        small = (g_vec[0], vr_qkv, vc_qkv, vr_out, vc_out, vr_up, vc_up, vr_down, vc_down, v_vec)
        sums = pl.pallas_call(
            functools.partial(reduce_kernel, tp_size),
            out_shape=[
                jax.ShapeDtypeStruct((LAYERS, 11, ROWS, LANES), F32),
                jax.ShapeDtypeStruct((LANES, LANES), F32),
                jax.ShapeDtypeStruct((LANES, LANES), F32),
                jax.ShapeDtypeStruct((LANES, LANES), F32),
                jax.ShapeDtypeStruct((LAYERS, VEC), F32),
                jax.ShapeDtypeStruct((LAYERS, VEC), F32),
            ],
            in_specs=[hbm] * (GROUP + SMALL),
            out_specs=[vmem] * UNITS,
            scratch_shapes=[pltpu.VMEM(a.shape, a.dtype) for a in small]
            + [
                pltpu.VMEM((GROUP, DIM, DIM), F32),
                pltpu.VMEM((1152, DIM), F32),
                pltpu.VMEM((DIM, DIM), F32),
                pltpu.VMEM((DIM, 1536), F32),
                pltpu.VMEM((PAIR, GROUP, DIM, DIM), F32),
                pltpu.VMEM((PAIR, 1152, DIM), F32),
                pltpu.VMEM((PAIR, DIM, DIM), F32),
                pltpu.VMEM((PAIR, DIM, 1536), F32),
                pltpu.VMEM((SLOTS, PAIR, PAIR, UNITS, PAIR, ROWS, LANES), F32),
                pltpu.VMEM((PIECES, PAIR, TILES, PAIR, ROWS, LANES), F32),
                pltpu.VMEM((PIECES, PAIR, TILES, PAIR, ROWS, LANES), F32),
                pltpu.VMEM((PIECES, TILES, PAIR, ROWS, LANES), F32),
                pltpu.VMEM((PIECES, TILES, PAIR, ROWS, LANES), F32),
                pltpu.VMEM((PAIR, PIECES, UNITS, ROWS, LANES), F32),
                pltpu.VMEM((PIECES, UNITS, ROWS, LANES), F32),
                pltpu.VMEM((PAIR, BAND, BAND, LANES), F32),
                pltpu.VMEM((PAIR, BAND, BAND, LANES), F32),
                pltpu.VMEM((PAIR, BAND, BAND, LANES), F32),
                pltpu.VMEM((BAND, BAND, LANES), F32),
                pltpu.VMEM((ROWS, LANES), F32),
                pltpu.VMEM((tp_size, ROWS, LANES), F32),
                pltpu.VMEM((ROWS, LANES), F32),
                pltpu.VMEM((LANES, LANES), F32),
                pltpu.VMEM((devices, 1, DIM), F32),
                pltpu.VMEM((devices, 1, LANES), F32),
                pltpu.VMEM((LANES, LANES), F32),
                pltpu.VMEM((LAYERS, 256), F32),
                pltpu.VMEM(half, F32),
                pltpu.VMEM(half, F32),
                pltpu.VMEM(half, F32),
                pltpu.VMEM((TILES,) + half, F32),
                pltpu.VMEM((LAYERS, VEC), F32),
                dma((SOURCES,)),
                dma((UNITS,)), dma((UNITS,)),
                dma((PAIR * IN_FLIGHT,)), dma((PAIR * IN_FLIGHT,)),
                dma((PAIR * IN_FLIGHT,)), dma((PAIR * IN_FLIGHT,)),
                dma((IN_FLIGHT,)), dma((IN_FLIGHT,)),
                dma((SOURCES,)), dma((SOURCES,)),
                dma((PAIR,)), dma((GROUP,)),
                dma((1,)), dma((GROUP,)),
                pltpu.SemaphoreType.REGULAR((PAIR,)),
            ],
            compiler_params=pltpu.CompilerParams(
                collective_id=0, has_side_effects=True, vmem_limit_bytes=46 * 1024 * 1024
            ),
            name="reduce",
        )(*[pltpu.with_memory_space_constraint(a, pltpu.HBM) for a in (flat(g_qkv), flat(g_out), g_up[0], flat(g_down)) + small])

        weights = (w_qkv, w_out, w_up, w_down, w_vec)
        moments = (m_qkv, m_out, m_up, m_down, m_vec)
        outs = weights + moments + small[1:]
        return tuple(
            pl.pallas_call(
                update_kernel,
                out_shape=[jax.ShapeDtypeStruct(a.shape, a.dtype) for a in outs],
                in_specs=[vmem] * (len(sums) + len(weights) + len(moments)),
                out_specs=[hbm] * OUTS,
                scratch_shapes=[pltpu.VMEM(a.shape, a.dtype) for a in outs] + [dma((OUTS,))],
                compiler_params=pltpu.CompilerParams(vmem_limit_bytes=24 * 1024 * 1024),
                name="update",
            )(*sums, *weights, *moments)
        )

    grad_spec = P("fsdp", None, None, "tp")
    vec_grad_spec = P("fsdp", None, "tp")
    mat_spec = P(None, "fsdp", "tp")
    vec_spec = P(None, "tp")
    row_spec = P(None, "fsdp")
    state_specs = (mat_spec,) * GROUP + (vec_spec,) + (mat_spec,) * GROUP + (vec_spec,) + (row_spec, vec_spec) * GROUP + (vec_spec,)
    arg_specs = (grad_spec,) * GROUP + (vec_grad_spec,) + state_specs
    return jax.shard_map(local_step, mesh=mesh, in_specs=arg_specs, out_specs=state_specs, check_vma=False)
```

```python
import functools

import jax
import jax.numpy as jnp
from jax import lax
from jax.experimental import pallas as pl
from jax.experimental.pallas import tpu as pltpu
from jax.sharding import PartitionSpec as P

TRAIN_STEP = 3
LEARN_RATE = 0.0008
WEIGHT_DECAY = 0.03
MOMENTUM = 0.9
EPSILON = 1e-30
BETA_TWO = 1.0 - TRAIN_STEP ** -0.8

MESH = pl.DeviceIdType.MESH
F32 = jnp.float32
LAYERS = 16
TILES = 3
PAIR = 2
GROUP = 4
OUTS = 19
SMALL = 10
SOURCES = 5
UNITS = 6
BAND = 8
ROWS = 48
HALF = 64
CHIP = 96
LANES = 128
DIM = 384
VEC = 1248
PIECES = 12
LATE = 104
IN_FLIGHT = 4
SLOTS = 6
TILE_SLOT = (0, 0, 0, 1, 1, 1, 2, 3, 4, 5, 6)
COLUMN_TILES = (
    ("u", 0, LANES), ("u", 1, LANES), ("u", PAIR, LANES),
    ("q", 0, LANES), ("q", 1, LANES), ("q", PAIR, 32), ("o", 0, CHIP), ("d", 0, CHIP),
)
TILE_COL = (0, 1, 2, 3, 4, 5, 6, 7, 7, 7, 7)


def row_parts(block):
    parts, row = [], LANES * block
    while row < LANES * block + LANES:
        stop = min((row // ROWS + 1) * ROWS, LANES * block + LANES)
        parts.append((row // ROWS, row % ROWS, row - LANES * block, stop - row))
        row = stop
    return parts


def lane_iota(shape):
    return lax.broadcasted_iota(jnp.int32, shape, len(shape) - 1)


def shifted(tiles, start, width):
    base, shift = start // LANES, start % LANES
    value = tiles[base] if shift == 0 else pltpu.roll(tiles[base], LANES - shift, 1)
    lane = lane_iota(value.shape)
    if shift + width > LANES:
        value = jnp.where(lane < LANES - shift, value, pltpu.roll(tiles[base + 1], LANES - shift, 1))
    return value if width == LANES else jnp.where(lane < width, value, 0.0)


def sum_down(value):
    slot = (lane_iota(value.shape) // BAND) % BAND
    part = jnp.where((slot >= TILES) & (slot <= UNITS), value, 0.0)
    total = part + pltpu.roll(part, BAND, 1) + pltpu.roll(part, LAYERS, 1) + pltpu.roll(part, 24, 1)
    total = jnp.where(slot == UNITS, total, 0.0)
    total = total + pltpu.roll(total, 120, 1) + pltpu.roll(total, 112, 1) + pltpu.roll(total, 104, 1)
    return jnp.where((slot >= TILES) & (slot <= UNITS), total, value)


def reduce_kernel(tp_size, gq, go, gu, gd, *refs):
    small_hbm, refs = refs[:SMALL], refs[SMALL:]
    ut, vr_new, vc_new, scale, u_vec, v_new, *refs = refs
    small, refs = refs[:SMALL], refs[SMALL:]
    gvec, vr_q, vc_q, vr_o, vc_o, vr_u, vc_u, vr_d, vc_d, v_old = small
    own_u, own_q, own_o, own_d, rr_u, rr_q, rr_o, rr_d, cs, rxa, ryb, r2a, r2b, ff, fs, *refs = refs
    ck, cg, co, cd, rs, late, rrx, lrx, rv, vco, trx, t2rx, table, vd_pad, vec_a, vec_b, vec_c, vec_rx, vec_full, *refs = refs
    own_sem, d_send, d_recv, s1_send, s1_recv, s2_send, s2_recv, f_send, f_recv, *refs = refs
    c_send, c_recv, r_sem, t_sem, v_send, v_recv, hello_sem = refs
    f = lax.axis_index("fsdp")
    z = lax.axis_index("tp")
    c, x, y = f % PAIR, (f // PAIR) % PAIR, f // GROUP
    xn, yn, cn = 1 - x, 1 - y, 1 - c
    f_c, f_x, f_y = f + 1 - PAIR * c, f + PAIR - GROUP * x, f + GROUP - BAND * y
    me = z * BAND + f
    flip_f = [
        f + (j % PAIR) * (1 - PAIR * c) + (j // PAIR % PAIR) * (PAIR - GROUP * x) + j // GROUP * (GROUP - BAND * y)
        for j in range(BAND)
    ]
    flip_z = [z, z + 1 - PAIR * (z % PAIR), z + PAIR - GROUP * (z // PAIR), tp_size - 1 - z][:tp_size]
    z_near = (z - 1 + (tp_size - 1 - z) // (tp_size - 1), z + 1 - z // (tp_size - 1))
    far_first = sorted(
        range(1, tp_size * BAND), key=lambda m: -(m // BAND + m // GROUP % PAIR + m // PAIR % PAIR)
    )
    devices = tp_size * BAND

    def remote(src, dst, send, recv, **device):
        return pltpu.make_async_remote_copy(
            src_ref=src, dst_ref=dst, send_sem=send, recv_sem=recv, device_id=device, device_id_type=MESH
        )

    def wait_bytes(ref, sem):
        pltpu.make_async_copy(ref, ref, sem).wait()

    def source(k, n, group):
        if n < PAIR:
            return gu.at[pl.ds(GROUP * group + PAIR * n, PAIR)], own_u.at[PAIR * n : PAIR * n + PAIR], rr_u.at[k, PAIR * n : PAIR * n + PAIR]
        if n == PAIR:
            return gq.at[pl.ds(pl.multiple_of(1152 * group, BAND), 1152)], own_q, rr_q.at[k]
        if n == TILES:
            return go.at[pl.ds(pl.multiple_of(DIM * group, BAND), DIM)], own_o, rr_o.at[k]
        return gd.at[pl.ds(pl.multiple_of(DIM * group, BAND), DIM)], own_d, rr_d.at[k]

    def own_copy(k, n):
        src, dst, _ = source(k, n, PAIR * k + c)
        return pltpu.make_async_copy(src, dst, own_sem.at[n])

    def core_copy(k, n):
        src, _, dst = source(k, n, PAIR * k + cn)
        return remote(src, dst, d_send.at[n], d_recv.at[n], fsdp=f_c)

    def s1_copies(p):
        slot, sem = p % SLOTS, PAIR * (p % IN_FLIGHT)
        return (
            remote(cs.at[slot, :, xn, 0:TILES], rxa.at[p], s1_send.at[sem], s1_recv.at[sem], fsdp=f_x),
            remote(cs.at[slot, yn, :, TILES:UNITS], ryb.at[p], s1_send.at[sem + 1], s1_recv.at[sem + 1], fsdp=f_y),
        )

    def s2_copies(p):
        sem = PAIR * (p % IN_FLIGHT)
        return (
            remote(rxa.at[p, yn], r2a.at[p], s2_send.at[sem], s2_recv.at[sem], fsdp=f_y),
            remote(ryb.at[p, xn], r2b.at[p], s2_send.at[sem + 1], s2_recv.at[sem + 1], fsdp=f_x),
        )

    def final_copy(p):
        return remote(fs.at[p], ff.at[c, p], f_send.at[p % IN_FLIGHT], f_recv.at[p % IN_FLIGHT], fsdp=f_c)

    own_copy(0, 0).start()
    idle_sems = [s2_send.at[n] for n in range(BAND)] + [f_send.at[n] for n in range(PAIR)]
    small_copies = [pltpu.make_async_copy(small_hbm[n], small[n], idle_sems[n]) for n in range(SMALL)]
    for copy in small_copies:
        copy.start()

    barrier = pltpu.get_barrier_semaphore()

    def signal_near(sem):
        for other in z_near:
            pl.semaphore_signal(sem, inc=1, device_id={"tp": other}, device_id_type=MESH)

    for other in (f_c, f_x, f_y):
        pl.semaphore_signal(barrier, inc=1, device_id={"fsdp": other}, device_id_type=MESH)
    signal_near(barrier)
    pl.semaphore_wait(barrier, SOURCES)

    def first_copies(xa, yb, sem):
        for layer, start, size in ((0, xa, CHIP), (0, PAIR + xa, CHIP), (1, PAIR * yb, PAIR * CHIP)):
            rows = pl.ds(pl.multiple_of(CHIP * start, BAND), size)
            remote(
                gu.at[GROUP * cn + layer, rows], rr_u.at[0, layer, rows], d_send.at[sem], d_recv.at[sem], fsdp=f_c
            ).start()

    first_copies(xn, yn, 0)
    first_copies(x, y, SOURCES)
    core_copy(0, 1).start()
    own_copy(0, 1).start()

    own_half = pl.ds(pl.multiple_of(BAND * c, BAND), BAND)
    other_half = pl.ds(pl.multiple_of(BAND * cn, BAND), BAND)
    vec_copies = (
        remote(gvec.at[other_half], vec_rx.at[0], v_send.at[0], v_recv.at[0], fsdp=f_c),
        remote(vec_a, vec_rx.at[1], v_send.at[0], v_recv.at[1], fsdp=f_x),
        remote(vec_b, vec_rx.at[PAIR], v_send.at[0], v_recv.at[PAIR], fsdp=f_y),
        remote(vec_c, vec_full.at[own_half], v_send.at[0], v_recv.at[TILES], fsdp=f_c),
    )

    def vec_step(n):
        if n > 0:
            vec_copies[n - 1].wait_recv()
            vec_copies[n - 1].wait_send()
        if n == 1:
            vec_a[...] = gvec[own_half] + vec_rx[0]
        elif n == PAIR:
            vec_b[...] = vec_a[...] + vec_rx[1]
        elif n == TILES:
            total = vec_b[...] + vec_rx[PAIR]
            vec_c[...] = total
            vec_full[own_half] = total
        if n < GROUP:
            vec_copies[n].start()

    def prepare_small():
        for copy in small_copies:
            copy.wait()
        vec_step(0)
        rs[...] = jnp.zeros((ROWS, LANES), F32)
        late[...] = jnp.zeros((BAND, LANES), F32)
        ck[1, 7] = jnp.zeros((BAND, LANES), F32)
        vco[...] = jnp.zeros((LANES, LANES), F32)
        table[...] = jnp.zeros((LANES, LANES), F32)
        vd_pad[...] = jnp.zeros((LAYERS, 256), F32)
        vd_pad[:, 0:192] = vr_d[...]
        for k in range(PAIR):
            rows = slice(BAND * k, BAND * k + BAND)
            for t, (name, tile, width) in enumerate(COLUMN_TILES):
                ref = {"u": vc_u, "q": vc_q, "o": vc_o, "d": vc_d}[name]
                row = HALF * k + BAND * t
                vco[row : row + BAND, 0:width] = ref[rows, LANES * tile : LANES * tile + width]
            for s, ref in enumerate((vr_u, vr_q, vr_o)):
                table[HALF * k + BAND * s : HALF * k + BAND * s + BAND, 0:ROWS] = ref[rows, :]
            tiles = (vd_pad[rows, 0:LANES], vd_pad[rows, LANES:256])
            for b in range(GROUP):
                table[HALF * k + 24 + BAND * b : HALF * k + 32 + BAND * b, :] = shifted(tiles, ROWS * b, ROWS)
        rv[...] = jnp.transpose(table[...])[0:ROWS, :]

    def pack_up(k, half, slot):
        def body(h, carry):
            q, core = h // PAIR, h % PAIR
            rows = pl.ds(pl.multiple_of(ROWS * h, BAND), ROWS)
            for i in range(PAIR):
                for t in range(TILES):
                    lanes = slice(LANES * t, LANES * t + LANES)
                    cs[slot, q // PAIR, q % PAIR, TILES * i + t, core] = (
                        own_u[PAIR * half + i, rows, lanes] + rr_u[k, PAIR * half + i, rows, lanes]
                    )
            return carry

        lax.fori_loop(0, BAND, body, 0)

    def pack_flat(own, other, slot, first, count, unit):
        def body(n, carry):
            rows = pl.ds(pl.multiple_of(LANES * (first + n), LANES), LANES)
            for block in range(TILES):
                lanes = slice(LANES * block, LANES * block + LANES)
                value = jnp.transpose(own[rows, lanes] + other[rows, lanes])
                for h, row, here, size in row_parts(block):
                    cs[slot, h // GROUP, (h // PAIR) % PAIR, unit + n, h % PAIR, row : row + size, :] = value[here : here + size]
            return carry

        lax.fori_loop(0, count, body, 0)

    def pack_down(k, slot):
        def body(n, carry):
            q, t = n // TILES, n % TILES
            rows = pl.ds(pl.multiple_of(LANES * t, LANES), LANES)
            for block in range(TILES):
                lanes = pl.ds(pl.multiple_of(DIM * q + LANES * block, LANES), LANES)
                value = jnp.transpose(own_d[rows, lanes] + rr_d[k, rows, lanes])
                for h, row, here, size in row_parts(block):
                    core, b = h // GROUP, h % GROUP
                    cs[slot + b // PAIR, q // PAIR, q % PAIR, TILES * (b % PAIR) + t, core, row : row + size, :] = value[
                        here : here + size
                    ]
            return carry

        lax.fori_loop(0, 12, body, 0)

    def pack_first(xa, yb):
        def body(n, carry):
            part, core = n // PAIR, n % PAIR
            for i, q in ((0, PAIR * part + xa), (1, PAIR * yb + part)):
                rows = pl.ds(pl.multiple_of(CHIP * q + ROWS * core, BAND), ROWS)
                for t in range(TILES):
                    lanes = slice(LANES * t, LANES * t + LANES)
                    cs[0, q // PAIR, q % PAIR, TILES * i + t, core] = own_u[i, rows, lanes] + rr_u[0, i, rows, lanes]
            return carry

        lax.fori_loop(0, GROUP, body, 0)

    def prepare_first():
        own_copy(0, 0).wait()
        wait_bytes(rr_u.at[0, 0], d_recv.at[0])
        pack_first(xn, yn)
        for copy in s1_copies(0):
            copy.start()
        for n in (PAIR, TILES):
            core_copy(0, n).start()
        for n in (PAIR, TILES, GROUP):
            own_copy(0, n).start()
        wait_bytes(rr_u.at[0, 0], d_recv.at[SOURCES])
        pack_first(x, y)
        own_copy(1, 0).start()

    def prepare(p):
        if p == 0:
            return prepare_first()
        k, n, slot = p // UNITS, p % UNITS, p % SLOTS
        needs = {0: (0,), 1: (1,), PAIR: (PAIR,), TILES: (TILES,), GROUP: (GROUP,), SOURCES: ()}[n]
        for source_index in needs:
            own_copy(k, source_index).wait()
            core_copy(k, source_index).wait_recv()
        if p >= IN_FLIGHT:
            for copy in s1_copies(p - IN_FLIGHT):
                copy.wait_send()
        if n < PAIR:
            pack_up(k, n, slot)
        elif n == PAIR:
            pack_flat(own_q, rr_q.at[k], slot, 0, UNITS, 0)
        elif n == TILES:
            pack_flat(own_q, rr_q.at[k], slot, UNITS, TILES, 0)
            pack_flat(own_o, rr_o.at[k], slot, 0, TILES, TILES)
        elif n == GROUP:
            pack_down(k, slot)
        for copy in s1_copies(p):
            copy.start()
        if p == 1:
            core_copy(0, GROUP).start()
        if k == 0:
            reload = {0: (0,), 1: (1,), TILES: (PAIR, TILES), GROUP: (GROUP,)}.get(n, ())
            for source_index in reload:
                own_copy(1, source_index).start()
        for source_index in {GROUP: (0, 1), SOURCES: (PAIR, TILES), UNITS: (GROUP,)}.get(p, ()):
            if source_index == 0:
                for sem in (0, SOURCES):
                    wait_bytes(rr_u.at[0, 0], d_send.at[sem])
            else:
                core_copy(0, source_index).wait_send()
            core_copy(1, source_index).start()

    def stage_two(p):
        slot = p % SLOTS
        for copy in s1_copies(p):
            copy.wait_recv()

        def body(u, carry):
            for core in range(PAIR):
                rxa[p, yn, u, core] = rxa[p, yn, u, core] + cs[slot, yn, x, u, core]
                ryb[p, xn, u, core] = ryb[p, xn, u, core] + cs[slot, y, xn, TILES + u, core]
            return carry

        lax.fori_loop(0, TILES, body, 0)
        if p >= IN_FLIGHT:
            for copy in s2_copies(p - IN_FLIGHT):
                copy.wait_send()
        for copy in s2_copies(p):
            copy.start()

    def stage_three(p):
        slot = p % SLOTS
        for copy in s2_copies(p):
            copy.wait_recv()

        def body(u, carry):
            fs[p, u] = cs[slot, y, x, u, cn] + rxa[p, y, u, cn] + r2a[p, u, cn]
            fs[p, TILES + u] = cs[slot, y, x, TILES + u, cn] + ryb[p, x, u, cn] + r2b[p, u, cn]
            return carry

        if p >= IN_FLIGHT:
            final_copy(p - IN_FLIGHT).wait_send()
        lax.fori_loop(0, TILES, body, 0)
        final_copy(p).start()

        def body_own(u, carry):
            ff[c, p, u] = cs[slot, y, x, u, c] + rxa[p, y, u, c] + r2a[p, u, c]
            ff[c, p, TILES + u] = cs[slot, y, x, TILES + u, c] + ryb[p, x, u, c] + r2b[p, u, c]
            return carry

        lax.fori_loop(0, TILES, body_own, 0)
        if p % UNITS >= GROUP:
            finish_down(p // UNITS, p % PAIR, c)

    def keep(step_k, layer, tile, value, first=True):
        ut[layer, tile] = value
        square = value * value
        sums = jnp.sum(square, axis=0, keepdims=True)
        row = pl.ds(layer % BAND, 1)
        column = TILE_COL[tile]
        ref = cd.at[f] if step_k == 1 and column == 7 else ck.at[step_k, column]
        ref[row, :] = sums if first else ref[row, :] + sums
        return square

    def keep_rows(layer, slot, square):
        lane = HALF * (layer // BAND) + BAND * slot + layer % BAND
        sums = jnp.sum(square, axis=1, keepdims=True)
        rs[...] = jnp.where(lane_iota((ROWS, LANES)) == lane, sums, rs[...])

    def keep_rows_late(layer, b, square):
        sums = jnp.sum(square, axis=1, keepdims=True)
        lane, value = lane_iota((BAND, LANES)), late[...]
        for g in range(UNITS):
            here = lane == LAYERS * g + BAND * (b - PAIR) + layer % BAND
            value = jnp.where(here, sums[BAND * g : BAND * g + BAND], value)
        late[...] = value

    def late_group(value, g):
        lane = lane_iota(value.shape)
        value = pltpu.roll(value, (LATE - LAYERS * g) % LANES, 1)
        return jnp.where((lane >= LATE) & (lane < LATE + LAYERS), value, 0.0)

    def send_rows(ref, sem):
        for other in flip_z[:0:-1]:
            remote(ref.at[z], ref.at[z], r_sem.at[sem], r_sem.at[sem + 1], tp=other).start()

    def finish_up(k):
        def body(i8, carry):
            core, i = i8 // GROUP, i8 % GROUP
            layer = BAND * k + i8
            square = [keep(k, layer, t, ff[core, UNITS * k + i // PAIR, TILES * (i % PAIR) + t]) for t in range(TILES)]
            keep_rows(layer, 0, square[0] + square[1] + square[PAIR])
            return carry

        lax.fori_loop(0, BAND, body, 0)

    def finish_qkv(k):
        def body(core, carry):
            tiles = [ff.at[core, UNITS * k + PAIR + t // UNITS, t % UNITS] for t in range(12)]
            for i in range(GROUP):
                layer = BAND * k + GROUP * core + i
                first = PAIR * i
                part = [tiles[t][...] for t in range(first, min(first + GROUP, 9))]
                square = [
                    keep(k, layer, TILES + t, shifted(part, 32 * i + LANES * t, LANES if t < PAIR else 32)) for t in range(TILES)
                ]
                keep_rows(layer, 1, square[0] + square[1] + square[PAIR])
                part = [tiles[9 + t][...] for t in range(TILES)]
                keep_rows(layer, PAIR, keep(k, layer, UNITS, shifted(part, CHIP * i, CHIP)))
            return carry

        lax.fori_loop(0, PAIR, body, 0)

    def finish_down(k, half, core):
        for b in (PAIR * half, PAIR * half + 1):
            part = [ff[core, UNITS * k + GROUP + half, TILES * (b % PAIR) + t] for t in range(TILES)]
            for i in range(GROUP):
                layer = BAND * k + GROUP * core + i
                square = keep(k, layer, 7 + b, shifted(part, CHIP * i, CHIP), first=b == 0)
                if k == 1 and half == 1:
                    keep_rows_late(layer, b, square)
                else:
                    keep_rows(layer, TILES + b, square)

    def columns_to_owner(k):
        for other in flip_f[:0:-1]:
            remote(ck.at[k, other], cg.at[k, f], c_send.at[PAIR * k], c_recv.at[PAIR * k], fsdp=other).start()
        cg[k, f] = ck[k, f]

    def columns_to_all(k):
        sem = PAIR * k + 1
        wait_bytes(cg.at[k, 0:7], c_recv.at[PAIR * k])
        total = cg[k, 0]
        for other in range(1, BAND):
            total = total + cg[k, other]
        co[k, f] = total
        for other in flip_f[:0:-1]:
            remote(co.at[k, f], co.at[k, f], c_send.at[sem], c_recv.at[sem], fsdp=other).start()

    def last_columns():
        for other in flip_f[:0:-1]:
            remote(cd.at[f], cd.at[f], c_send.at[GROUP], c_recv.at[GROUP], fsdp=other).start()

    def finish(p):
        k, n = p // UNITS, p % UNITS
        final_copy(p).wait_recv()
        if n == 1:
            finish_up(k)
        elif n == TILES:
            finish_qkv(k)
            if k == 1:
                columns_to_owner(k)
        elif n >= GROUP:
            finish_down(k, n % PAIR, cn)
            if n == SOURCES:
                columns_to_owner(k) if k == 0 else last_columns()
            elif k == 1:
                rrx[z] = rs[...]
                send_rows(rrx, 0)

    def send_all(ref, sems):
        for m in far_first:
            device = {"tp": flip_z[m // BAND], "fsdp": flip_f[m % BAND]}
            remote(ref.at[me], ref.at[me], sems.at[0], sems.at[1], **device).start()

    def prepare_totals():
        square = vec_full[...] * vec_full[...]
        vec_total = jnp.sum(jnp.sum(square, axis=1, keepdims=True), axis=0, keepdims=True)
        trx[me, :, LANES : PAIR * LANES] = jnp.sum(rv[...], axis=0, keepdims=True)
        trx[me, :, PAIR * LANES : TILES * LANES] = jnp.broadcast_to(vec_total, (1, LANES))

    def send_totals():
        lane = lane_iota((1, LANES))
        total = jnp.sum(rs[...], axis=0, keepdims=True)
        late_sum = jnp.sum(late[...], axis=0, keepdims=True)
        for g in range(UNITS):
            total = total + late_group(late_sum, g)
        for i in range(GROUP):
            square = None
            for b in range(PAIR):
                value = shifted([fs[PIECES - 1, TILES * b + t] for t in range(TILES)], CHIP * i, CHIP)
                square = value * value if square is None else square + value * value
            sums = jnp.sum(jnp.sum(square, axis=0, keepdims=True), axis=1, keepdims=True)
            total = total + jnp.where(lane == HALF + BAND * TILES + GROUP * c + i, sums, 0.0)
        trx[me, :, 0:LANES] = total
        send_all(trx, t_sem)

    for step in range(PIECES + TILES):
        for lag, part in ((0, prepare), (1, stage_two), (TILES, finish), (PAIR, stage_three)):
            if 0 <= step - lag < PIECES:
                with jax.named_scope(f"{part.__name__}_{step - lag}"):
                    part(step - lag)
        if step == 0:
            prepare_small()
        if step in (1, TILES, SOURCES, 7):
            vec_step((step + 1) // PAIR)
        if step in (PAIR, GROUP):
            signal_near(hello_sem.at[step // GROUP])
        if step in (TILES, SOURCES):
            pl.semaphore_wait(hello_sem.at[step // SOURCES], PAIR)
        if step == 10:
            columns_to_all(0)
            prepare_totals()
        if step == PIECES + 1:
            send_totals()

    lrx[z] = late[...]
    send_rows(lrx, PAIR)
    columns_to_all(1)
    wait_bytes(trx.at[0 : devices - 1], t_sem.at[1])
    totals = jnp.sum(trx[...], axis=0)
    square_sum = totals[:, 0:LANES]
    old_sum = totals[:, LANES:256] * (1.0 / tp_size)
    vec_part = totals[:, 256:257] * 0.125
    total = jnp.sum(square_sum, axis=1, keepdims=True) + vec_part
    clip = jnp.minimum(1.0, 1.0 / jnp.sqrt(total))

    def clipped(value):
        return jnp.where(clip > 0.0, clip * (clip * value), 0.0)

    slot = (lane_iota((1, LANES)) // BAND) % BAND
    row_inv = jnp.where(slot >= TILES, 1.0 / 1536.0, 1.0 / 384.0).astype(F32)
    col_inv = jnp.where(
        slot == 0, 1.0 / (384.0 * tp_size), jnp.where(slot == 1, 1.0 / (288.0 * tp_size), 1.0 / (96.0 * tp_size))
    ).astype(F32)
    mean_new = BETA_TWO * (sum_down(old_sum) * row_inv) + (1.0 - BETA_TWO) * (
        clipped(sum_down(square_sum)) * (row_inv * col_inv) + EPSILON
    )
    wait_bytes(rrx.at[0 : tp_size - 1], r_sem.at[1])
    wait_bytes(lrx.at[0 : tp_size - 1], r_sem.at[TILES])
    row_sum, late_sum = jnp.sum(rrx[...], axis=0), jnp.sum(lrx[...], axis=0)
    row_sum = row_sum + jnp.concatenate([late_group(late_sum, g) for g in range(UNITS)], axis=0)
    row_new = BETA_TWO * rv[...] + (1.0 - BETA_TWO) * (clipped(row_sum) * col_inv + EPSILON)
    rv[...] = clip * lax.rsqrt(row_new / mean_new)
    rs[...] = row_new

    for k in range(PAIR):
        wait_bytes(co.at[k, 0:7], c_recv.at[PAIR * k + 1])
    wait_bytes(cd.at[0:7], c_recv.at[GROUP])
    last_sum = cd[0]
    for other in range(1, BAND):
        last_sum = last_sum + cd[other]
    wait_bytes(cd.at[0:7], c_send.at[TILES])
    co[1, 7] = last_sum
    col_sum = co[...].reshape(LANES, LANES)
    down_row = (lax.broadcasted_iota(jnp.int32, (LANES, LANES), 0) // BAND) % BAND == 7
    col_new = BETA_TWO * vco[...] + (1.0 - BETA_TWO) * (
        clipped(col_sum) * jnp.where(down_row, 1.0 / 1536.0, 1.0 / 384.0).astype(F32) + EPSILON
    )
    vc_new[...] = col_new
    vco[...] = lax.rsqrt(col_new)

    vec_grad = vec_full[...] * clip
    vec_var = BETA_TWO * v_old[...] + (1.0 - BETA_TWO) * (vec_grad * vec_grad + EPSILON)
    v_new[...] = vec_var
    vec_update = vec_grad / jnp.sqrt(vec_var)
    u_vec[...] = vec_update
    vec_rows = jnp.sum(vec_update * vec_update, axis=1, keepdims=True) * (0.125 / 128.0)
    vec_rows = jnp.broadcast_to(vec_rows, (LAYERS, LANES))
    table[56:HALF, :] = vec_rows[0:BAND]
    table[120:LANES, :] = vec_rows[BAND:LAYERS]

    def update(layer, carry):
        index = HALF * (layer // BAND) + layer % BAND
        lane = lane_iota((ROWS, LANES))
        factors = rv[...]
        tile = 0
        for s in range(7):
            row = jnp.sum(jnp.where(lane == index + BAND * s, factors, 0.0), axis=1, keepdims=True)
            square = None
            while tile < 11 and TILE_SLOT[tile] == s:
                value = ut[layer, tile] * row * vco[pl.ds(index + BAND * TILE_COL[tile], 1), :]
                ut[layer, tile] = value
                square = value * value if square is None else square + value * value
                tile += 1
            table[pl.ds(index + BAND * s, 1), :] = jnp.sum(square, axis=0, keepdims=True)
        return carry

    lax.fori_loop(0, LAYERS, update, 0, unroll=PAIR)

    t2rx[me] = jnp.sum(jnp.transpose(table[...]), axis=0, keepdims=True)
    send_all(t2rx, t_sem.at[PAIR:GROUP])
    table[0:ROWS, :] = rs[...]
    vr_new[...] = jnp.transpose(table[...])
    wait_bytes(t2rx.at[0 : devices - 1], t_sem.at[TILES])
    update_sum = sum_down(jnp.sum(t2rx[...], axis=0))
    inverse = jnp.where(slot == 7, 1.0 / (1248.0 * tp_size), row_inv * col_inv).astype(F32)
    factor = (1.0 - MOMENTUM) / jnp.maximum(1.0, jnp.sqrt(update_sum * inverse))
    scale[...] = jnp.transpose(jnp.broadcast_to(factor, (LANES, LANES)))

    for n in range(SOURCES):
        core_copy(1, n).wait_send()
    for n in (0, 1, PAIR, GROUP):
        wait_bytes(cd.at[0:7], c_send.at[n])
    for p in range(PIECES - IN_FLIGHT, PIECES):
        for copy in s1_copies(p) + s2_copies(p):
            copy.wait_send()
        final_copy(p).wait_send()
    wait_bytes(rrx.at[0 : tp_size - 1], r_sem.at[0])
    wait_bytes(lrx.at[0 : tp_size - 1], r_sem.at[PAIR])
    wait_bytes(trx.at[0 : devices - 1], t_sem.at[0])
    wait_bytes(t2rx.at[0 : devices - 1], t_sem.at[PAIR])


def update_kernel(ut, vr_new, vc_new, scale, u_vec, v_new, w_q, w_o, w_u, w_d, w_v, m_q, m_o, m_u, m_d, m_v, *refs):
    outs, refs = refs[:OUTS], refs[OUTS:]
    buffers, sems = refs[:OUTS], refs[OUTS]
    wo_q, wo_o, wo_u, wo_d, wo_v, mo_q, mo_o, mo_u, mo_d, mo_v, *rest = buffers
    vr_q, vc_q, vr_o, vc_o, vr_u, vc_u, vr_d, vc_d, v_out = rest
    by_layer = [n for n in range(OUTS) if len(outs[n].shape) == TILES]
    copies = [pltpu.make_async_copy(buffers[n], outs[n], sems.at[n]) for n in range(OUTS)]

    def finish(update, weight, moment):
        moment_new = (MOMENTUM * moment.astype(F32) + update).astype(jnp.bfloat16)
        return (1.0 - LEARN_RATE * WEIGHT_DECAY) * weight - LEARN_RATE * moment_new.astype(F32), moment_new

    v_out[...] = v_new[...]
    for k in range(PAIR):
        rows = slice(BAND * k, BAND * k + BAND)
        for t in range(10):
            lanes = slice(LANES * t, min(LANES * t + LANES, VEC))
            factor = scale[HALF * k + 56 : HALF * k + HALF, 0 : lanes.stop - lanes.start]
            weight_new, moment_new = finish(u_vec[rows, lanes] * factor, w_v[rows, lanes], m_v[rows, lanes])
            wo_v[rows, lanes] = weight_new
            mo_v[rows, lanes] = moment_new
        for t, (name, tile, width) in enumerate(COLUMN_TILES):
            ref = {"u": vc_u, "q": vc_q, "o": vc_o, "d": vc_d}[name]
            row = HALF * k + BAND * t
            ref[rows, LANES * tile : LANES * tile + width] = vc_new[row : row + BAND, 0:width]
        for s, ref in enumerate((vr_u, vr_q, vr_o)):
            row = HALF * k + BAND * s
            ref[rows, :] = vr_new[row : row + BAND, 0:ROWS]
        b0, b1, b2, b3 = (vr_new[HALF * k + BAND * (TILES + b) : HALF * k + BAND * (GROUP + b), :] for b in range(GROUP))
        lane = lane_iota((BAND, LANES))
        b2 = pltpu.roll(b2, CHIP, 1)
        vr_d[rows, 0:LANES] = jnp.where(lane < ROWS, b0, jnp.where(lane < CHIP, pltpu.roll(b1, ROWS, 1), b2))
        vr_d[rows, LANES:192] = jnp.where(lane < LAYERS, b2, pltpu.roll(b3, LAYERS, 1))[:, 0:HALF]
    for n in range(OUTS):
        if n not in by_layer:
            copies[n].start()

    def body(layer):
        index = HALF * (layer // BAND) + layer % BAND

        def one(tile, slot, w, m, wo, mo, rows, lanes):
            factor = scale[pl.ds(index + BAND * slot, 1), :]
            update = (ut[layer, tile] * factor)[:, 0 : lanes.stop - lanes.start]
            weight_new, moment_new = finish(update, w[layer, rows, lanes], m[layer, rows, lanes])
            wo[layer, rows, lanes] = weight_new
            mo[layer, rows, lanes] = moment_new

        every = slice(0, ROWS)
        for t in range(TILES):
            one(t, 0, w_u, m_u, wo_u, mo_u, every, slice(LANES * t, LANES * t + LANES))
            one(TILES + t, 1, w_q, m_q, wo_q, mo_q, every, slice(LANES * t, min(LANES * t + LANES, 288)))
        one(UNITS, PAIR, w_o, m_o, wo_o, mo_o, every, slice(0, CHIP))
        for b in range(GROUP):
            one(7 + b, TILES, w_d, m_d, wo_d, mo_d, slice(ROWS * b, ROWS * b + ROWS), slice(0, CHIP))

    def two_layers(i, carry):
        for layer in range(PAIR):
            body(PAIR * i + layer)
        layers = pl.ds(PAIR * i, PAIR)
        for n in by_layer:
            pltpu.make_async_copy(buffers[n].at[layers], outs[n].at[layers], sems.at[n]).start()
        return carry

    lax.fori_loop(0, BAND, two_layers, 0)
    for copy in copies:
        copy.wait()


def solution(mesh):
    tp_size = mesh.shape["tp"]
    devices = tp_size * mesh.shape["fsdp"]
    vmem = pl.BlockSpec(memory_space=pltpu.VMEM)
    hbm = pl.BlockSpec(memory_space=pltpu.HBM)

    def local_step(g_qkv, g_out, g_up, g_down, g_vec, w_qkv, w_out, w_up, w_down, w_vec, m_qkv, m_out, m_up, m_down, m_vec, vr_qkv, vc_qkv, vr_out, vc_out, vr_up, vc_up, vr_down, vc_down, v_vec):
        def flat(g):
            g = jnp.swapaxes(g[0], 1, PAIR)
            return g.reshape(g.shape[0] * g.shape[1], g.shape[PAIR])

        dma = pltpu.SemaphoreType.DMA
        half = (BAND, VEC)
        small = (g_vec[0], vr_qkv, vc_qkv, vr_out, vc_out, vr_up, vc_up, vr_down, vc_down, v_vec)
        sums = pl.pallas_call(
            functools.partial(reduce_kernel, tp_size),
            out_shape=[
                jax.ShapeDtypeStruct((LAYERS, 11, ROWS, LANES), F32),
                jax.ShapeDtypeStruct((LANES, LANES), F32),
                jax.ShapeDtypeStruct((LANES, LANES), F32),
                jax.ShapeDtypeStruct((LANES, LANES), F32),
                jax.ShapeDtypeStruct((LAYERS, VEC), F32),
                jax.ShapeDtypeStruct((LAYERS, VEC), F32),
            ],
            in_specs=[hbm] * (GROUP + SMALL),
            out_specs=[vmem] * UNITS,
            scratch_shapes=[pltpu.VMEM(a.shape, a.dtype) for a in small]
            + [
                pltpu.VMEM((GROUP, DIM, DIM), F32),
                pltpu.VMEM((1152, DIM), F32),
                pltpu.VMEM((DIM, DIM), F32),
                pltpu.VMEM((DIM, 1536), F32),
                pltpu.VMEM((PAIR, GROUP, DIM, DIM), F32),
                pltpu.VMEM((PAIR, 1152, DIM), F32),
                pltpu.VMEM((PAIR, DIM, DIM), F32),
                pltpu.VMEM((PAIR, DIM, 1536), F32),
                pltpu.VMEM((SLOTS, PAIR, PAIR, UNITS, PAIR, ROWS, LANES), F32),
                pltpu.VMEM((PIECES, PAIR, TILES, PAIR, ROWS, LANES), F32),
                pltpu.VMEM((PIECES, PAIR, TILES, PAIR, ROWS, LANES), F32),
                pltpu.VMEM((PIECES, TILES, PAIR, ROWS, LANES), F32),
                pltpu.VMEM((PIECES, TILES, PAIR, ROWS, LANES), F32),
                pltpu.VMEM((PAIR, PIECES, UNITS, ROWS, LANES), F32),
                pltpu.VMEM((PIECES, UNITS, ROWS, LANES), F32),
                pltpu.VMEM((PAIR, BAND, BAND, LANES), F32),
                pltpu.VMEM((PAIR, BAND, BAND, LANES), F32),
                pltpu.VMEM((PAIR, BAND, BAND, LANES), F32),
                pltpu.VMEM((BAND, BAND, LANES), F32),
                pltpu.VMEM((ROWS, LANES), F32),
                pltpu.VMEM((BAND, LANES), F32),
                pltpu.VMEM((tp_size, ROWS, LANES), F32),
                pltpu.VMEM((tp_size, BAND, LANES), F32),
                pltpu.VMEM((ROWS, LANES), F32),
                pltpu.VMEM((LANES, LANES), F32),
                pltpu.VMEM((devices, 1, DIM), F32),
                pltpu.VMEM((devices, 1, LANES), F32),
                pltpu.VMEM((LANES, LANES), F32),
                pltpu.VMEM((LAYERS, 256), F32),
                pltpu.VMEM(half, F32),
                pltpu.VMEM(half, F32),
                pltpu.VMEM(half, F32),
                pltpu.VMEM((TILES,) + half, F32),
                pltpu.VMEM((LAYERS, VEC), F32),
                dma((SOURCES,)),
                dma((UNITS,)), dma((UNITS,)),
                dma((PAIR * IN_FLIGHT,)), dma((PAIR * IN_FLIGHT,)),
                dma((PAIR * IN_FLIGHT,)), dma((PAIR * IN_FLIGHT,)),
                dma((IN_FLIGHT,)), dma((IN_FLIGHT,)),
                dma((SOURCES,)), dma((SOURCES,)),
                dma((GROUP,)), dma((GROUP,)),
                dma((1,)), dma((GROUP,)),
                pltpu.SemaphoreType.REGULAR((PAIR,)),
            ],
            compiler_params=pltpu.CompilerParams(
                collective_id=0, has_side_effects=True, vmem_limit_bytes=46 * 1024 * 1024
            ),
            name="reduce",
        )(*[pltpu.with_memory_space_constraint(a, pltpu.HBM) for a in (flat(g_qkv), flat(g_out), g_up[0], flat(g_down)) + small])

        weights = (w_qkv, w_out, w_up, w_down, w_vec)
        moments = (m_qkv, m_out, m_up, m_down, m_vec)
        outs = weights + moments + small[1:]
        return tuple(
            pl.pallas_call(
                update_kernel,
                out_shape=[jax.ShapeDtypeStruct(a.shape, a.dtype) for a in outs],
                in_specs=[vmem] * (len(sums) + len(weights) + len(moments)),
                out_specs=[hbm] * OUTS,
                scratch_shapes=[pltpu.VMEM(a.shape, a.dtype) for a in outs] + [dma((OUTS,))],
                compiler_params=pltpu.CompilerParams(vmem_limit_bytes=24 * 1024 * 1024),
                name="update",
            )(*sums, *weights, *moments)
        )

    grad_spec = P("fsdp", None, None, "tp")
    vec_grad_spec = P("fsdp", None, "tp")
    mat_spec = P(None, "fsdp", "tp")
    vec_spec = P(None, "tp")
    row_spec = P(None, "fsdp")
    state_specs = (mat_spec,) * GROUP + (vec_spec,) + (mat_spec,) * GROUP + (vec_spec,) + (row_spec, vec_spec) * GROUP + (vec_spec,)
    arg_specs = (grad_spec,) * GROUP + (vec_grad_spec,) + state_specs
    return jax.shard_map(local_step, mesh=mesh, in_specs=arg_specs, out_specs=state_specs, check_vma=False)
```

```python
import functools

import jax
import jax.numpy as jnp
from jax import lax
from jax.experimental import pallas as pl
from jax.experimental.pallas import tpu as pltpu
from jax.sharding import PartitionSpec as P

TRAIN_STEP = 3
LEARN_RATE = 0.0008
WEIGHT_DECAY = 0.03
MOMENTUM = 0.9
EPSILON = 1e-30
BETA_TWO = 1.0 - TRAIN_STEP ** -0.8

MESH = pl.DeviceIdType.MESH
F32 = jnp.float32
LAYERS = 16
TILES = 3
PAIR = 2
GROUP = 4
OUTS = 19
STATE = 10
SMALL = 10
SOURCES = 5
UNITS = 6
BAND = 8
ROWS = 48
HALF = 64
CHIP = 96
LANES = 128
DIM = 384
VEC = 1248
PIECES = 12
LATE = 104
IN_FLIGHT = 4
SLOTS = 6
TILE_SLOT = (0, 0, 0, 1, 1, 1, 2, 3, 4, 5, 6)
COLUMN_TILES = (
    ("u", 0, LANES), ("u", 1, LANES), ("u", PAIR, LANES),
    ("q", 0, LANES), ("q", 1, LANES), ("q", PAIR, 32), ("o", 0, CHIP), ("d", 0, CHIP),
)
TILE_COL = (0, 1, 2, 3, 4, 5, 6, 7, 7, 7, 7)


def row_parts(block):
    parts, row = [], LANES * block
    while row < LANES * block + LANES:
        stop = min((row // ROWS + 1) * ROWS, LANES * block + LANES)
        parts.append((row // ROWS, row % ROWS, row - LANES * block, stop - row))
        row = stop
    return parts


def lane_iota(shape):
    return lax.broadcasted_iota(jnp.int32, shape, len(shape) - 1)


def shifted(tiles, start, width):
    base, shift = start // LANES, start % LANES
    value = tiles[base] if shift == 0 else pltpu.roll(tiles[base], LANES - shift, 1)
    lane = lane_iota(value.shape)
    if shift + width > LANES:
        value = jnp.where(lane < LANES - shift, value, pltpu.roll(tiles[base + 1], LANES - shift, 1))
    return value if width == LANES else jnp.where(lane < width, value, 0.0)


def sum_down(value):
    slot = (lane_iota(value.shape) // BAND) % BAND
    part = jnp.where((slot >= TILES) & (slot <= UNITS), value, 0.0)
    total = part + pltpu.roll(part, BAND, 1) + pltpu.roll(part, LAYERS, 1) + pltpu.roll(part, 24, 1)
    total = jnp.where(slot == UNITS, total, 0.0)
    total = total + pltpu.roll(total, 120, 1) + pltpu.roll(total, 112, 1) + pltpu.roll(total, 104, 1)
    return jnp.where((slot >= TILES) & (slot <= UNITS), total, value)


def reduce_kernel(tp_size, gq, go, gu, gd, *refs):
    small_hbm, refs = refs[:SMALL], refs[SMALL:]
    state_hbm, refs = refs[:STATE], refs[STATE:]
    ut, vr_new, vc_new, scale, u_vec, v_new, *refs = refs
    state, refs = refs[:STATE], refs[STATE:]
    small, refs = refs[:SMALL], refs[SMALL:]
    gvec, vr_q, vc_q, vr_o, vc_o, vr_u, vc_u, vr_d, vc_d, v_old = small
    own_u, own_q, own_o, own_d, rr_u, rr_q, rr_o, rr_d, cs, rxa, ryb, r2a, r2b, ff, fs, *refs = refs
    ck, cg, co, cd, rs, late, rrx, lrx, rv, vco, trx, t2rx, table, vd_pad, vec_a, vec_b, vec_c, vec_rx, vec_full, *refs = refs
    own_sem, d_send, d_recv, s1_send, s1_recv, s2_send, s2_recv, f_send, f_recv, *refs = refs
    c_send, c_recv, r_sem, t_sem, v_send, v_recv, hello_sem = refs
    f = lax.axis_index("fsdp")
    z = lax.axis_index("tp")
    c, x, y = f % PAIR, (f // PAIR) % PAIR, f // GROUP
    xn, yn, cn = 1 - x, 1 - y, 1 - c
    f_c, f_x, f_y = f + 1 - PAIR * c, f + PAIR - GROUP * x, f + GROUP - BAND * y
    me = z * BAND + f
    flip_f = [
        f + (j % PAIR) * (1 - PAIR * c) + (j // PAIR % PAIR) * (PAIR - GROUP * x) + j // GROUP * (GROUP - BAND * y)
        for j in range(BAND)
    ]
    flip_z = [z, z + 1 - PAIR * (z % PAIR), z + PAIR - GROUP * (z // PAIR), tp_size - 1 - z][:tp_size]
    z_near = (z - 1 + (tp_size - 1 - z) // (tp_size - 1), z + 1 - z // (tp_size - 1))
    far_first = sorted(
        range(1, tp_size * BAND), key=lambda m: -(m // BAND + m // GROUP % PAIR + m // PAIR % PAIR)
    )
    devices = tp_size * BAND

    def remote(src, dst, send, recv, **device):
        return pltpu.make_async_remote_copy(
            src_ref=src, dst_ref=dst, send_sem=send, recv_sem=recv, device_id=device, device_id_type=MESH
        )

    def wait_bytes(ref, sem):
        pltpu.make_async_copy(ref, ref, sem).wait()

    def source(k, n, group):
        if n < PAIR:
            return gu.at[pl.ds(GROUP * group + PAIR * n, PAIR)], own_u.at[PAIR * n : PAIR * n + PAIR], rr_u.at[PAIR * n : PAIR * n + PAIR]
        if n == PAIR:
            return gq.at[pl.ds(pl.multiple_of(1152 * group, BAND), 1152)], own_q, rr_q
        if n == TILES:
            return go.at[pl.ds(pl.multiple_of(DIM * group, BAND), DIM)], own_o, rr_o
        return gd.at[pl.ds(pl.multiple_of(DIM * group, BAND), DIM)], own_d, rr_d

    def own_copy(k, n):
        src, dst, _ = source(k, n, PAIR * k + c)
        return pltpu.make_async_copy(src, dst, own_sem.at[n])

    def core_copy(k, n):
        src, _, dst = source(k, n, PAIR * k + cn)
        return remote(src, dst, d_send.at[n], d_recv.at[n], fsdp=f_c)

    def s1_copies(p):
        slot, sems = p % SLOTS, (s1_send.at[p % IN_FLIGHT], s1_recv.at[p % IN_FLIGHT])
        return (
            remote(cs.at[slot, :, xn, 0:TILES], rxa.at[p], *sems, fsdp=f_x),
            remote(cs.at[slot, yn, :, TILES:UNITS], ryb.at[p], *sems, fsdp=f_y),
        )

    def s2_copies(p):
        sems = (s2_send.at[p % IN_FLIGHT], s2_recv.at[p % IN_FLIGHT])
        return (
            remote(rxa.at[p, yn], r2a.at[p], *sems, fsdp=f_y),
            remote(ryb.at[p, xn], r2b.at[p], *sems, fsdp=f_x),
        )

    def final_copy(p):
        return remote(fs.at[p], ff.at[c, p], f_send.at[p % IN_FLIGHT], f_recv.at[p % IN_FLIGHT], fsdp=f_c)

    own_copy(0, 0).start()
    idle_sems = [sems.at[n] for sems in (s2_send, f_send, c_send) for n in range(GROUP)]
    small_copies = [pltpu.make_async_copy(small_hbm[n], small[n], idle_sems[n]) for n in range(SMALL)]
    for copy in small_copies:
        copy.start()

    barrier = pltpu.get_barrier_semaphore()

    def signal_near(sem):
        for other in z_near:
            pl.semaphore_signal(sem, inc=1, device_id={"tp": other}, device_id_type=MESH)

    for other in (f_c, f_x, f_y):
        pl.semaphore_signal(barrier, inc=1, device_id={"fsdp": other}, device_id_type=MESH)
    signal_near(barrier)
    pl.semaphore_wait(barrier, SOURCES)

    def first_copies(xa, yb, sem):
        for layer, start, size in ((0, xa, CHIP), (0, PAIR + xa, CHIP), (1, PAIR * yb, PAIR * CHIP)):
            rows = pl.ds(pl.multiple_of(CHIP * start, BAND), size)
            remote(
                gu.at[GROUP * cn + layer, rows], rr_u.at[layer, rows], d_send.at[sem], d_recv.at[sem], fsdp=f_c
            ).start()

    first_copies(xn, yn, 0)
    first_copies(x, y, SOURCES)
    core_copy(0, 1).start()
    own_copy(0, 1).start()

    own_half = pl.ds(pl.multiple_of(BAND * c, BAND), BAND)
    other_half = pl.ds(pl.multiple_of(BAND * cn, BAND), BAND)
    vec_copies = (
        remote(gvec.at[other_half], vec_rx.at[0], v_send.at[0], v_recv.at[0], fsdp=f_c),
        remote(vec_a, vec_rx.at[1], v_send.at[0], v_recv.at[1], fsdp=f_x),
        remote(vec_b, vec_rx.at[PAIR], v_send.at[0], v_recv.at[PAIR], fsdp=f_y),
        remote(vec_c, vec_full.at[own_half], v_send.at[0], v_recv.at[TILES], fsdp=f_c),
    )

    def vec_step(n):
        if n > 0:
            vec_copies[n - 1].wait_recv()
            vec_copies[n - 1].wait_send()
        if n == 1:
            vec_a[...] = gvec[own_half] + vec_rx[0]
        elif n == PAIR:
            vec_b[...] = vec_a[...] + vec_rx[1]
        elif n == TILES:
            total = vec_b[...] + vec_rx[PAIR]
            vec_c[...] = total
            vec_full[own_half] = total
        if n < GROUP:
            vec_copies[n].start()

    def prepare_small():
        for copy in small_copies:
            copy.wait()
        vec_step(0)
        rs[...] = jnp.zeros((ROWS, LANES), F32)
        late[...] = jnp.zeros((BAND, LANES), F32)
        ck[1, 7] = jnp.zeros((BAND, LANES), F32)
        vco[...] = jnp.zeros((LANES, LANES), F32)
        table[...] = jnp.zeros((LANES, LANES), F32)
        vd_pad[...] = jnp.zeros((LAYERS, 256), F32)
        vd_pad[:, 0:192] = vr_d[...]
        for k in range(PAIR):
            rows = slice(BAND * k, BAND * k + BAND)
            for t, (name, tile, width) in enumerate(COLUMN_TILES):
                ref = {"u": vc_u, "q": vc_q, "o": vc_o, "d": vc_d}[name]
                row = HALF * k + BAND * t
                vco[row : row + BAND, 0:width] = ref[rows, LANES * tile : LANES * tile + width]
            for s, ref in enumerate((vr_u, vr_q, vr_o)):
                table[HALF * k + BAND * s : HALF * k + BAND * s + BAND, 0:ROWS] = ref[rows, :]
            tiles = (vd_pad[rows, 0:LANES], vd_pad[rows, LANES:256])
            for b in range(GROUP):
                table[HALF * k + 24 + BAND * b : HALF * k + 32 + BAND * b, :] = shifted(tiles, ROWS * b, ROWS)
        rv[...] = jnp.transpose(table[...])[0:ROWS, :]

    def pack_up(k, half, slot):
        def body(h, carry):
            q, core = h // PAIR, h % PAIR
            rows = pl.ds(pl.multiple_of(ROWS * h, BAND), ROWS)
            for i in range(PAIR):
                for t in range(TILES):
                    lanes = slice(LANES * t, LANES * t + LANES)
                    cs[slot, q // PAIR, q % PAIR, TILES * i + t, core] = (
                        own_u[PAIR * half + i, rows, lanes] + rr_u[PAIR * half + i, rows, lanes]
                    )
            return carry

        lax.fori_loop(0, BAND, body, 0)

    def pack_flat(own, other, slot, first, count, unit):
        def body(n, carry):
            rows = pl.ds(pl.multiple_of(LANES * (first + n), LANES), LANES)
            for block in range(TILES):
                lanes = slice(LANES * block, LANES * block + LANES)
                value = jnp.transpose(own[rows, lanes] + other[rows, lanes])
                for h, row, here, size in row_parts(block):
                    cs[slot, h // GROUP, (h // PAIR) % PAIR, unit + n, h % PAIR, row : row + size, :] = value[here : here + size]
            return carry

        lax.fori_loop(0, count, body, 0)

    def pack_down(k, slot):
        def body(n, carry):
            q, t = n // TILES, n % TILES
            rows = pl.ds(pl.multiple_of(LANES * t, LANES), LANES)
            for block in range(TILES):
                lanes = pl.ds(pl.multiple_of(DIM * q + LANES * block, LANES), LANES)
                value = jnp.transpose(own_d[rows, lanes] + rr_d[rows, lanes])
                for h, row, here, size in row_parts(block):
                    core, b = h // GROUP, h % GROUP
                    cs[slot + b // PAIR, q // PAIR, q % PAIR, TILES * (b % PAIR) + t, core, row : row + size, :] = value[
                        here : here + size
                    ]
            return carry

        lax.fori_loop(0, 12, body, 0)

    def pack_first(xa, yb):
        def body(n, carry):
            part, core = n // PAIR, n % PAIR
            for i, q in ((0, PAIR * part + xa), (1, PAIR * yb + part)):
                rows = pl.ds(pl.multiple_of(CHIP * q + ROWS * core, BAND), ROWS)
                for t in range(TILES):
                    lanes = slice(LANES * t, LANES * t + LANES)
                    cs[0, q // PAIR, q % PAIR, TILES * i + t, core] = own_u[i, rows, lanes] + rr_u[i, rows, lanes]
            return carry

        lax.fori_loop(0, GROUP, body, 0)

    def prepare_first():
        own_copy(0, 0).wait()
        wait_bytes(rr_u.at[0], d_recv.at[0])
        pack_first(xn, yn)
        for copy in s1_copies(0):
            copy.start()
        for n in (PAIR, TILES):
            core_copy(0, n).start()
        for n in (PAIR, TILES, GROUP):
            own_copy(0, n).start()
        wait_bytes(rr_u.at[0], d_recv.at[SOURCES])
        pack_first(x, y)
        own_copy(1, 0).start()

    def prepare(p):
        if p == 0:
            return prepare_first()
        k, n, slot = p // UNITS, p % UNITS, p % SLOTS
        needs = {0: (0,), 1: (1,), PAIR: (PAIR,), TILES: (TILES,), GROUP: (GROUP,), SOURCES: ()}[n]
        for source_index in needs:
            own_copy(k, source_index).wait()
            core_copy(k, source_index).wait_recv()
        if p >= IN_FLIGHT:
            wait_bytes(rxa.at[0:PAIR], s1_send.at[p % IN_FLIGHT])
        if n < PAIR:
            pack_up(k, n, slot)
        elif n == PAIR:
            pack_flat(own_q, rr_q, slot, 0, UNITS, 0)
        elif n == TILES:
            pack_flat(own_q, rr_q, slot, UNITS, TILES, 0)
            pack_flat(own_o, rr_o, slot, 0, TILES, TILES)
        elif n == GROUP:
            pack_down(k, slot)
        for copy in s1_copies(p):
            copy.start()
        if p == 1:
            core_copy(0, GROUP).start()
        if k == 0:
            reload = {0: (0,), 1: (1,), TILES: (PAIR, TILES), GROUP: (GROUP,)}.get(n, ())
            for source_index in reload:
                own_copy(1, source_index).start()
        for source_index in {GROUP: (0, 1), SOURCES: (PAIR, TILES), UNITS: (GROUP,)}.get(p, ()):
            if source_index == 0:
                for sem in (0, SOURCES):
                    wait_bytes(rr_u.at[0], d_send.at[sem])
            else:
                core_copy(0, source_index).wait_send()
            core_copy(1, source_index).start()

    def stage_two(p):
        slot = p % SLOTS
        wait_bytes(rxa.at[0:PAIR], s1_recv.at[p % IN_FLIGHT])

        def body(u, carry):
            for core in range(PAIR):
                rxa[p, yn, u, core] = rxa[p, yn, u, core] + cs[slot, yn, x, u, core]
                ryb[p, xn, u, core] = ryb[p, xn, u, core] + cs[slot, y, xn, TILES + u, core]
            return carry

        lax.fori_loop(0, TILES, body, 0)
        if p >= IN_FLIGHT:
            wait_bytes(r2a.at[0:PAIR], s2_send.at[p % IN_FLIGHT])
        for copy in s2_copies(p):
            copy.start()

    def stage_three(p):
        slot = p % SLOTS
        wait_bytes(r2a.at[0:PAIR], s2_recv.at[p % IN_FLIGHT])

        def body(u, carry):
            fs[p, u] = cs[slot, y, x, u, cn] + rxa[p, y, u, cn] + r2a[p, u, cn]
            fs[p, TILES + u] = cs[slot, y, x, TILES + u, cn] + ryb[p, x, u, cn] + r2b[p, u, cn]
            return carry

        if p >= IN_FLIGHT:
            final_copy(p - IN_FLIGHT).wait_send()
        lax.fori_loop(0, TILES, body, 0)
        final_copy(p).start()

        def body_own(u, carry):
            ff[c, p, u] = cs[slot, y, x, u, c] + rxa[p, y, u, c] + r2a[p, u, c]
            ff[c, p, TILES + u] = cs[slot, y, x, TILES + u, c] + ryb[p, x, u, c] + r2b[p, u, c]
            return carry

        lax.fori_loop(0, TILES, body_own, 0)
        if p % UNITS >= GROUP:
            finish_down(p // UNITS, p % PAIR, c)

    def keep(step_k, layer, tile, value, first=True):
        ut[layer, tile] = value
        square = value * value
        sums = jnp.sum(square, axis=0, keepdims=True)
        row = pl.ds(layer % BAND, 1)
        column = TILE_COL[tile]
        ref = cd.at[f] if step_k == 1 and column == 7 else ck.at[step_k, column]
        ref[row, :] = sums if first else ref[row, :] + sums
        return square

    def keep_rows(layer, slot, square):
        lane = HALF * (layer // BAND) + BAND * slot + layer % BAND
        sums = jnp.sum(square, axis=1, keepdims=True)
        rs[...] = jnp.where(lane_iota((ROWS, LANES)) == lane, sums, rs[...])

    def keep_rows_late(layer, b, square):
        sums = jnp.sum(square, axis=1, keepdims=True)
        lane, value = lane_iota((BAND, LANES)), late[...]
        for g in range(UNITS):
            here = lane == LAYERS * g + BAND * (b - PAIR) + layer % BAND
            value = jnp.where(here, sums[BAND * g : BAND * g + BAND], value)
        late[...] = value

    def late_group(value, g):
        lane = lane_iota(value.shape)
        value = pltpu.roll(value, (LATE - LAYERS * g) % LANES, 1)
        return jnp.where((lane >= LATE) & (lane < LATE + LAYERS), value, 0.0)

    def send_rows(ref, sem):
        for other in flip_z[:0:-1]:
            remote(ref.at[z], ref.at[z], r_sem.at[sem], r_sem.at[sem + 1], tp=other).start()

    def finish_up(k):
        def body(i8, carry):
            core, i = i8 // GROUP, i8 % GROUP
            layer = BAND * k + i8
            square = [keep(k, layer, t, ff[core, UNITS * k + i // PAIR, TILES * (i % PAIR) + t]) for t in range(TILES)]
            keep_rows(layer, 0, square[0] + square[1] + square[PAIR])
            return carry

        lax.fori_loop(0, BAND, body, 0)

    def finish_qkv(k):
        def body(core, carry):
            tiles = [ff.at[core, UNITS * k + PAIR + t // UNITS, t % UNITS] for t in range(12)]
            for i in range(GROUP):
                layer = BAND * k + GROUP * core + i
                first = PAIR * i
                part = [tiles[t][...] for t in range(first, min(first + GROUP, 9))]
                square = [
                    keep(k, layer, TILES + t, shifted(part, 32 * i + LANES * t, LANES if t < PAIR else 32)) for t in range(TILES)
                ]
                keep_rows(layer, 1, square[0] + square[1] + square[PAIR])
                part = [tiles[9 + t][...] for t in range(TILES)]
                keep_rows(layer, PAIR, keep(k, layer, UNITS, shifted(part, CHIP * i, CHIP)))
            return carry

        lax.fori_loop(0, PAIR, body, 0)

    def finish_down(k, half, core):
        for b in (PAIR * half, PAIR * half + 1):
            part = [ff[core, UNITS * k + GROUP + half, TILES * (b % PAIR) + t] for t in range(TILES)]
            for i in range(GROUP):
                layer = BAND * k + GROUP * core + i
                square = keep(k, layer, 7 + b, shifted(part, CHIP * i, CHIP), first=b == 0)
                if k == 1 and half == 1:
                    keep_rows_late(layer, b, square)
                else:
                    keep_rows(layer, TILES + b, square)

    def columns_to_owner(k):
        for other in flip_f[:0:-1]:
            remote(ck.at[k, other], cg.at[k, f], c_send.at[PAIR * k], c_recv.at[PAIR * k], fsdp=other).start()
        cg[k, f] = ck[k, f]

    def columns_to_all(k):
        sem = PAIR * k + 1
        wait_bytes(cg.at[k, 0:7], c_recv.at[PAIR * k])
        total = cg[k, 0]
        for other in range(1, BAND):
            total = total + cg[k, other]
        co[k, f] = total
        for other in flip_f[:0:-1]:
            remote(co.at[k, f], co.at[k, f], c_send.at[sem], c_recv.at[sem], fsdp=other).start()

    def last_columns():
        for other in flip_f[:0:-1]:
            remote(cd.at[f], cd.at[f], c_send.at[GROUP], c_recv.at[GROUP], fsdp=other).start()

    def finish(p):
        k, n = p // UNITS, p % UNITS
        final_copy(p).wait_recv()
        if n == 1:
            finish_up(k)
        elif n == TILES:
            finish_qkv(k)
            if k == 1:
                columns_to_owner(k)
        elif n >= GROUP:
            finish_down(k, n % PAIR, cn)
            if n == SOURCES:
                columns_to_owner(k) if k == 0 else last_columns()
            elif k == 1:
                rrx[z] = rs[...]
                send_rows(rrx, 0)

    def send_all(ref, sems):
        for m in far_first:
            device = {"tp": flip_z[m // BAND], "fsdp": flip_f[m % BAND]}
            remote(ref.at[me], ref.at[me], sems.at[0], sems.at[1], **device).start()

    state_sems = [sems.at[n] for sems in (own_sem, d_recv) for n in range(SOURCES)]
    state_copies = [pltpu.make_async_copy(state_hbm[n], state[n], state_sems[n]) for n in range(STATE)]

    def prepare_totals():
        square = vec_full[...] * vec_full[...]
        vec_total = jnp.sum(jnp.sum(square, axis=1, keepdims=True), axis=0, keepdims=True)
        trx[me, :, LANES : PAIR * LANES] = jnp.sum(rv[...], axis=0, keepdims=True)
        trx[me, :, PAIR * LANES : TILES * LANES] = jnp.broadcast_to(vec_total, (1, LANES))

    def send_totals():
        lane = lane_iota((1, LANES))
        total = jnp.sum(rs[...], axis=0, keepdims=True)
        late_sum = jnp.sum(late[...], axis=0, keepdims=True)
        for g in range(UNITS):
            total = total + late_group(late_sum, g)
        for i in range(GROUP):
            square = None
            for b in range(PAIR):
                value = shifted([fs[PIECES - 1, TILES * b + t] for t in range(TILES)], CHIP * i, CHIP)
                square = value * value if square is None else square + value * value
            sums = jnp.sum(jnp.sum(square, axis=0, keepdims=True), axis=1, keepdims=True)
            total = total + jnp.where(lane == HALF + BAND * TILES + GROUP * c + i, sums, 0.0)
        trx[me, :, 0:LANES] = total
        send_all(trx, t_sem)

    for step in range(PIECES + TILES):
        for lag, part in ((0, prepare), (1, stage_two), (TILES, finish), (PAIR, stage_three)):
            if 0 <= step - lag < PIECES:
                with jax.named_scope(f"{part.__name__}_{step - lag}"):
                    part(step - lag)
        if step == 0:
            prepare_small()
        if step in (1, TILES, SOURCES, 7):
            vec_step((step + 1) // PAIR)
        if step in (PAIR, GROUP):
            signal_near(hello_sem.at[step // GROUP])
        if step in (TILES, SOURCES):
            pl.semaphore_wait(hello_sem.at[step // SOURCES], PAIR)
        if step == 10:
            columns_to_all(0)
            prepare_totals()
        if step == PIECES - 1:
            for copy in state_copies:
                copy.start()
        if step == PIECES + 1:
            send_totals()

    lrx[z] = late[...]
    send_rows(lrx, PAIR)
    columns_to_all(1)
    wait_bytes(trx.at[0 : devices - 1], t_sem.at[1])
    totals = jnp.sum(trx[...], axis=0)
    square_sum = totals[:, 0:LANES]
    old_sum = totals[:, LANES:256] * (1.0 / tp_size)
    vec_part = totals[:, 256:257] * 0.125
    total = jnp.sum(square_sum, axis=1, keepdims=True) + vec_part
    clip = jnp.minimum(1.0, 1.0 / jnp.sqrt(total))

    def clipped(value):
        return jnp.where(clip > 0.0, clip * (clip * value), 0.0)

    slot = (lane_iota((1, LANES)) // BAND) % BAND
    row_inv = jnp.where(slot >= TILES, 1.0 / 1536.0, 1.0 / 384.0).astype(F32)
    col_inv = jnp.where(
        slot == 0, 1.0 / (384.0 * tp_size), jnp.where(slot == 1, 1.0 / (288.0 * tp_size), 1.0 / (96.0 * tp_size))
    ).astype(F32)
    mean_new = BETA_TWO * (sum_down(old_sum) * row_inv) + (1.0 - BETA_TWO) * (
        clipped(sum_down(square_sum)) * (row_inv * col_inv) + EPSILON
    )
    wait_bytes(rrx.at[0 : tp_size - 1], r_sem.at[1])
    wait_bytes(lrx.at[0 : tp_size - 1], r_sem.at[TILES])
    row_sum, late_sum = jnp.sum(rrx[...], axis=0), jnp.sum(lrx[...], axis=0)
    row_sum = row_sum + jnp.concatenate([late_group(late_sum, g) for g in range(UNITS)], axis=0)
    row_new = BETA_TWO * rv[...] + (1.0 - BETA_TWO) * (clipped(row_sum) * col_inv + EPSILON)
    rv[...] = clip * lax.rsqrt(row_new / mean_new)
    rs[...] = row_new

    for k in range(PAIR):
        wait_bytes(co.at[k, 0:7], c_recv.at[PAIR * k + 1])
    wait_bytes(cd.at[0:7], c_recv.at[GROUP])
    last_sum = cd[0]
    for other in range(1, BAND):
        last_sum = last_sum + cd[other]
    wait_bytes(cd.at[0:7], c_send.at[TILES])
    co[1, 7] = last_sum
    col_sum = co[...].reshape(LANES, LANES)
    down_row = (lax.broadcasted_iota(jnp.int32, (LANES, LANES), 0) // BAND) % BAND == 7
    col_new = BETA_TWO * vco[...] + (1.0 - BETA_TWO) * (
        clipped(col_sum) * jnp.where(down_row, 1.0 / 1536.0, 1.0 / 384.0).astype(F32) + EPSILON
    )
    vc_new[...] = col_new
    vco[...] = lax.rsqrt(col_new)

    vec_grad = vec_full[...] * clip
    vec_var = BETA_TWO * v_old[...] + (1.0 - BETA_TWO) * (vec_grad * vec_grad + EPSILON)
    v_new[...] = vec_var
    vec_update = vec_grad / jnp.sqrt(vec_var)
    u_vec[...] = vec_update
    vec_rows = jnp.sum(vec_update * vec_update, axis=1, keepdims=True) * (0.125 / 128.0)
    vec_rows = jnp.broadcast_to(vec_rows, (LAYERS, LANES))
    table[56:HALF, :] = vec_rows[0:BAND]
    table[120:LANES, :] = vec_rows[BAND:LAYERS]

    def update(layer, carry):
        index = HALF * (layer // BAND) + layer % BAND
        lane = lane_iota((ROWS, LANES))
        factors = rv[...]
        tile = 0
        for s in range(7):
            row = jnp.sum(jnp.where(lane == index + BAND * s, factors, 0.0), axis=1, keepdims=True)
            square = None
            while tile < 11 and TILE_SLOT[tile] == s:
                value = ut[layer, tile] * row * vco[pl.ds(index + BAND * TILE_COL[tile], 1), :]
                ut[layer, tile] = value
                square = value * value if square is None else square + value * value
                tile += 1
            table[pl.ds(index + BAND * s, 1), :] = jnp.sum(square, axis=0, keepdims=True)
        return carry

    lax.fori_loop(0, LAYERS, update, 0, unroll=PAIR)

    t2rx[me] = jnp.sum(jnp.transpose(table[...]), axis=0, keepdims=True)
    send_all(t2rx, t_sem.at[PAIR:GROUP])
    table[0:ROWS, :] = rs[...]
    vr_new[...] = jnp.transpose(table[...])
    wait_bytes(t2rx.at[0 : devices - 1], t_sem.at[TILES])
    update_sum = sum_down(jnp.sum(t2rx[...], axis=0))
    inverse = jnp.where(slot == 7, 1.0 / (1248.0 * tp_size), row_inv * col_inv).astype(F32)
    factor = (1.0 - MOMENTUM) / jnp.maximum(1.0, jnp.sqrt(update_sum * inverse))
    scale[...] = jnp.transpose(jnp.broadcast_to(factor, (LANES, LANES)))

    for copy in state_copies:
        copy.wait()
    for n in range(SOURCES):
        core_copy(1, n).wait_send()
    for n in (0, 1, PAIR, GROUP):
        wait_bytes(cd.at[0:7], c_send.at[n])
    for p in range(PIECES - IN_FLIGHT, PIECES):
        wait_bytes(rxa.at[0:PAIR], s1_send.at[p % IN_FLIGHT])
        wait_bytes(r2a.at[0:PAIR], s2_send.at[p % IN_FLIGHT])
        final_copy(p).wait_send()
    wait_bytes(rrx.at[0 : tp_size - 1], r_sem.at[0])
    wait_bytes(lrx.at[0 : tp_size - 1], r_sem.at[PAIR])
    wait_bytes(trx.at[0 : devices - 1], t_sem.at[0])
    wait_bytes(t2rx.at[0 : devices - 1], t_sem.at[PAIR])


def update_kernel(ut, vr_new, vc_new, scale, u_vec, v_new, w_q, w_o, w_u, w_d, w_v, m_q, m_o, m_u, m_d, m_v, *refs):
    outs, refs = refs[:OUTS], refs[OUTS:]
    buffers, sems = refs[:OUTS], refs[OUTS]
    wo_q, wo_o, wo_u, wo_d, wo_v, mo_q, mo_o, mo_u, mo_d, mo_v, *rest = buffers
    vr_q, vc_q, vr_o, vc_o, vr_u, vc_u, vr_d, vc_d, v_out = rest
    by_layer = [n for n in range(OUTS) if len(outs[n].shape) == TILES]
    copies = [pltpu.make_async_copy(buffers[n], outs[n], sems.at[n]) for n in range(OUTS)]

    def finish(update, weight, moment):
        moment_new = (MOMENTUM * moment.astype(F32) + update).astype(jnp.bfloat16)
        return (1.0 - LEARN_RATE * WEIGHT_DECAY) * weight - LEARN_RATE * moment_new.astype(F32), moment_new

    v_out[...] = v_new[...]
    for k in range(PAIR):
        rows = slice(BAND * k, BAND * k + BAND)
        for t in range(10):
            lanes = slice(LANES * t, min(LANES * t + LANES, VEC))
            factor = scale[HALF * k + 56 : HALF * k + HALF, 0 : lanes.stop - lanes.start]
            weight_new, moment_new = finish(u_vec[rows, lanes] * factor, w_v[rows, lanes], m_v[rows, lanes])
            wo_v[rows, lanes] = weight_new
            mo_v[rows, lanes] = moment_new
        for t, (name, tile, width) in enumerate(COLUMN_TILES):
            ref = {"u": vc_u, "q": vc_q, "o": vc_o, "d": vc_d}[name]
            row = HALF * k + BAND * t
            ref[rows, LANES * tile : LANES * tile + width] = vc_new[row : row + BAND, 0:width]
        for s, ref in enumerate((vr_u, vr_q, vr_o)):
            row = HALF * k + BAND * s
            ref[rows, :] = vr_new[row : row + BAND, 0:ROWS]
        b0, b1, b2, b3 = (vr_new[HALF * k + BAND * (TILES + b) : HALF * k + BAND * (GROUP + b), :] for b in range(GROUP))
        lane = lane_iota((BAND, LANES))
        b2 = pltpu.roll(b2, CHIP, 1)
        vr_d[rows, 0:LANES] = jnp.where(lane < ROWS, b0, jnp.where(lane < CHIP, pltpu.roll(b1, ROWS, 1), b2))
        vr_d[rows, LANES:192] = jnp.where(lane < LAYERS, b2, pltpu.roll(b3, LAYERS, 1))[:, 0:HALF]
    for n in range(OUTS):
        if n not in by_layer:
            copies[n].start()

    def body(layer):
        index = HALF * (layer // BAND) + layer % BAND

        def one(tile, slot, w, m, wo, mo, rows, lanes):
            factor = scale[pl.ds(index + BAND * slot, 1), :]
            update = (ut[layer, tile] * factor)[:, 0 : lanes.stop - lanes.start]
            weight_new, moment_new = finish(update, w[layer, rows, lanes], m[layer, rows, lanes])
            wo[layer, rows, lanes] = weight_new
            mo[layer, rows, lanes] = moment_new

        every = slice(0, ROWS)
        for t in range(TILES):
            one(t, 0, w_u, m_u, wo_u, mo_u, every, slice(LANES * t, LANES * t + LANES))
            one(TILES + t, 1, w_q, m_q, wo_q, mo_q, every, slice(LANES * t, min(LANES * t + LANES, 288)))
        one(UNITS, PAIR, w_o, m_o, wo_o, mo_o, every, slice(0, CHIP))
        for b in range(GROUP):
            one(7 + b, TILES, w_d, m_d, wo_d, mo_d, slice(ROWS * b, ROWS * b + ROWS), slice(0, CHIP))

    def two_layers(i, carry):
        for layer in range(PAIR):
            body(PAIR * i + layer)
        layers = pl.ds(PAIR * i, PAIR)
        for n in by_layer:
            pltpu.make_async_copy(buffers[n].at[layers], outs[n].at[layers], sems.at[n]).start()
        return carry

    lax.fori_loop(0, BAND, two_layers, 0)
    for copy in copies:
        copy.wait()


def solution(mesh):
    tp_size = mesh.shape["tp"]
    devices = tp_size * mesh.shape["fsdp"]
    vmem = pl.BlockSpec(memory_space=pltpu.VMEM)
    hbm = pl.BlockSpec(memory_space=pltpu.HBM)

    def local_step(g_qkv, g_out, g_up, g_down, g_vec, w_qkv, w_out, w_up, w_down, w_vec, m_qkv, m_out, m_up, m_down, m_vec, vr_qkv, vc_qkv, vr_out, vc_out, vr_up, vc_up, vr_down, vc_down, v_vec):
        def flat(g):
            g = jnp.swapaxes(g[0], 1, PAIR)
            return g.reshape(g.shape[0] * g.shape[1], g.shape[PAIR])

        dma = pltpu.SemaphoreType.DMA
        half = (BAND, VEC)
        small = (g_vec[0], vr_qkv, vc_qkv, vr_out, vc_out, vr_up, vc_up, vr_down, vc_down, v_vec)
        weights = (w_qkv, w_out, w_up, w_down, w_vec)
        moments = (m_qkv, m_out, m_up, m_down, m_vec)
        results = pl.pallas_call(
            functools.partial(reduce_kernel, tp_size),
            out_shape=[
                jax.ShapeDtypeStruct((LAYERS, 11, ROWS, LANES), F32),
                jax.ShapeDtypeStruct((LANES, LANES), F32),
                jax.ShapeDtypeStruct((LANES, LANES), F32),
                jax.ShapeDtypeStruct((LANES, LANES), F32),
                jax.ShapeDtypeStruct((LAYERS, VEC), F32),
                jax.ShapeDtypeStruct((LAYERS, VEC), F32),
            ]
            + [jax.ShapeDtypeStruct(a.shape, a.dtype) for a in weights + moments],
            in_specs=[hbm] * (GROUP + SMALL + STATE),
            out_specs=[vmem] * (UNITS + STATE),
            scratch_shapes=[pltpu.VMEM(a.shape, a.dtype) for a in small]
            + [
                pltpu.VMEM((GROUP, DIM, DIM), F32),
                pltpu.VMEM((1152, DIM), F32),
                pltpu.VMEM((DIM, DIM), F32),
                pltpu.VMEM((DIM, 1536), F32),
                pltpu.VMEM((GROUP, DIM, DIM), F32),
                pltpu.VMEM((1152, DIM), F32),
                pltpu.VMEM((DIM, DIM), F32),
                pltpu.VMEM((DIM, 1536), F32),
                pltpu.VMEM((SLOTS, PAIR, PAIR, UNITS, PAIR, ROWS, LANES), F32),
                pltpu.VMEM((PIECES, PAIR, TILES, PAIR, ROWS, LANES), F32),
                pltpu.VMEM((PIECES, PAIR, TILES, PAIR, ROWS, LANES), F32),
                pltpu.VMEM((PIECES, TILES, PAIR, ROWS, LANES), F32),
                pltpu.VMEM((PIECES, TILES, PAIR, ROWS, LANES), F32),
                pltpu.VMEM((PAIR, PIECES, UNITS, ROWS, LANES), F32),
                pltpu.VMEM((PIECES, UNITS, ROWS, LANES), F32),
                pltpu.VMEM((PAIR, BAND, BAND, LANES), F32),
                pltpu.VMEM((PAIR, BAND, BAND, LANES), F32),
                pltpu.VMEM((PAIR, BAND, BAND, LANES), F32),
                pltpu.VMEM((BAND, BAND, LANES), F32),
                pltpu.VMEM((ROWS, LANES), F32),
                pltpu.VMEM((BAND, LANES), F32),
                pltpu.VMEM((tp_size, ROWS, LANES), F32),
                pltpu.VMEM((tp_size, BAND, LANES), F32),
                pltpu.VMEM((ROWS, LANES), F32),
                pltpu.VMEM((LANES, LANES), F32),
                pltpu.VMEM((devices, 1, DIM), F32),
                pltpu.VMEM((devices, 1, LANES), F32),
                pltpu.VMEM((LANES, LANES), F32),
                pltpu.VMEM((LAYERS, 256), F32),
                pltpu.VMEM(half, F32),
                pltpu.VMEM(half, F32),
                pltpu.VMEM(half, F32),
                pltpu.VMEM((TILES,) + half, F32),
                pltpu.VMEM((LAYERS, VEC), F32),
                dma((SOURCES,)),
                dma((UNITS,)), dma((UNITS,)),
                dma((IN_FLIGHT,)), dma((IN_FLIGHT,)),
                dma((IN_FLIGHT,)), dma((IN_FLIGHT,)),
                dma((IN_FLIGHT,)), dma((IN_FLIGHT,)),
                dma((SOURCES,)), dma((SOURCES,)),
                dma((GROUP,)), dma((GROUP,)),
                dma((1,)), dma((GROUP,)),
                pltpu.SemaphoreType.REGULAR((PAIR,)),
            ],
            compiler_params=pltpu.CompilerParams(
                collective_id=0, has_side_effects=True, vmem_limit_bytes=40 * 1024 * 1024
            ),
            name="reduce",
        )(*[pltpu.with_memory_space_constraint(a, pltpu.HBM) for a in (flat(g_qkv), flat(g_out), g_up[0], flat(g_down)) + small + weights + moments])

        outs = weights + moments + small[1:]
        return tuple(
            pl.pallas_call(
                update_kernel,
                out_shape=[jax.ShapeDtypeStruct(a.shape, a.dtype) for a in outs],
                in_specs=[vmem] * len(results),
                out_specs=[hbm] * OUTS,
                scratch_shapes=[pltpu.VMEM(a.shape, a.dtype) for a in outs] + [dma((OUTS,))],
                compiler_params=pltpu.CompilerParams(vmem_limit_bytes=24 * 1024 * 1024),
                name="update",
            )(*results)
        )

    grad_spec = P("fsdp", None, None, "tp")
    vec_grad_spec = P("fsdp", None, "tp")
    mat_spec = P(None, "fsdp", "tp")
    vec_spec = P(None, "tp")
    row_spec = P(None, "fsdp")
    state_specs = (mat_spec,) * GROUP + (vec_spec,) + (mat_spec,) * GROUP + (vec_spec,) + (row_spec, vec_spec) * GROUP + (vec_spec,)
    arg_specs = (grad_spec,) * GROUP + (vec_grad_spec,) + state_specs
    return jax.shard_map(local_step, mesh=mesh, in_specs=arg_specs, out_specs=state_specs, check_vma=False)
```

```python
import functools

import jax
import jax.numpy as jnp
from jax import lax
from jax.experimental import pallas as pl
from jax.experimental.pallas import tpu as pltpu
from jax.sharding import PartitionSpec as P

TRAIN_STEP = 3
LEARN_RATE = 0.0008
WEIGHT_DECAY = 0.03
MOMENTUM = 0.9
EPSILON = 1e-30
BETA_TWO = 1.0 - TRAIN_STEP ** -0.8

MESH = pl.DeviceIdType.MESH
F32 = jnp.float32
LAYERS = 16
TILES = 3
PAIR = 2
GROUP = 4
OUTS = 19
STATE = 10
SMALL = 10
SOURCES = 5
UNITS = 6
BAND = 8
ROWS = 48
HALF = 64
CHIP = 96
LANES = 128
DIM = 384
VEC = 1248
PIECES = 12
LATE = 104
IN_FLIGHT = 4
SLOTS = 6
TILE_SLOT = (0, 0, 0, 1, 1, 1, 2, 3, 4, 5, 6)
COLUMN_TILES = (
    ("u", 0, LANES), ("u", 1, LANES), ("u", PAIR, LANES),
    ("q", 0, LANES), ("q", 1, LANES), ("q", PAIR, 32), ("o", 0, CHIP), ("d", 0, CHIP),
)
TILE_COL = (0, 1, 2, 3, 4, 5, 6, 7, 7, 7, 7)


def row_parts(block):
    parts, row = [], LANES * block
    while row < LANES * block + LANES:
        stop = min((row // ROWS + 1) * ROWS, LANES * block + LANES)
        parts.append((row // ROWS, row % ROWS, row - LANES * block, stop - row))
        row = stop
    return parts


def lane_iota(shape):
    return lax.broadcasted_iota(jnp.int32, shape, len(shape) - 1)


def shifted(tiles, start, width):
    base, shift = start // LANES, start % LANES
    value = tiles[base] if shift == 0 else pltpu.roll(tiles[base], LANES - shift, 1)
    lane = lane_iota(value.shape)
    if shift + width > LANES:
        value = jnp.where(lane < LANES - shift, value, pltpu.roll(tiles[base + 1], LANES - shift, 1))
    return value if width == LANES else jnp.where(lane < width, value, 0.0)


def sum_down(value):
    slot = (lane_iota(value.shape) // BAND) % BAND
    part = jnp.where((slot >= TILES) & (slot <= UNITS), value, 0.0)
    total = part + pltpu.roll(part, BAND, 1) + pltpu.roll(part, LAYERS, 1) + pltpu.roll(part, 24, 1)
    total = jnp.where(slot == UNITS, total, 0.0)
    total = total + pltpu.roll(total, 120, 1) + pltpu.roll(total, 112, 1) + pltpu.roll(total, 104, 1)
    return jnp.where((slot >= TILES) & (slot <= UNITS), total, value)


def reduce_kernel(tp_size, gq, go, gu, gd, *refs):
    small_hbm, refs = refs[:SMALL], refs[SMALL:]
    state_hbm, refs = refs[:STATE], refs[STATE:]
    ut, vr_new, vc_new, scale, u_vec, v_new, *refs = refs
    state, refs = refs[:STATE], refs[STATE:]
    small, refs = refs[:SMALL], refs[SMALL:]
    gvec, vr_q, vc_q, vr_o, vc_o, vr_u, vc_u, vr_d, vc_d, v_old = small
    own_u, own_q, own_o, own_d, rr_u, rr_q, rr_o, rr_d, cs, rxa, ryb, r2a, r2b, ff, fs, *refs = refs
    ck, cg, co, cd, rs, late, rrx, lrx, rv, vco, trx, t2rx, table, vd_pad, vec_a, vec_b, vec_c, vec_rx, vec_full, *refs = refs
    own_sem, d_send, d_recv, s1_send, s1_recv, s2_send, s2_recv, f_send, f_recv, *refs = refs
    c_send, c_recv, r_sem, t_sem, v_send, v_recv, hello_sem = refs
    f = lax.axis_index("fsdp")
    z = lax.axis_index("tp")
    c, x, y = f % PAIR, (f // PAIR) % PAIR, f // GROUP
    xn, yn, cn = 1 - x, 1 - y, 1 - c
    f_c, f_x, f_y = f + 1 - PAIR * c, f + PAIR - GROUP * x, f + GROUP - BAND * y
    me = z * BAND + f
    flip_f = [
        f + (j % PAIR) * (1 - PAIR * c) + (j // PAIR % PAIR) * (PAIR - GROUP * x) + j // GROUP * (GROUP - BAND * y)
        for j in range(BAND)
    ]
    flip_z = [z, z + 1 - PAIR * (z % PAIR), z + PAIR - GROUP * (z // PAIR), tp_size - 1 - z][:tp_size]
    z_near = (z - 1 + (tp_size - 1 - z) // (tp_size - 1), z + 1 - z // (tp_size - 1))
    far_first = sorted(
        range(1, tp_size * BAND), key=lambda m: -(m // BAND + m // GROUP % PAIR + m // PAIR % PAIR)
    )
    devices = tp_size * BAND

    def remote(src, dst, send, recv, **device):
        return pltpu.make_async_remote_copy(
            src_ref=src, dst_ref=dst, send_sem=send, recv_sem=recv, device_id=device, device_id_type=MESH
        )

    def wait_bytes(ref, sem):
        pltpu.make_async_copy(ref, ref, sem).wait()

    def source(k, n, group):
        if n < PAIR:
            return gu.at[pl.ds(GROUP * group + PAIR * n, PAIR)], own_u.at[PAIR * n : PAIR * n + PAIR], rr_u.at[PAIR * n : PAIR * n + PAIR]
        if n == PAIR:
            return gq.at[pl.ds(pl.multiple_of(1152 * group, BAND), 1152)], own_q, rr_q
        if n == TILES:
            return go.at[pl.ds(pl.multiple_of(DIM * group, BAND), DIM)], own_o, rr_o
        return gd.at[pl.ds(pl.multiple_of(DIM * group, BAND), DIM)], own_d, rr_d

    def own_copy(k, n):
        src, dst, _ = source(k, n, PAIR * k + c)
        return pltpu.make_async_copy(src, dst, own_sem.at[n])

    def core_copy(k, n):
        src, _, dst = source(k, n, PAIR * k + cn)
        return remote(src, dst, d_send.at[n], d_recv.at[n], fsdp=f_c)

    def s1_copies(p):
        slot, sems = p % SLOTS, (s1_send.at[p % IN_FLIGHT], s1_recv.at[p % IN_FLIGHT])
        return (
            remote(cs.at[slot, :, xn, 0:TILES], rxa.at[p], *sems, fsdp=f_x),
            remote(cs.at[slot, yn, :, TILES:UNITS], ryb.at[p], *sems, fsdp=f_y),
        )

    def s2_copies(p):
        sems = (s2_send.at[p % IN_FLIGHT], s2_recv.at[p % IN_FLIGHT])
        return (
            remote(rxa.at[p, yn], r2a.at[p], *sems, fsdp=f_y),
            remote(ryb.at[p, xn], r2b.at[p], *sems, fsdp=f_x),
        )

    def final_copy(p):
        return remote(fs.at[p], ff.at[c, p], f_send.at[p % IN_FLIGHT], f_recv.at[p % IN_FLIGHT], fsdp=f_c)

    own_copy(0, 0).start()
    idle_sems = [sems.at[n] for sems in (s2_send, f_send, c_send) for n in range(GROUP)]
    small_copies = [pltpu.make_async_copy(small_hbm[n], small[n], idle_sems[n]) for n in range(SMALL)]
    for copy in small_copies:
        copy.start()

    barrier = pltpu.get_barrier_semaphore()

    def signal_near(sem):
        for other in z_near:
            pl.semaphore_signal(sem, inc=1, device_id={"tp": other}, device_id_type=MESH)

    for other in (f_c, f_x, f_y):
        pl.semaphore_signal(barrier, inc=1, device_id={"fsdp": other}, device_id_type=MESH)
    signal_near(barrier)
    pl.semaphore_wait(barrier, SOURCES)

    def first_copies(xa, yb, sem):
        for layer, start, size in ((0, xa, CHIP), (0, PAIR + xa, CHIP), (1, PAIR * yb, PAIR * CHIP)):
            rows = pl.ds(pl.multiple_of(CHIP * start, BAND), size)
            remote(
                gu.at[GROUP * cn + layer, rows], rr_u.at[layer, rows], d_send.at[sem], d_recv.at[sem], fsdp=f_c
            ).start()

    first_copies(xn, yn, 0)
    first_copies(x, y, SOURCES)
    core_copy(0, 1).start()
    own_copy(0, 1).start()

    own_half = pl.ds(pl.multiple_of(BAND * c, BAND), BAND)
    other_half = pl.ds(pl.multiple_of(BAND * cn, BAND), BAND)
    vec_copies = (
        remote(gvec.at[other_half], vec_rx.at[0], v_send.at[0], v_recv.at[0], fsdp=f_c),
        remote(vec_a, vec_rx.at[1], v_send.at[0], v_recv.at[1], fsdp=f_x),
        remote(vec_b, vec_rx.at[PAIR], v_send.at[0], v_recv.at[PAIR], fsdp=f_y),
        remote(vec_c, vec_full.at[own_half], v_send.at[0], v_recv.at[TILES], fsdp=f_c),
    )

    def vec_step(n):
        if n > 0:
            vec_copies[n - 1].wait_recv()
            vec_copies[n - 1].wait_send()
        if n == 1:
            vec_a[...] = gvec[own_half] + vec_rx[0]
        elif n == PAIR:
            vec_b[...] = vec_a[...] + vec_rx[1]
        elif n == TILES:
            total = vec_b[...] + vec_rx[PAIR]
            vec_c[...] = total
            vec_full[own_half] = total
        if n < GROUP:
            vec_copies[n].start()

    def prepare_small():
        for copy in small_copies:
            copy.wait()
        vec_step(0)
        rs[...] = jnp.zeros((ROWS, LANES), F32)
        late[...] = jnp.zeros((BAND, LANES), F32)
        ck[1, 7] = jnp.zeros((BAND, LANES), F32)
        vco[...] = jnp.zeros((LANES, LANES), F32)
        table[...] = jnp.zeros((LANES, LANES), F32)
        vd_pad[...] = jnp.zeros((LAYERS, 256), F32)
        vd_pad[:, 0:192] = vr_d[...]
        for k in range(PAIR):
            rows = slice(BAND * k, BAND * k + BAND)
            for t, (name, tile, width) in enumerate(COLUMN_TILES):
                ref = {"u": vc_u, "q": vc_q, "o": vc_o, "d": vc_d}[name]
                row = HALF * k + BAND * t
                vco[row : row + BAND, 0:width] = ref[rows, LANES * tile : LANES * tile + width]
            for s, ref in enumerate((vr_u, vr_q, vr_o)):
                table[HALF * k + BAND * s : HALF * k + BAND * s + BAND, 0:ROWS] = ref[rows, :]
            tiles = (vd_pad[rows, 0:LANES], vd_pad[rows, LANES:256])
            for b in range(GROUP):
                table[HALF * k + 24 + BAND * b : HALF * k + 32 + BAND * b, :] = shifted(tiles, ROWS * b, ROWS)
        rv[...] = jnp.transpose(table[...])[0:ROWS, :]

    def pack_up(k, half, slot):
        def body(h, carry):
            q, core = h // PAIR, h % PAIR
            rows = pl.ds(pl.multiple_of(ROWS * h, BAND), ROWS)
            for i in range(PAIR):
                for t in range(TILES):
                    lanes = slice(LANES * t, LANES * t + LANES)
                    cs[slot, q // PAIR, q % PAIR, TILES * i + t, core] = (
                        own_u[PAIR * half + i, rows, lanes] + rr_u[PAIR * half + i, rows, lanes]
                    )
            return carry

        lax.fori_loop(0, BAND, body, 0)

    def pack_flat(own, other, slot, first, count, unit):
        def body(n, carry):
            rows = pl.ds(pl.multiple_of(LANES * (first + n), LANES), LANES)
            for block in range(TILES):
                lanes = slice(LANES * block, LANES * block + LANES)
                value = jnp.transpose(own[rows, lanes] + other[rows, lanes])
                for h, row, here, size in row_parts(block):
                    cs[slot, h // GROUP, (h // PAIR) % PAIR, unit + n, h % PAIR, row : row + size, :] = value[here : here + size]
            return carry

        lax.fori_loop(0, count, body, 0)

    def pack_down(k, slot):
        def body(n, carry):
            q, t = n // TILES, n % TILES
            rows = pl.ds(pl.multiple_of(LANES * t, LANES), LANES)
            for block in range(TILES):
                lanes = pl.ds(pl.multiple_of(DIM * q + LANES * block, LANES), LANES)
                value = jnp.transpose(own_d[rows, lanes] + rr_d[rows, lanes])
                for h, row, here, size in row_parts(block):
                    core, b = h // GROUP, h % GROUP
                    cs[slot + b // PAIR, q // PAIR, q % PAIR, TILES * (b % PAIR) + t, core, row : row + size, :] = value[
                        here : here + size
                    ]
            return carry

        lax.fori_loop(0, 12, body, 0)

    def pack_first(xa, yb):
        def body(n, carry):
            part, core = n // PAIR, n % PAIR
            for i, q in ((0, PAIR * part + xa), (1, PAIR * yb + part)):
                rows = pl.ds(pl.multiple_of(CHIP * q + ROWS * core, BAND), ROWS)
                for t in range(TILES):
                    lanes = slice(LANES * t, LANES * t + LANES)
                    cs[0, q // PAIR, q % PAIR, TILES * i + t, core] = own_u[i, rows, lanes] + rr_u[i, rows, lanes]
            return carry

        lax.fori_loop(0, GROUP, body, 0)

    def prepare_first():
        own_copy(0, 0).wait()
        wait_bytes(rr_u.at[0], d_recv.at[0])
        pack_first(xn, yn)
        for copy in s1_copies(0):
            copy.start()
        for n in (PAIR, TILES, GROUP):
            own_copy(0, n).start()
        wait_bytes(rr_u.at[0], d_recv.at[SOURCES])
        pack_first(x, y)
        own_copy(1, 0).start()

    def prepare(p):
        if p == 0:
            return prepare_first()
        k, n, slot = p // UNITS, p % UNITS, p % SLOTS
        needs = {0: (0,), 1: (1,), PAIR: (PAIR,), TILES: (TILES,), GROUP: (GROUP,), SOURCES: ()}[n]
        for source_index in needs:
            own_copy(k, source_index).wait()
            core_copy(k, source_index).wait_recv()
        if p >= IN_FLIGHT:
            wait_bytes(rxa.at[0:PAIR], s1_send.at[p % IN_FLIGHT])
        if n < PAIR:
            pack_up(k, n, slot)
        elif n == PAIR:
            pack_flat(own_q, rr_q, slot, 0, UNITS, 0)
        elif n == TILES:
            pack_flat(own_q, rr_q, slot, UNITS, TILES, 0)
            pack_flat(own_o, rr_o, slot, 0, TILES, TILES)
        elif n == GROUP:
            pack_down(k, slot)
        for copy in s1_copies(p):
            copy.start()
        for source_index in {1: (PAIR, TILES), PAIR: (GROUP,)}.get(p, ()):
            core_copy(0, source_index).start()
        if k == 0:
            reload = {0: (0,), 1: (1,), TILES: (PAIR, TILES), GROUP: (GROUP,)}.get(n, ())
            for source_index in reload:
                own_copy(1, source_index).start()
        for source_index in {GROUP: (0, 1), SOURCES: (PAIR, TILES), UNITS: (GROUP,)}.get(p, ()):
            if source_index == 0:
                for sem in (0, SOURCES):
                    wait_bytes(rr_u.at[0], d_send.at[sem])
            else:
                core_copy(0, source_index).wait_send()
            core_copy(1, source_index).start()

    def stage_two(p):
        slot = p % SLOTS
        wait_bytes(rxa.at[0:PAIR], s1_recv.at[p % IN_FLIGHT])

        def body(u, carry):
            for core in range(PAIR):
                rxa[p, yn, u, core] = rxa[p, yn, u, core] + cs[slot, yn, x, u, core]
                ryb[p, xn, u, core] = ryb[p, xn, u, core] + cs[slot, y, xn, TILES + u, core]
            return carry

        lax.fori_loop(0, TILES, body, 0)
        if p >= IN_FLIGHT:
            wait_bytes(r2a.at[0:PAIR], s2_send.at[p % IN_FLIGHT])
        for copy in s2_copies(p):
            copy.start()

    def stage_three(p):
        slot = p % SLOTS
        wait_bytes(r2a.at[0:PAIR], s2_recv.at[p % IN_FLIGHT])

        def body(u, carry):
            fs[p, u] = cs[slot, y, x, u, cn] + rxa[p, y, u, cn] + r2a[p, u, cn]
            fs[p, TILES + u] = cs[slot, y, x, TILES + u, cn] + ryb[p, x, u, cn] + r2b[p, u, cn]
            return carry

        if p >= IN_FLIGHT:
            final_copy(p - IN_FLIGHT).wait_send()
        lax.fori_loop(0, TILES, body, 0)
        final_copy(p).start()

        def body_own(u, carry):
            ff[c, p, u] = cs[slot, y, x, u, c] + rxa[p, y, u, c] + r2a[p, u, c]
            ff[c, p, TILES + u] = cs[slot, y, x, TILES + u, c] + ryb[p, x, u, c] + r2b[p, u, c]
            return carry

        lax.fori_loop(0, TILES, body_own, 0)
        if p % UNITS >= GROUP:
            finish_down(p // UNITS, p % PAIR, c)

    def keep(step_k, layer, tile, value, first=True):
        ut[layer, tile] = value
        square = value * value
        sums = jnp.sum(square, axis=0, keepdims=True)
        row = pl.ds(layer % BAND, 1)
        column = TILE_COL[tile]
        ref = cd.at[f] if step_k == 1 and column == 7 else ck.at[step_k, column]
        ref[row, :] = sums if first else ref[row, :] + sums
        return square

    def keep_rows(layer, slot, square):
        lane = HALF * (layer // BAND) + BAND * slot + layer % BAND
        sums = jnp.sum(square, axis=1, keepdims=True)
        rs[...] = jnp.where(lane_iota((ROWS, LANES)) == lane, sums, rs[...])

    def keep_rows_late(layer, b, square):
        sums = jnp.sum(square, axis=1, keepdims=True)
        lane, value = lane_iota((BAND, LANES)), late[...]
        for g in range(UNITS):
            here = lane == LAYERS * g + BAND * (b - PAIR) + layer % BAND
            value = jnp.where(here, sums[BAND * g : BAND * g + BAND], value)
        late[...] = value

    def late_group(value, g):
        lane = lane_iota(value.shape)
        value = pltpu.roll(value, (LATE - LAYERS * g) % LANES, 1)
        return jnp.where((lane >= LATE) & (lane < LATE + LAYERS), value, 0.0)

    def send_rows(ref, sem):
        for other in flip_z[:0:-1]:
            remote(ref.at[z], ref.at[z], r_sem.at[sem], r_sem.at[sem + 1], tp=other).start()

    def finish_up(k):
        def body(i8, carry):
            core, i = i8 // GROUP, i8 % GROUP
            layer = BAND * k + i8
            square = [keep(k, layer, t, ff[core, UNITS * k + i // PAIR, TILES * (i % PAIR) + t]) for t in range(TILES)]
            keep_rows(layer, 0, square[0] + square[1] + square[PAIR])
            return carry

        lax.fori_loop(0, BAND, body, 0)

    def finish_qkv(k):
        def body(core, carry):
            tiles = [ff.at[core, UNITS * k + PAIR + t // UNITS, t % UNITS] for t in range(12)]
            for i in range(GROUP):
                layer = BAND * k + GROUP * core + i
                first = PAIR * i
                part = [tiles[t][...] for t in range(first, min(first + GROUP, 9))]
                square = [
                    keep(k, layer, TILES + t, shifted(part, 32 * i + LANES * t, LANES if t < PAIR else 32)) for t in range(TILES)
                ]
                keep_rows(layer, 1, square[0] + square[1] + square[PAIR])
                part = [tiles[9 + t][...] for t in range(TILES)]
                keep_rows(layer, PAIR, keep(k, layer, UNITS, shifted(part, CHIP * i, CHIP)))
            return carry

        lax.fori_loop(0, PAIR, body, 0)

    def finish_down(k, half, core):
        for b in (PAIR * half, PAIR * half + 1):
            part = [ff[core, UNITS * k + GROUP + half, TILES * (b % PAIR) + t] for t in range(TILES)]
            for i in range(GROUP):
                layer = BAND * k + GROUP * core + i
                square = keep(k, layer, 7 + b, shifted(part, CHIP * i, CHIP), first=b == 0)
                if k == 1 and half == 1:
                    keep_rows_late(layer, b, square)
                else:
                    keep_rows(layer, TILES + b, square)

    def columns_to_owner(k):
        for other in flip_f[:0:-1]:
            remote(ck.at[k, other], cg.at[k, f], c_send.at[PAIR * k], c_recv.at[PAIR * k], fsdp=other).start()
        cg[k, f] = ck[k, f]

    def columns_to_all(k):
        sem = PAIR * k + 1
        wait_bytes(cg.at[k, 0:7], c_recv.at[PAIR * k])
        total = cg[k, 0]
        for other in range(1, BAND):
            total = total + cg[k, other]
        co[k, f] = total
        for other in flip_f[:0:-1]:
            remote(co.at[k, f], co.at[k, f], c_send.at[sem], c_recv.at[sem], fsdp=other).start()

    def last_columns():
        for other in flip_f[:0:-1]:
            remote(cd.at[f], cd.at[f], c_send.at[GROUP], c_recv.at[GROUP], fsdp=other).start()

    def finish(p):
        k, n = p // UNITS, p % UNITS
        final_copy(p).wait_recv()
        if n == 1:
            finish_up(k)
        elif n == TILES:
            finish_qkv(k)
            if k == 1:
                columns_to_owner(k)
        elif n >= GROUP:
            finish_down(k, n % PAIR, cn)
            if n == SOURCES:
                columns_to_owner(k) if k == 0 else last_columns()
            elif k == 1:
                rrx[z] = rs[...]
                send_rows(rrx, 0)

    def send_all(ref, sems):
        for m in far_first:
            device = {"tp": flip_z[m // BAND], "fsdp": flip_f[m % BAND]}
            remote(ref.at[me], ref.at[me], sems.at[0], sems.at[1], **device).start()

    state_sems = [sems.at[n] for sems in (own_sem, d_recv) for n in range(SOURCES)]
    state_copies = [pltpu.make_async_copy(state_hbm[n], state[n], state_sems[n]) for n in range(STATE)]

    def prepare_totals():
        square = vec_full[...] * vec_full[...]
        vec_total = jnp.sum(jnp.sum(square, axis=1, keepdims=True), axis=0, keepdims=True)
        trx[me, :, LANES : PAIR * LANES] = jnp.sum(rv[...], axis=0, keepdims=True)
        trx[me, :, PAIR * LANES : TILES * LANES] = jnp.broadcast_to(vec_total, (1, LANES))

    def send_totals():
        lane = lane_iota((1, LANES))
        total = jnp.sum(rs[...], axis=0, keepdims=True)
        late_sum = jnp.sum(late[...], axis=0, keepdims=True)
        for g in range(UNITS):
            total = total + late_group(late_sum, g)
        for i in range(GROUP):
            square = None
            for b in range(PAIR):
                value = shifted([fs[PIECES - 1, TILES * b + t] for t in range(TILES)], CHIP * i, CHIP)
                square = value * value if square is None else square + value * value
            sums = jnp.sum(jnp.sum(square, axis=0, keepdims=True), axis=1, keepdims=True)
            total = total + jnp.where(lane == HALF + BAND * TILES + GROUP * c + i, sums, 0.0)
        trx[me, :, 0:LANES] = total
        send_all(trx, t_sem)

    for step in range(PIECES + TILES):
        for lag, part in ((0, prepare), (1, stage_two), (TILES, finish), (PAIR, stage_three)):
            if 0 <= step - lag < PIECES:
                with jax.named_scope(f"{part.__name__}_{step - lag}"):
                    part(step - lag)
        if step == 0:
            prepare_small()
        if step in (1, TILES, SOURCES, 7):
            vec_step((step + 1) // PAIR)
        if step in (PAIR, GROUP):
            signal_near(hello_sem.at[step // GROUP])
        if step in (TILES, SOURCES):
            pl.semaphore_wait(hello_sem.at[step // SOURCES], PAIR)
        if step == 10:
            columns_to_all(0)
            prepare_totals()
        if step == PIECES - 1:
            for copy in state_copies:
                copy.start()
        if step == PIECES + 1:
            send_totals()

    lrx[z] = late[...]
    send_rows(lrx, PAIR)
    columns_to_all(1)
    wait_bytes(trx.at[0 : devices - 1], t_sem.at[1])
    totals = jnp.sum(trx[...], axis=0)
    square_sum = totals[:, 0:LANES]
    old_sum = totals[:, LANES:256] * (1.0 / tp_size)
    vec_part = totals[:, 256:257] * 0.125
    total = jnp.sum(square_sum, axis=1, keepdims=True) + vec_part
    clip = jnp.minimum(1.0, 1.0 / jnp.sqrt(total))

    def clipped(value):
        return jnp.where(clip > 0.0, clip * (clip * value), 0.0)

    slot = (lane_iota((1, LANES)) // BAND) % BAND
    row_inv = jnp.where(slot >= TILES, 1.0 / 1536.0, 1.0 / 384.0).astype(F32)
    col_inv = jnp.where(
        slot == 0, 1.0 / (384.0 * tp_size), jnp.where(slot == 1, 1.0 / (288.0 * tp_size), 1.0 / (96.0 * tp_size))
    ).astype(F32)
    mean_new = BETA_TWO * (sum_down(old_sum) * row_inv) + (1.0 - BETA_TWO) * (
        clipped(sum_down(square_sum)) * (row_inv * col_inv) + EPSILON
    )
    wait_bytes(rrx.at[0 : tp_size - 1], r_sem.at[1])
    wait_bytes(lrx.at[0 : tp_size - 1], r_sem.at[TILES])
    row_sum, late_sum = jnp.sum(rrx[...], axis=0), jnp.sum(lrx[...], axis=0)
    row_sum = row_sum + jnp.concatenate([late_group(late_sum, g) for g in range(UNITS)], axis=0)
    row_new = BETA_TWO * rv[...] + (1.0 - BETA_TWO) * (clipped(row_sum) * col_inv + EPSILON)
    rv[...] = clip * lax.rsqrt(row_new / mean_new)
    rs[...] = row_new

    for k in range(PAIR):
        wait_bytes(co.at[k, 0:7], c_recv.at[PAIR * k + 1])
    wait_bytes(cd.at[0:7], c_recv.at[GROUP])
    last_sum = cd[0]
    for other in range(1, BAND):
        last_sum = last_sum + cd[other]
    wait_bytes(cd.at[0:7], c_send.at[TILES])
    co[1, 7] = last_sum
    col_sum = co[...].reshape(LANES, LANES)
    down_row = (lax.broadcasted_iota(jnp.int32, (LANES, LANES), 0) // BAND) % BAND == 7
    col_new = BETA_TWO * vco[...] + (1.0 - BETA_TWO) * (
        clipped(col_sum) * jnp.where(down_row, 1.0 / 1536.0, 1.0 / 384.0).astype(F32) + EPSILON
    )
    vc_new[...] = col_new
    vco[...] = lax.rsqrt(col_new)

    vec_grad = vec_full[...] * clip
    vec_var = BETA_TWO * v_old[...] + (1.0 - BETA_TWO) * (vec_grad * vec_grad + EPSILON)
    v_new[...] = vec_var
    vec_update = vec_grad / jnp.sqrt(vec_var)
    u_vec[...] = vec_update
    vec_rows = jnp.sum(vec_update * vec_update, axis=1, keepdims=True) * (0.125 / 128.0)
    vec_rows = jnp.broadcast_to(vec_rows, (LAYERS, LANES))
    table[56:HALF, :] = vec_rows[0:BAND]
    table[120:LANES, :] = vec_rows[BAND:LAYERS]

    def update(layer, carry):
        index = HALF * (layer // BAND) + layer % BAND
        lane = lane_iota((ROWS, LANES))
        factors = rv[...]
        tile = 0
        for s in range(7):
            row = jnp.sum(jnp.where(lane == index + BAND * s, factors, 0.0), axis=1, keepdims=True)
            square = None
            while tile < 11 and TILE_SLOT[tile] == s:
                value = ut[layer, tile] * row * vco[pl.ds(index + BAND * TILE_COL[tile], 1), :]
                ut[layer, tile] = value
                square = value * value if square is None else square + value * value
                tile += 1
            table[pl.ds(index + BAND * s, 1), :] = jnp.sum(square, axis=0, keepdims=True)
        return carry

    lax.fori_loop(0, LAYERS, update, 0, unroll=GROUP)

    t2rx[me] = jnp.sum(jnp.transpose(table[...]), axis=0, keepdims=True)
    send_all(t2rx, t_sem.at[PAIR:GROUP])
    table[0:ROWS, :] = rs[...]
    vr_new[...] = jnp.transpose(table[...])
    wait_bytes(t2rx.at[0 : devices - 1], t_sem.at[TILES])
    update_sum = sum_down(jnp.sum(t2rx[...], axis=0))
    inverse = jnp.where(slot == 7, 1.0 / (1248.0 * tp_size), row_inv * col_inv).astype(F32)
    factor = (1.0 - MOMENTUM) / jnp.maximum(1.0, jnp.sqrt(update_sum * inverse))
    scale[...] = jnp.transpose(jnp.broadcast_to(factor, (LANES, LANES)))

    for copy in state_copies:
        copy.wait()
    for n in range(SOURCES):
        core_copy(1, n).wait_send()
    for n in (0, 1, PAIR, GROUP):
        wait_bytes(cd.at[0:7], c_send.at[n])
    for p in range(PIECES - IN_FLIGHT, PIECES):
        wait_bytes(rxa.at[0:PAIR], s1_send.at[p % IN_FLIGHT])
        wait_bytes(r2a.at[0:PAIR], s2_send.at[p % IN_FLIGHT])
        final_copy(p).wait_send()
    wait_bytes(rrx.at[0 : tp_size - 1], r_sem.at[0])
    wait_bytes(lrx.at[0 : tp_size - 1], r_sem.at[PAIR])
    wait_bytes(trx.at[0 : devices - 1], t_sem.at[0])
    wait_bytes(t2rx.at[0 : devices - 1], t_sem.at[PAIR])


def update_kernel(ut, vr_new, vc_new, scale, u_vec, v_new, w_q, w_o, w_u, w_d, w_v, m_q, m_o, m_u, m_d, m_v, *refs):
    outs, refs = refs[:OUTS], refs[OUTS:]
    buffers, sems = refs[:OUTS], refs[OUTS]
    wo_q, wo_o, wo_u, wo_d, wo_v, mo_q, mo_o, mo_u, mo_d, mo_v, *rest = buffers
    vr_q, vc_q, vr_o, vc_o, vr_u, vc_u, vr_d, vc_d, v_out = rest
    by_layer = [n for n in range(OUTS) if len(outs[n].shape) == TILES]
    copies = [pltpu.make_async_copy(buffers[n], outs[n], sems.at[n]) for n in range(OUTS)]

    def finish(update, weight, moment):
        moment_new = (MOMENTUM * moment.astype(F32) + update).astype(jnp.bfloat16)
        return (1.0 - LEARN_RATE * WEIGHT_DECAY) * weight - LEARN_RATE * moment_new.astype(F32), moment_new

    v_out[...] = v_new[...]
    for k in range(PAIR):
        rows = slice(BAND * k, BAND * k + BAND)
        for t in range(10):
            lanes = slice(LANES * t, min(LANES * t + LANES, VEC))
            factor = scale[HALF * k + 56 : HALF * k + HALF, 0 : lanes.stop - lanes.start]
            weight_new, moment_new = finish(u_vec[rows, lanes] * factor, w_v[rows, lanes], m_v[rows, lanes])
            wo_v[rows, lanes] = weight_new
            mo_v[rows, lanes] = moment_new
        for t, (name, tile, width) in enumerate(COLUMN_TILES):
            ref = {"u": vc_u, "q": vc_q, "o": vc_o, "d": vc_d}[name]
            row = HALF * k + BAND * t
            ref[rows, LANES * tile : LANES * tile + width] = vc_new[row : row + BAND, 0:width]
        for s, ref in enumerate((vr_u, vr_q, vr_o)):
            row = HALF * k + BAND * s
            ref[rows, :] = vr_new[row : row + BAND, 0:ROWS]
        b0, b1, b2, b3 = (vr_new[HALF * k + BAND * (TILES + b) : HALF * k + BAND * (GROUP + b), :] for b in range(GROUP))
        lane = lane_iota((BAND, LANES))
        b2 = pltpu.roll(b2, CHIP, 1)
        vr_d[rows, 0:LANES] = jnp.where(lane < ROWS, b0, jnp.where(lane < CHIP, pltpu.roll(b1, ROWS, 1), b2))
        vr_d[rows, LANES:192] = jnp.where(lane < LAYERS, b2, pltpu.roll(b3, LAYERS, 1))[:, 0:HALF]
    for n in range(OUTS):
        if n not in by_layer:
            copies[n].start()

    def body(layer):
        index = HALF * (layer // BAND) + layer % BAND

        def one(tile, slot, w, m, wo, mo, rows, lanes):
            factor = scale[pl.ds(index + BAND * slot, 1), :]
            update = (ut[layer, tile] * factor)[:, 0 : lanes.stop - lanes.start]
            weight_new, moment_new = finish(update, w[layer, rows, lanes], m[layer, rows, lanes])
            wo[layer, rows, lanes] = weight_new
            mo[layer, rows, lanes] = moment_new

        every = slice(0, ROWS)
        for t in range(TILES):
            one(t, 0, w_u, m_u, wo_u, mo_u, every, slice(LANES * t, LANES * t + LANES))
            one(TILES + t, 1, w_q, m_q, wo_q, mo_q, every, slice(LANES * t, min(LANES * t + LANES, 288)))
        one(UNITS, PAIR, w_o, m_o, wo_o, mo_o, every, slice(0, CHIP))
        for b in range(GROUP):
            one(7 + b, TILES, w_d, m_d, wo_d, mo_d, slice(ROWS * b, ROWS * b + ROWS), slice(0, CHIP))

    def two_layers(i, carry):
        for layer in range(PAIR):
            body(PAIR * i + layer)
        layers = pl.ds(PAIR * i, PAIR)
        for n in by_layer:
            pltpu.make_async_copy(buffers[n].at[layers], outs[n].at[layers], sems.at[n]).start()
        return carry

    lax.fori_loop(0, BAND, two_layers, 0)
    for copy in copies:
        copy.wait()


def solution(mesh):
    tp_size = mesh.shape["tp"]
    devices = tp_size * mesh.shape["fsdp"]
    vmem = pl.BlockSpec(memory_space=pltpu.VMEM)
    hbm = pl.BlockSpec(memory_space=pltpu.HBM)

    def local_step(g_qkv, g_out, g_up, g_down, g_vec, w_qkv, w_out, w_up, w_down, w_vec, m_qkv, m_out, m_up, m_down, m_vec, vr_qkv, vc_qkv, vr_out, vc_out, vr_up, vc_up, vr_down, vc_down, v_vec):
        def flat(g):
            g = jnp.swapaxes(g[0], 1, PAIR)
            return g.reshape(g.shape[0] * g.shape[1], g.shape[PAIR])

        dma = pltpu.SemaphoreType.DMA
        half = (BAND, VEC)
        small = (g_vec[0], vr_qkv, vc_qkv, vr_out, vc_out, vr_up, vc_up, vr_down, vc_down, v_vec)
        weights = (w_qkv, w_out, w_up, w_down, w_vec)
        moments = (m_qkv, m_out, m_up, m_down, m_vec)
        results = pl.pallas_call(
            functools.partial(reduce_kernel, tp_size),
            out_shape=[
                jax.ShapeDtypeStruct((LAYERS, 11, ROWS, LANES), F32),
                jax.ShapeDtypeStruct((LANES, LANES), F32),
                jax.ShapeDtypeStruct((LANES, LANES), F32),
                jax.ShapeDtypeStruct((LANES, LANES), F32),
                jax.ShapeDtypeStruct((LAYERS, VEC), F32),
                jax.ShapeDtypeStruct((LAYERS, VEC), F32),
            ]
            + [jax.ShapeDtypeStruct(a.shape, a.dtype) for a in weights + moments],
            in_specs=[hbm] * (GROUP + SMALL + STATE),
            out_specs=[vmem] * (UNITS + STATE),
            scratch_shapes=[pltpu.VMEM(a.shape, a.dtype) for a in small]
            + [
                pltpu.VMEM((GROUP, DIM, DIM), F32),
                pltpu.VMEM((1152, DIM), F32),
                pltpu.VMEM((DIM, DIM), F32),
                pltpu.VMEM((DIM, 1536), F32),
                pltpu.VMEM((GROUP, DIM, DIM), F32),
                pltpu.VMEM((1152, DIM), F32),
                pltpu.VMEM((DIM, DIM), F32),
                pltpu.VMEM((DIM, 1536), F32),
                pltpu.VMEM((SLOTS, PAIR, PAIR, UNITS, PAIR, ROWS, LANES), F32),
                pltpu.VMEM((PIECES, PAIR, TILES, PAIR, ROWS, LANES), F32),
                pltpu.VMEM((PIECES, PAIR, TILES, PAIR, ROWS, LANES), F32),
                pltpu.VMEM((PIECES, TILES, PAIR, ROWS, LANES), F32),
                pltpu.VMEM((PIECES, TILES, PAIR, ROWS, LANES), F32),
                pltpu.VMEM((PAIR, PIECES, UNITS, ROWS, LANES), F32),
                pltpu.VMEM((PIECES, UNITS, ROWS, LANES), F32),
                pltpu.VMEM((PAIR, BAND, BAND, LANES), F32),
                pltpu.VMEM((PAIR, BAND, BAND, LANES), F32),
                pltpu.VMEM((PAIR, BAND, BAND, LANES), F32),
                pltpu.VMEM((BAND, BAND, LANES), F32),
                pltpu.VMEM((ROWS, LANES), F32),
                pltpu.VMEM((BAND, LANES), F32),
                pltpu.VMEM((tp_size, ROWS, LANES), F32),
                pltpu.VMEM((tp_size, BAND, LANES), F32),
                pltpu.VMEM((ROWS, LANES), F32),
                pltpu.VMEM((LANES, LANES), F32),
                pltpu.VMEM((devices, 1, DIM), F32),
                pltpu.VMEM((devices, 1, LANES), F32),
                pltpu.VMEM((LANES, LANES), F32),
                pltpu.VMEM((LAYERS, 256), F32),
                pltpu.VMEM(half, F32),
                pltpu.VMEM(half, F32),
                pltpu.VMEM(half, F32),
                pltpu.VMEM((TILES,) + half, F32),
                pltpu.VMEM((LAYERS, VEC), F32),
                dma((SOURCES,)),
                dma((UNITS,)), dma((UNITS,)),
                dma((IN_FLIGHT,)), dma((IN_FLIGHT,)),
                dma((IN_FLIGHT,)), dma((IN_FLIGHT,)),
                dma((IN_FLIGHT,)), dma((IN_FLIGHT,)),
                dma((SOURCES,)), dma((SOURCES,)),
                dma((GROUP,)), dma((GROUP,)),
                dma((1,)), dma((GROUP,)),
                pltpu.SemaphoreType.REGULAR((PAIR,)),
            ],
            compiler_params=pltpu.CompilerParams(
                collective_id=0, has_side_effects=True, vmem_limit_bytes=40 * 1024 * 1024
            ),
            name="reduce",
        )(*[pltpu.with_memory_space_constraint(a, pltpu.HBM) for a in (flat(g_qkv), flat(g_out), g_up[0], flat(g_down)) + small + weights + moments])

        outs = weights + moments + small[1:]
        return tuple(
            pl.pallas_call(
                update_kernel,
                out_shape=[jax.ShapeDtypeStruct(a.shape, a.dtype) for a in outs],
                in_specs=[vmem] * len(results),
                out_specs=[hbm] * OUTS,
                scratch_shapes=[pltpu.VMEM(a.shape, a.dtype) for a in outs] + [dma((OUTS,))],
                compiler_params=pltpu.CompilerParams(vmem_limit_bytes=24 * 1024 * 1024),
                name="update",
            )(*results)
        )

    grad_spec = P("fsdp", None, None, "tp")
    vec_grad_spec = P("fsdp", None, "tp")
    mat_spec = P(None, "fsdp", "tp")
    vec_spec = P(None, "tp")
    row_spec = P(None, "fsdp")
    state_specs = (mat_spec,) * GROUP + (vec_spec,) + (mat_spec,) * GROUP + (vec_spec,) + (row_spec, vec_spec) * GROUP + (vec_spec,)
    arg_specs = (grad_spec,) * GROUP + (vec_grad_spec,) + state_specs
    return jax.shard_map(local_step, mesh=mesh, in_specs=arg_specs, out_specs=state_specs, check_vma=False)
```
